32 devices in a mesh: seq: 8 (over y, x, core), tp: 4 (over z).
Axes of the slice: x: 2, y: 2, z: 4, core: 2. Of those that a mesh axis runs over, the one named last changes fastest.
Arguments:
- queries: bfloat16 [4096, 8192], P('seq', 'tp'), may hold values from -6 to 6
- keys: bfloat16 [4096, 8192], P('seq', 'tp'), may hold values from -0.5 to 0.5
- values: bfloat16 [4096, 8192], P('seq', 'tp'), may hold values from -6 to 6
- gate: bfloat16 [4096, 8192], P('seq', 'tp'), may hold values from -6 to 6
- log_decay: float32 [4096, 64], P('seq', 'tp'), may hold values from -0.8 to 0
- out_grad: bfloat16 [4096, 8192], P('seq', 'tp'), may hold values from -6 to 6
Outputs:
- output: bfloat16 [4096, 8192], P('seq', 'tp')
- query_grad: bfloat16 [4096, 8192], P('seq', 'tp')
- key_grad: bfloat16 [4096, 8192], P('seq', 'tp')
- value_grad: bfloat16 [4096, 8192], P('seq', 'tp')
- gate_grad: bfloat16 [4096, 8192], P('seq', 'tp')
The draws below stay inside these ranges and needn't reach their ends.
All inputs are finite; a program needn't handle non-finite values.
Results may differ from the reference program's by a relative error of at most 0.0051.
Values sent between devices are 32-bit elements; how exact they have to be, the bound alone decides.
A program may use at most 128 MiB of HBM per device.

```python
import jax
import jax.numpy as jnp
from jax import lax

HEAD_COUNT = 64
HEAD = 128
TOK_DEV = 512
TOKEN_COUNT = 4096
N_SEQ = 8


def draw_log_decay(key, part):
    every_key = jax.random.split(jax.random.fold_in(key, 7), 6)
    share = 0.5
    slow = jax.random.uniform(every_key[0], (HEAD_COUNT,)) < share
    slow_rate = jnp.exp(jax.random.uniform(every_key[1], (HEAD_COUNT,), jnp.float32, jnp.log(0.05), jnp.log(0.5))) / TOKEN_COUNT
    fast_rate = jax.random.uniform(every_key[2], (HEAD_COUNT,), jnp.float32, 1.0 / 50.0, 1.0 / 30.0)
    decay_rate = jnp.where(slow, slow_rate, fast_rate)
    random_noise = jax.random.uniform(every_key[3], (TOKEN_COUNT, HEAD_COUNT), jnp.float32, 0.5, 1.5)
    decay_spike = jax.random.uniform(every_key[4], (TOKEN_COUNT, HEAD_COUNT)) < 3.0 / TOKEN_COUNT
    decay_falloff = jnp.log(jax.random.uniform(every_key[5], (TOKEN_COUNT, HEAD_COUNT), jnp.float32, 0.5, 0.8))
    return (-decay_rate[None, :] * random_noise + jnp.where(decay_spike, decay_falloff, 0.0)).astype(jnp.float32)


def steps_of(key, shape, cuts, smallest, top_value):
    def one(position, parts):
        draws = jax.random.uniform(jax.random.fold_in(jax.random.fold_in(key, 6), position), (parts,), jnp.float32, smallest / len(cuts), top_value / len(cuts))
        return jnp.repeat(jnp.exp(draws), shape[position] // parts).reshape((-1,) + (1,) * (len(shape) - position - 1))

    loudness = one(*cuts[0])
    for cut in cuts[1:]:
        loudness = loudness * one(*cut)
    return loudness


def scatter_about(own_key, extent, scale, reach, cuts=(), dtype=jnp.bfloat16):
    drawn = scale * jax.random.normal(own_key, extent, jnp.float32)
    if cuts:
        drawn = drawn * steps_of(own_key, extent, cuts, -0.22, 0.18)
    return jnp.clip(drawn, -reach, reach).astype(dtype)


def setup_inputs(seed: int = 0) -> dict:
    key_of = jax.random.split(jax.random.key(seed), 7)
    queries = scatter_about(key_of[0], (TOKEN_COUNT, HEAD_COUNT * HEAD), 1.0, 6.0, ((0, 8), (1, 4)))
    keys = scatter_about(key_of[1], (TOKEN_COUNT, HEAD_COUNT * HEAD), HEAD ** -0.5, 0.5, ((0, 8), (1, 4)))
    values = scatter_about(key_of[2], (TOKEN_COUNT, HEAD_COUNT * HEAD), 1.0, 6.0, ((0, 8), (1, 4)))
    gate = scatter_about(key_of[3], (TOKEN_COUNT, HEAD_COUNT * HEAD), 1.0, 6.0, ((0, 8), (1, 4)))
    log_decay = draw_log_decay(jax.random.fold_in(key_of[6], 71), 0)
    out_grad = scatter_about(key_of[5], (TOKEN_COUNT, HEAD_COUNT * HEAD), 1.0, 6.0, ((0, 8), (1, 4)))
    return {"queries": queries, "keys": keys, "values": values, "gate": gate, "log_decay": log_decay, "out_grad": out_grad}


HIGH = lax.Precision.HIGHEST

def decay_table(within):
    gap = within.T[:, :, None] - within.T[:, None, :]
    rows = lax.broadcasted_iota(jnp.int32, gap.shape, 1)
    cols = lax.broadcasted_iota(jnp.int32, gap.shape, 2)
    return jnp.where(rows >= cols, jnp.exp(jnp.minimum(gap, 0.0)), 0.0)

def block_probs(qh, kh, decay):
    scores = jnp.einsum('thd,shd->hts', qh.astype(jnp.float32), kh.astype(jnp.float32))
    return (scores * decay).astype(jnp.bfloat16)

def forward_block(state, pieces):
    qh, kh, vh, rates = pieces
    within = jnp.cumsum(rates, axis=0)
    last = within[-1]
    decay = decay_table(within)
    probs = block_probs(qh, kh, decay)
    qf = qh.astype(jnp.float32)
    kf = kh.astype(jnp.float32)
    vf = vh.astype(jnp.float32)
    intra = jnp.einsum('hts,shd->thd', probs.astype(jnp.float32), vf)
    inter = jnp.exp(within)[:, :, None] * jnp.einsum('thd,hde->the', qf, state, precision=HIGH)
    tail = jnp.exp(last[None, :] - within)
    local = jnp.einsum('thd,the->hde', kf * tail[:, :, None], vf, precision=HIGH)
    fresh = jnp.exp(last)[:, None, None] * state + local
    return (fresh, (intra + inter, state))

def backward_block(grad_state, pieces):
    qh, kh, vh, rates, grad_b, state = pieces
    within = jnp.cumsum(rates, axis=0)
    last = within[-1]
    decay = decay_table(within)
    probs = block_probs(qh, kh, decay)
    qf = qh.astype(jnp.float32)
    kf = kh.astype(jnp.float32)
    vf = vh.astype(jnp.float32)
    gradf = grad_b.astype(jnp.float32)
    pgrad = (jnp.einsum('thd,shd->hts', gradf, vf) * decay).astype(jnp.bfloat16).astype(jnp.float32)
    grow = jnp.exp(within)[:, :, None]
    tail = jnp.exp(last[None, :] - within)[:, :, None]
    query_grad = jnp.einsum('hts,shd->thd', pgrad, kf) + grow * jnp.einsum('the,hde->thd', gradf, state, precision=HIGH)
    key_grad = jnp.einsum('hts,thd->shd', pgrad, qf) + tail * jnp.einsum('the,hde->thd', vf, grad_state, precision=HIGH)
    value_grad = jnp.einsum('hts,thd->shd', probs.astype(jnp.float32), gradf) + tail * jnp.einsum('thd,hde->the', kf, grad_state, precision=HIGH)
    weighted = jnp.einsum('thd,the->hde', qf * grow, gradf, precision=HIGH)
    fresh = weighted + jnp.exp(last)[:, None, None] * grad_state
    return (fresh, (query_grad.astype(jnp.bfloat16), key_grad.astype(jnp.bfloat16), value_grad.astype(jnp.bfloat16)))

def reference(queries, keys, values, gate, log_decay, out_grad):
    blocks = N_SEQ
    width = HEAD_COUNT * HEAD
    qb = queries.reshape(blocks, TOK_DEV, HEAD_COUNT, HEAD)
    kb = keys.reshape(blocks, TOK_DEV, HEAD_COUNT, HEAD)
    vb = values.reshape(blocks, TOK_DEV, HEAD_COUNT, HEAD)
    rb = log_decay.reshape(blocks, TOK_DEV, HEAD_COUNT)
    start = jnp.zeros((HEAD_COUNT, HEAD, HEAD), jnp.float32)
    unused, (attn_blocks, states) = lax.scan(forward_block, start, (qb, kb, vb, rb))
    attn = attn_blocks.reshape(TOKEN_COUNT, width)
    scale = lax.rsqrt(lax.optimization_barrier(jnp.sum(attn * attn, axis=1)) / width + 1e-06)
    normed = attn * scale[:, None]
    sig = jax.nn.sigmoid(gate.astype(jnp.float32))
    output = (normed * sig).astype(jnp.bfloat16)
    upstream = out_grad.astype(jnp.float32)
    dnorm = upstream * sig
    gate_grad = (upstream * normed * sig * (1.0 - sig)).astype(jnp.bfloat16)
    center = lax.optimization_barrier(jnp.sum(dnorm * normed, axis=1)) / width
    attn_grad = (scale[:, None] * (dnorm - normed * center[:, None])).astype(jnp.bfloat16)
    gb = attn_grad.reshape(blocks, TOK_DEV, HEAD_COUNT, HEAD)
    unused2, (dq, dk, dv) = lax.scan(backward_block, start, (qb, kb, vb, rb, gb, states), reverse=True)
    return (output, dq.reshape(TOKEN_COUNT, width), dk.reshape(TOKEN_COUNT, width), dv.reshape(TOKEN_COUNT, width), gate_grad)
```

```python
import functools

import jax
import jax.numpy as jnp
from jax import lax
from jax.experimental import pallas as pl
from jax.experimental.pallas import tpu as pltpu
from jax.sharding import PartitionSpec as P

MESH = pl.DeviceIdType.MESH
F32 = jnp.float32
BF16 = jnp.bfloat16


def nt(a, b):
    return lax.dot_general(a, b, (((1,), (1,)), ((), ())), preferred_element_type=F32)


def tn(a, b):
    return lax.dot_general(a, b, (((0,), (0,)), ((), ())), preferred_element_type=F32)


def nn(a, b):
    return lax.dot_general(a, b, (((1,), (0,)), ((), ())), preferred_element_type=F32)


def three_parts(x):
    high = x.astype(BF16).astype(F32)
    rest = x - high
    middle = rest.astype(BF16).astype(F32)
    low = (rest - middle).astype(BF16).astype(F32)
    return high, middle, low


def stacked(x):
    parts = three_parts(x)
    spare = 128 - 3 * x.shape[0]
    return jnp.concatenate([*parts, jnp.zeros((spare, x.shape[1]), F32)], axis=0)


def kernel(
    n_seq, n_tp, heads, dim, tokens,
    q_hbm, k_hbm, v_hbm, gate_hbm, rate_hbm, up_hbm,
    up, gate, q, k, v, attn, dvp, state_grad, cols,
    rate, rows, split, grad, probs,
    own, other, sent, got, edge, far, state, span, span_in, factor,
    sums, sums_in, scale_ref, center_ref,
    in_sem, sp_send, sp_recv, s0_send, s0_recv, st_send, st_recv, fin_send, fin_recv, tp_send, tp_recv,
):
    width = heads * dim * n_tp
    half = heads // 2
    bits = n_seq.bit_length() - 1
    chips = bits - 1
    block = min(256, tokens)
    nb = tokens // block
    me = lax.axis_index("seq")
    z = lax.axis_index("tp")
    core = lax.rem(me, 2)

    def bit_of(b):
        return lax.rem(me // (1 << b), 2)

    def partner(b):
        return (me + (1 << b) * (1 - 2 * bit_of(b)), z)

    def takes(d, b):
        return bit_of(b) if d == 0 else 1 - bit_of(b)

    def load(i, a, b):
        return pltpu.make_async_copy(a, b, in_sem.at[i])

    loads = [
        load(i, a, b)
        for i, (a, b) in enumerate(
            ((rate_hbm, rate), (k_hbm, k), (v_hbm, v), (q_hbm, q), (up_hbm, up), (gate_hbm, gate))
        )
    ]
    for c in loads[:3]:
        c.start()

    barrier = pltpu.get_barrier_semaphore()
    for b in range(bits):
        pl.semaphore_signal(barrier, inc=1, device_id=partner(b), device_id_type=MESH)
    for d in range(1, n_tp):
        pl.semaphore_signal(
            barrier, inc=1, device_id=(me, lax.rem(z + d, n_tp)), device_id_type=MESH
        )

    def lane(h):
        return pl.ds(pl.multiple_of(h * dim, dim), dim)

    def mine(c):
        return core * half + c

    def others(c):
        return (1 - core) * half + c

    loads[0].wait()
    upto = (
        lax.broadcasted_iota(jnp.int32, (tokens, tokens), 0)
        <= lax.broadcasted_iota(jnp.int32, (tokens, tokens), 1)
    ).astype(BF16)
    parts = nn(stacked(rate[...]).astype(BF16), upto)
    across = parts[0:heads] + parts[heads : 2 * heads] + parts[2 * heads : 3 * heads]
    rows[...] = across
    split[...] = stacked(across).T.astype(BF16)
    span[0] = jnp.broadcast_to(across[:, tokens - 1 : tokens], (heads, dim))
    loads[3].start()
    pl.semaphore_wait(barrier, bits + n_tp - 1)

    def sp_copy(b):
        return pltpu.make_async_remote_copy(
            src_ref=span.at[b], dst_ref=span_in.at[b], send_sem=sp_send.at[b],
            recv_sem=sp_recv.at[b], device_id=partner(b), device_id_type=MESH,
        )

    sp_copy(0).start()

    def s0_copy(d, h):
        return pltpu.make_async_remote_copy(
            src_ref=own.at[d, h], dst_ref=other.at[d, h], send_sem=s0_send.at[d, h],
            recv_sem=s0_recv.at[d, h], device_id=partner(0), device_id_type=MESH,
        )

    def st_copy(d, s, c):
        return pltpu.make_async_remote_copy(
            src_ref=sent.at[d, s, c], dst_ref=got.at[d, s, c], send_sem=st_send.at[d, s, c],
            recv_sem=st_recv.at[d, s, c], device_id=partner(s + 1), device_id_type=MESH,
        )

    def fin_copy(d, c):
        return pltpu.make_async_remote_copy(
            src_ref=edge.at[d, c], dst_ref=far.at[d, c], send_sem=fin_send.at[d, c],
            recv_sem=fin_recv.at[d, c], device_id=partner(0), device_id_type=MESH,
        )

    def span_step(b):
        sp_copy(b).wait_recv()
        here, there = span[b], span_in[b]
        if b + 1 < bits:
            span[b + 1] = here + there
            sp_copy(b + 1).start()
        for d in (0, 1):
            f = takes(d, b).astype(F32)
            factor[d, b, 0] = jnp.exp(there * (1.0 - f))
            factor[d, b, 1] = jnp.exp(here * f)
            if b == 0:
                factor[d, b, 2] = jnp.exp(there * f)
            else:
                before = jnp.zeros((heads, dim), F32)
                for r in range(1, b):
                    before = before + takes(d, r).astype(F32) * span_in[r]
                factor[d, b, 2] = f * jnp.exp(before)

    def row_of(d, b, n, h):
        return factor[d, b, n, pl.ds(h, 1), :]

    def send_level(d, s, c):
        if s == chips - 1:

            @pl.when(takes(d, s + 1) == 0)
            def _():
                st_copy(d, s, c).start()
        else:
            st_copy(d, s, c).start()

    def level0(d, c):
        h = mine(c)
        s0_copy(d, h).wait_recv()
        sent[d, 0, c] = row_of(d, 0, 0, h) * own[d, h] + row_of(d, 0, 1, h) * other[d, h]
        send_level(d, 0, c)

    def step(d, s, c):
        h = mine(c)

        def arrive():
            st_copy(d, s, c).wait_recv()
            theirs = got[d, s, c]
            on_top = row_of(d, s + 1, 2, h) * theirs
            edge[d, c] = on_top if s == 0 else edge[d, c] + on_top
            if s + 1 < chips:
                sent[d, s + 1, c] = (
                    row_of(d, s + 1, 0, h) * sent[d, s, c] + row_of(d, s + 1, 1, h) * theirs
                )

        if s + 1 < chips:
            arrive()
            send_level(d, s + 1, c)
            return
        pl.when(takes(d, s + 1) == 1)(arrive)
        if s == 0:

            @pl.when(takes(d, s + 1) == 0)
            def _():
                edge[d, c] = jnp.zeros((dim, dim), F32)

        fin_copy(d, c).start()

    def put(d, c, target):
        f = takes(d, 0).astype(F32)
        h = mine(c)
        target[h] = (row_of(d, 0, 2, h) * edge[d, c] + f * other[d, h]).astype(BF16)
        h = others(c)
        s0_copy(d, h).wait_recv()
        fin_copy(d, c).wait_recv()
        target[h] = (row_of(d, 0, 2, h) * far[d, c] + f * other[d, h]).astype(BF16)

    def local_pair(c):
        pair = (others(c), mine(c))
        at = lax.broadcasted_iota(jnp.int32, (128, dim), 0)
        pick = jnp.concatenate(
            [
                ((at == h) | (at == h + heads) | (at == h + 2 * heads)).astype(F32).astype(BF16)
                for h in pair
            ],
            axis=1,
        )
        wide = nn(split[...], pick)
        for n, h in enumerate(pair):
            col = wide[:, n * dim : (n + 1) * dim]
            cols[h] = col
            last = col[tokens - 1 : tokens, :]
            scaled = (k[:, lane(h)].astype(F32) * jnp.exp(last - col)).astype(BF16)
            own[0, h] = tn(scaled, v[:, lane(h)])
        for h in pair:
            s0_copy(0, h).start()

    def first_exchange(d, body, lead):
        lead = min(lead, half)

        @pl.loop(0, lead)
        def _(c):
            body(c)

        if d == 0:
            span_step(0)

        @pl.loop(lead, half)
        def _(c):
            body(c)
            level0(d, c - lead)

        if d == 0:
            for b in range(1, bits):
                span_step(b)

        @pl.loop(half - lead, half)
        def _(c):
            level0(d, c)

    def ticks(d, body, early, finish):
        lags = [2 * s - early for s in range(chips)]
        lag = lags[-1] + 1
        for s in range(chips):
            for c in range(max(0, -lags[s])):
                step(d, s, c)

        @pl.loop(0, half + lag)
        def _(t):
            @pl.when(t < half)
            def _():
                body(t)

            for s in range(chips):

                @pl.when((t >= max(0, lags[s])) & (t < half + lags[s]))
                def _():
                    step(d, s, t - lags[s])

            @pl.when(t >= lag)
            def _():
                finish(t - lag)

    loads[1].wait()
    loads[2].wait()
    first_exchange(0, local_pair, 3)
    loads[4].start()
    loads[5].start()

    tiles = [(i, j) for i in range(nb) for j in range(i + 1)]
    keep = (
        lax.broadcasted_iota(jnp.int32, (block, block), 0)
        >= lax.broadcasted_iota(jnp.int32, (block, block), 1)
    )

    def decay_of(h, i, j):
        col = cols[h, i * block : (i + 1) * block, :]
        col = jnp.concatenate([col] * (block // dim), axis=1)
        row = rows[pl.ds(h, 1), j * block : (j + 1) * block]
        value = jnp.exp(jnp.minimum(col - row, 0.0))
        return jnp.where(keep, value, 0.0) if i == j else value

    def span_of(i):
        return slice(i * block, (i + 1) * block)

    def intra(h):
        for i in range(nb):
            total = None
            for j in range(i + 1):
                s = nt(q[span_of(i), lane(h)], k[span_of(j), lane(h)])
                p = (s * decay_of(h, i, j)).astype(BF16)
                probs[h, tiles.index((i, j))] = p
                o = nn(p, v[span_of(j), lane(h)])
                total = o if total is None else total + o
            attn[span_of(i), lane(h)] = total

    def both(body):
        def pair(c):
            body(mine(c))
            body(others(c))

        return pair

    def finish_attn(c):
        put(0, c, state)
        for i in range(nb):
            r = span_of(i)
            square, inner = scale_ref[r, :], center_ref[r, :]
            for h in (mine(c), others(c)):
                a = attn[r, lane(h)] + jnp.exp(cols[h, r, :]) * nn(q[r, lane(h)], state[h])
                attn[r, lane(h)] = a
                square = square + a * a
                sig = jax.nn.sigmoid(gate[r, lane(h)].astype(F32))
                inner = inner + up[r, lane(h)].astype(F32) * sig * a
            scale_ref[r, :] = square
            center_ref[r, :] = inner

    scale_ref[...] = jnp.zeros_like(scale_ref)
    center_ref[...] = jnp.zeros_like(center_ref)
    loads[3].wait()
    loads[4].wait()
    loads[5].wait()
    ticks(0, both(intra), 0, finish_attn)

    strips = tokens // 128

    def packed(x):
        turned = jnp.sum(x.T, axis=0, keepdims=True)
        return [turned[:, n * 128 : (n + 1) * 128] for n in range(strips)]

    spare = -2 * strips % 8
    pieces = packed(scale_ref[...]) + packed(center_ref[...])
    if spare:
        pieces.append(jnp.zeros((spare, 128), F32))
    sums[...] = jnp.concatenate(pieces, axis=0)

    def tp_copy(d):
        return pltpu.make_async_remote_copy(
            src_ref=sums, dst_ref=sums_in.at[d - 1], send_sem=tp_send.at[d - 1],
            recv_sem=tp_recv.at[d - 1], device_id=(me, lax.rem(z + d, n_tp)), device_id_type=MESH,
        )

    for d in range(1, n_tp):
        tp_copy(d).start()
    total = sums[...]
    for d in range(1, n_tp):
        tp_copy(d).wait_recv()
        total = total + sums_in[d - 1]
    scale = lax.rsqrt(total[0:strips] / width + 1e-06)
    center = total[strips : 2 * strips] * scale / width
    for n in range(strips):
        r = slice(n * 128, (n + 1) * 128)
        scale_ref[r, :] = jnp.broadcast_to(scale[n : n + 1, :], (128, 128)).T
        center_ref[r, :] = jnp.broadcast_to(center[n : n + 1, :], (128, 128)).T

    def pointwise(h):
        weighted = None
        for i in range(nb):
            r = span_of(i)
            sc = scale_ref[r, :]
            normed = attn[r, lane(h)] * sc
            sig = jax.nn.sigmoid(gate[r, lane(h)].astype(F32))
            dnorm = up[r, lane(h)].astype(F32) * sig
            g = (sc * (dnorm - normed * center_ref[r, :])).astype(BF16)
            grad[r, lane(h)] = g
            up[r, lane(h)] = (normed * sig).astype(BF16)
            gate[r, lane(h)] = (dnorm * normed * (1.0 - sig)).astype(BF16)
            grown = (q[r, lane(h)].astype(F32) * jnp.exp(cols[h, r, :])).astype(BF16)
            w = tn(grown, g)
            weighted = w if weighted is None else weighted + w
        own[1, h] = weighted

    def pointwise_pair(c):
        pair = (others(c), mine(c))
        for h in pair:
            pointwise(h)
        for h in pair:
            s0_copy(1, h).start()

    first_exchange(1, pointwise_pair, 3)

    def backward(h):
        dq = [None] * nb
        dk = [None] * nb
        dv = [None] * nb

        def add(parts, n, x):
            parts[n] = x if parts[n] is None else parts[n] + x

        for i, j in tiles:
            g = grad[span_of(i), lane(h)]
            pg = (nt(g, v[span_of(j), lane(h)]) * decay_of(h, i, j)).astype(BF16)
            add(dq, i, nn(pg, k[span_of(j), lane(h)]))
            add(dk, j, tn(pg, q[span_of(i), lane(h)]))
            add(dv, j, tn(probs[h, tiles.index((i, j))], g))
        for i in range(nb):
            r = span_of(i)
            carried = jnp.exp(cols[h, r, :]) * nt(grad[r, lane(h)], state[h])
            q[r, lane(h)] = (dq[i] + carried).astype(BF16)
            attn[r, lane(h)] = dk[i]
            dvp[r, lane(h)] = dv[i]

    ticks(1, both(backward), 1, lambda c: put(1, c, state_grad))

    for b in range(bits):
        sp_copy(b).wait_send()
    for d in (0, 1):

        @pl.loop(0, heads)
        def _(h):
            s0_copy(d, h).wait_send()

        @pl.loop(0, half)
        def _(c):
            for s in range(chips - 1):
                st_copy(d, s, c).wait_send()

            @pl.when(takes(d, chips) == 0)
            def _():
                st_copy(d, chips - 1, c).wait_send()

            fin_copy(d, c).wait_send()

    for d in range(1, n_tp):
        tp_copy(d).wait_send()


def last_kernel(
    heads, dim, tokens,
    out_ref, gg_ref, dq_ref, k, v, dkp, dvp, state_grad, cols,
    out_hbm, dq_hbm, dk_hbm, dv_hbm, gg_hbm,
    dk, dv, sem, pair_sem,
):
    block = min(256, tokens)
    trips = heads // 2
    whole = [
        pltpu.make_async_copy(a, b, sem.at[i])
        for i, (a, b) in enumerate(((out_ref, out_hbm), (gg_ref, gg_hbm), (dq_ref, dq_hbm)))
    ]
    for c in whole:
        c.start()

    def strips(i):
        part = pl.ds(pl.multiple_of(i * 2 * dim, 2 * dim), 2 * dim)
        return [
            pltpu.make_async_copy(a.at[:, part], b.at[:, part], pair_sem.at[n, i])
            for n, (a, b) in enumerate(((dk, dk_hbm), (dv, dv_hbm)))
        ]

    @pl.loop(0, trips)
    def _(i):
        for h in (2 * i, 2 * i + 1):
            at = pl.ds(pl.multiple_of(h * dim, dim), dim)
            last = cols[h, tokens - 1 : tokens, :]
            for n in range(tokens // block):
                r = slice(n * block, (n + 1) * block)
                tail = jnp.exp(last - cols[h, r, :])
                key = dkp[r, at] + tail * nt(v[r, at], state_grad[h])
                value = dvp[r, at] + tail * nn(k[r, at], state_grad[h])
                dk[r, at] = key.astype(BF16)
                dv[r, at] = value.astype(BF16)
        for c in strips(i):
            c.start()

    @pl.loop(0, trips)
    def _(i):
        for c in strips(i):
            c.wait()

    for c in whole:
        c.wait()


def solution(mesh):
    n_seq, n_tp = mesh.shape["seq"], mesh.shape["tp"]

    def shards(queries, keys, values, gate, log_decay, out_grad):
        tokens, flat = queries.shape
        heads = log_decay.shape[1]
        dim = flat // heads
        half = heads // 2
        bits = n_seq.bit_length() - 1
        chips = bits - 1
        block = min(256, tokens)
        nb = tokens // block
        tile = (dim, dim)
        dma = pltpu.SemaphoreType.DMA
        peers = max(n_tp - 1, 1)
        sums = (-(-2 * (tokens // 128) // 8) * 8, 128)
        hbm = pl.BlockSpec(memory_space=pltpu.HBM)
        vmem = pl.BlockSpec(memory_space=pltpu.VMEM)
        big = pltpu.VMEM((tokens, flat), BF16)
        wide = pltpu.VMEM((tokens, flat), F32)
        flops = 2 * tokens * tokens * flat * 5 + 2 * tokens * flat * dim * 7
        up, gg, dq, k, v, dkp, dvp, state_grad, cols = pl.pallas_call(
            functools.partial(kernel, n_seq, n_tp, heads, dim, tokens),
            out_shape=[
                big, big, big, big, big, wide, wide,
                pltpu.VMEM((heads, *tile), BF16), pltpu.VMEM((heads, tokens, dim), F32),
            ],
            in_specs=[hbm] * 6,
            out_specs=[vmem] * 9,
            scratch_shapes=[
                pltpu.VMEM((heads, tokens), F32), pltpu.VMEM((heads, tokens), F32),
                pltpu.VMEM((tokens, 128), BF16), big,
                pltpu.VMEM((heads, nb * (nb + 1) // 2, block, block), BF16),
                pltpu.VMEM((2, heads, *tile), F32),
                pltpu.VMEM((2, heads, *tile), F32),
                pltpu.VMEM((2, chips, half, *tile), F32),
                pltpu.VMEM((2, chips, half, *tile), F32),
                pltpu.VMEM((2, half, *tile), F32),
                pltpu.VMEM((2, half, *tile), F32),
                pltpu.VMEM((heads, *tile), BF16),
                pltpu.VMEM((bits, heads, dim), F32), pltpu.VMEM((bits, heads, dim), F32),
                pltpu.VMEM((2, bits, 3, heads, dim), F32),
                pltpu.VMEM(sums, F32), pltpu.VMEM((peers, *sums), F32),
                pltpu.VMEM((tokens, dim), F32), pltpu.VMEM((tokens, dim), F32),
                dma((6,)), dma((bits,)), dma((bits,)), dma((2, heads)), dma((2, heads)),
                dma((2, chips, half)), dma((2, chips, half)), dma((2, half)), dma((2, half)),
                dma((peers,)), dma((peers,)),
            ],
            compiler_params=pltpu.CompilerParams(
                collective_id=0, has_side_effects=True, vmem_limit_bytes=36 << 20
            ),
            cost_estimate=pl.CostEstimate(
                flops=flops, bytes_accessed=tokens * flat * 10, transcendentals=0
            ),
        )(queries, keys, values, gate, log_decay.T, out_grad)
        return tuple(
            pl.pallas_call(
                functools.partial(last_kernel, heads, dim, tokens),
                out_shape=[jax.ShapeDtypeStruct((tokens, flat), BF16)] * 5,
                in_specs=[vmem] * 9,
                out_specs=[hbm] * 5,
                scratch_shapes=[big, big, dma((3,)), dma((2, half))],
                compiler_params=pltpu.CompilerParams(vmem_limit_bytes=16 << 20),
                cost_estimate=pl.CostEstimate(
                    flops=4 * tokens * flat * dim, bytes_accessed=tokens * flat * 10, transcendentals=0
                ),
            )(up, gg, dq, k, v, dkp, dvp, state_grad, cols)
        )

    spec = P("seq", "tp")
    return jax.shard_map(
        shards, mesh=mesh, in_specs=(spec,) * 6, out_specs=(spec,) * 5, check_vma=False
    )
```

```python
import functools

import jax
import jax.numpy as jnp
from jax import lax
from jax.experimental import pallas as pl
from jax.experimental.pallas import tpu as pltpu
from jax.sharding import PartitionSpec as P

MESH = pl.DeviceIdType.MESH
F32 = jnp.float32
BF16 = jnp.bfloat16
LOG2E = 1.4426950408889634
LOW = -1e9


def nt(a, b):
    return lax.dot_general(a, b, (((1,), (1,)), ((), ())), preferred_element_type=F32)


def tn(a, b):
    return lax.dot_general(a, b, (((0,), (0,)), ((), ())), preferred_element_type=F32)


def nn(a, b):
    return lax.dot_general(a, b, (((1,), (0,)), ((), ())), preferred_element_type=F32)


def three_parts(x):
    high = x.astype(BF16).astype(F32)
    rest = x - high
    middle = rest.astype(BF16).astype(F32)
    low = (rest - middle).astype(BF16).astype(F32)
    return high, middle, low


def stacked(x):
    parts = three_parts(x)
    spare = 128 - 3 * x.shape[0]
    return jnp.concatenate([*parts, jnp.zeros((spare, x.shape[1]), F32)], axis=0)


def kernel(
    n_seq, n_tp, heads, dim, tokens,
    q_hbm, k_hbm, v_hbm, gate_hbm, rate_hbm, up_hbm,
    up, gate, grown, k, v, dkt, dvt, state_grad, rows,
    rate, q, cols, split, bias, inside, attn, sig, dnorm, grad, probs,
    own, other, sent, got, edge, far, state, span, span_in, factor,
    sums, sums_in, scale_ref, center_ref,
    in_sem, sp_send, sp_recv, s0_send, s0_recv, st_send, st_recv, fin_send, fin_recv, tp_send, tp_recv,
):
    width = heads * dim * n_tp
    half = heads // 2
    bits = n_seq.bit_length() - 1
    chips = bits - 1
    block = min(256, tokens)
    nb = tokens // block
    me = lax.axis_index("seq")
    z = lax.axis_index("tp")
    core = lax.rem(me, 2)

    def bit_of(b):
        return lax.rem(me // (1 << b), 2)

    def partner(b):
        return (me + (1 << b) * (1 - 2 * bit_of(b)), z)

    def takes(d, b):
        return bit_of(b) if d == 0 else 1 - bit_of(b)

    def load(i, a, b):
        return pltpu.make_async_copy(a, b, in_sem.at[i])

    loads = [
        load(i, a, b)
        for i, (a, b) in enumerate(
            ((rate_hbm, rate), (k_hbm, k), (v_hbm, v), (q_hbm, q), (up_hbm, up), (gate_hbm, gate))
        )
    ]
    for c in loads[:3]:
        c.start()

    barrier = pltpu.get_barrier_semaphore()
    for b in range(bits):
        pl.semaphore_signal(barrier, inc=1, device_id=partner(b), device_id_type=MESH)
    for d in range(1, n_tp):
        pl.semaphore_signal(
            barrier, inc=1, device_id=(me, lax.rem(z + d, n_tp)), device_id_type=MESH
        )

    def lane(h):
        return pl.ds(pl.multiple_of(h * dim, dim), dim)

    def mine(c):
        return core * half + c

    def others(c):
        return (1 - core) * half + c

    loads[0].wait()
    upto = (
        lax.broadcasted_iota(jnp.int32, (tokens, tokens), 0)
        <= lax.broadcasted_iota(jnp.int32, (tokens, tokens), 1)
    ).astype(BF16)
    parts = nn(stacked(rate[...]).astype(BF16), upto)
    across = parts[0:heads] + parts[heads : 2 * heads] + parts[2 * heads : 3 * heads]
    across = across * LOG2E
    rows[...] = across
    split[...] = stacked(across).T.astype(BF16)
    span[0] = jnp.broadcast_to(across[:, tokens - 1 : tokens], (heads, dim))
    loads[3].start()
    corner = lax.broadcasted_iota(jnp.int32, (dim, dim), 0) >= lax.broadcasted_iota(
        jnp.int32, (dim, dim), 1
    )
    bias[...] = jnp.where(corner, 0.0, LOW)

    @pl.loop(0, half)
    def _(i):
        pair = (2 * i, 2 * i + 1)
        at = lax.broadcasted_iota(jnp.int32, (128, dim), 0)
        pick = jnp.concatenate(
            [
                ((at == h) | (at == h + heads) | (at == h + 2 * heads)).astype(F32).astype(BF16)
                for h in pair
            ],
            axis=1,
        )
        for r in (slice(n, n + 256) for n in range(0, tokens, 256)):
            wide = nn(split[r, :], pick)
            for n, h in enumerate(pair):
                cols[h, r, :] = wide[:, n * dim : (n + 1) * dim]

    pl.semaphore_wait(barrier, bits + n_tp - 1)

    def sp_copy(b):
        return pltpu.make_async_remote_copy(
            src_ref=span.at[b], dst_ref=span_in.at[b], send_sem=sp_send.at[b],
            recv_sem=sp_recv.at[b], device_id=partner(b), device_id_type=MESH,
        )

    sp_copy(0).start()

    def s0_copy(d, h):
        return pltpu.make_async_remote_copy(
            src_ref=own.at[d, h], dst_ref=other.at[d, h], send_sem=s0_send.at[d],
            recv_sem=s0_recv.at[d, h], device_id=partner(0), device_id_type=MESH,
        )

    def st_copy(d, s, c):
        return pltpu.make_async_remote_copy(
            src_ref=sent.at[d, s, c], dst_ref=got.at[d, s, c], send_sem=st_send.at[d, s],
            recv_sem=st_recv.at[d, s, c], device_id=partner(s + 1), device_id_type=MESH,
        )

    def fin_copy(d, c):
        return pltpu.make_async_remote_copy(
            src_ref=edge.at[d, c], dst_ref=far.at[d, c], send_sem=fin_send.at[d],
            recv_sem=fin_recv.at[d, c], device_id=partner(0), device_id_type=MESH,
        )

    def span_step(b):
        sp_copy(b).wait_recv()
        here, there = span[b], span_in[b]
        if b + 1 < bits:
            span[b + 1] = here + there
            sp_copy(b + 1).start()
        for d in (0, 1):
            f = takes(d, b).astype(F32)
            factor[d, b, 0] = jnp.exp2(there * (1.0 - f))
            factor[d, b, 1] = jnp.exp2(here * f)
            if b == 0:
                factor[d, b, 2] = jnp.exp2(there * f)
            else:
                before = jnp.zeros((heads, dim), F32)
                for r in range(1, b):
                    before = before + takes(d, r).astype(F32) * span_in[r]
                factor[d, b, 2] = f * jnp.exp2(before)

    def row_of(d, b, n, h):
        return factor[d, b, n, pl.ds(h, 1), :]

    def send_level(d, s, c):
        if s == chips - 1:

            @pl.when(takes(d, s + 1) == 0)
            def _():
                st_copy(d, s, c).start()
        else:
            st_copy(d, s, c).start()

    def level0(d, c):
        h = mine(c)
        s0_copy(d, h).wait_recv()
        sent[d, 0, c] = row_of(d, 0, 0, h) * own[d, h] + row_of(d, 0, 1, h) * other[d, h]
        send_level(d, 0, c)

    def step(d, s, c):
        h = mine(c)

        def arrive():
            st_copy(d, s, c).wait_recv()
            theirs = got[d, s, c]
            on_top = row_of(d, s + 1, 2, h) * theirs
            edge[d, c] = on_top if s == 0 else edge[d, c] + on_top
            if s + 1 < chips:
                sent[d, s + 1, c] = (
                    row_of(d, s + 1, 0, h) * sent[d, s, c] + row_of(d, s + 1, 1, h) * theirs
                )

        if s + 1 < chips:
            arrive()
            send_level(d, s + 1, c)
            return
        pl.when(takes(d, s + 1) == 1)(arrive)
        if s == 0:

            @pl.when(takes(d, s + 1) == 0)
            def _():
                edge[d, c] = jnp.zeros((dim, dim), F32)

        fin_copy(d, c).start()

    def put(d, c, target):
        f = takes(d, 0).astype(F32)
        h = mine(c)
        target[h] = (row_of(d, 0, 2, h) * edge[d, c] + f * other[d, h]).astype(BF16)
        h = others(c)
        s0_copy(d, h).wait_recv()
        fin_copy(d, c).wait_recv()
        target[h] = (row_of(d, 0, 2, h) * far[d, c] + f * other[d, h]).astype(BF16)

    def local_pair(c):
        pair = (others(c), mine(c))
        scaled = []
        for h in pair:
            last = cols[h, tokens - 1 : tokens, :]
            scaled.append((k[:, lane(h)].astype(F32) * jnp.exp2(last - cols[h])).astype(BF16))
        for h, x in zip(pair, scaled):
            own[0, h] = tn(x, v[:, lane(h)])
        for h in pair:
            s0_copy(0, h).start()

    def first_exchange(d, body, lead):
        lead = min(lead, half)

        @pl.loop(0, lead)
        def _(c):
            body(c)

        if d == 0:
            span_step(0)

        @pl.loop(lead, half)
        def _(c):
            body(c)
            level0(d, c - lead)

        if d == 0:
            for b in range(1, bits):
                span_step(b)

        @pl.loop(half - lead, half)
        def _(c):
            level0(d, c)

    def ticks(d, body, early, finish):
        lags = [2 * s - early for s in range(chips)]
        lag = lags[-1] + 1
        for s in range(chips):
            for c in range(max(0, -lags[s])):
                step(d, s, c)

        @pl.loop(0, half + lag)
        def _(t):
            @pl.when(t < half)
            def _():
                body(t)

            for s in range(chips):

                @pl.when((t >= max(0, lags[s])) & (t < half + lags[s]))
                def _():
                    step(d, s, t - lags[s])

            @pl.when(t >= lag)
            def _():
                finish(t - lag)

    loads[1].wait()
    loads[2].wait()
    first_exchange(0, local_pair, 3)
    loads[4].start()
    loads[5].start()

    tiles = [(i, j) for i in range(nb) for j in range(i + 1)]
    sub = block // dim

    def span_of(i):
        return slice(i * block, (i + 1) * block)

    def decayed(s, h, i, j):
        row = rows[pl.ds(h, 1), j * block : (j + 1) * block]

        def parted(x, t, lo, hi):
            m = cols[h, j * block + hi - 1 : j * block + hi, :]
            width = (hi - lo) // dim
            right = jnp.exp2(jnp.concatenate([m] * width, axis=1) - row[:, lo:hi])
            left = jnp.exp2(cols[h, t : t + x.shape[0], :] - m)
            return (x * right) * jnp.concatenate([left] * width, axis=1)

        if i != j:
            return parted(s, i * block, 0, block).astype(BF16)
        lines = []
        for a in range(sub):
            t = slice(a * dim, (a + 1) * dim)
            line = []
            if a:
                for b in range(a):
                    line.append(
                        parted(s[t, b * dim : (b + 1) * dim], i * block + a * dim, b * dim, (b + 1) * dim)
                    )
            gap = cols[h, i * block + a * dim : i * block + (a + 1) * dim, :] - row[:, t]
            line.append(s[t, t] * jnp.exp2(gap + bias[...]))
            if a + 1 < sub:
                line.append(jnp.zeros((dim, (sub - 1 - a) * dim), F32))
            lines.append(jnp.concatenate([x.astype(BF16) for x in line], axis=1))
        return jnp.concatenate(lines, axis=0)

    def before_norm(h, i):
        r = span_of(i)
        grow = jnp.exp2(cols[h, r, :])
        grown[r, lane(h)] = (q[r, lane(h)].astype(F32) * grow).astype(BF16)
        s = jax.nn.sigmoid(gate[r, lane(h)].astype(F32))
        sig[h, r, :] = s
        dnorm[h, r, :] = up[r, lane(h)].astype(F32) * s

    def intra_pair(c):
        work = [(h, i, j) for h in (mine(c), others(c)) for i, j in tiles]

        def scores(h, i, j):
            return nt(q[span_of(i), lane(h)], k[span_of(j), lane(h)])

        ahead = scores(*work[0])
        total = None
        for n, (h, i, j) in enumerate(work):
            s = ahead
            if n + 1 < len(work):
                ahead = scores(*work[n + 1])
            p = decayed(s, h, i, j)
            probs[h, tiles.index((i, j))] = p
            o = nn(p, v[span_of(j), lane(h)])
            total = o if j == 0 else total + o
            if i == j:
                inside[h, span_of(i), :] = total
                before_norm(h, i)

    def finish_attn(c):
        put(0, c, state)
        for i in range(nb):
            r = span_of(i)
            square, inner = scale_ref[r, :], center_ref[r, :]
            for h in (mine(c), others(c)):
                a = inside[h, r, :] + nn(grown[r, lane(h)], state[h])
                attn[h, r, :] = a
                square = square + a * a
                inner = inner + dnorm[h, r, :] * a
            scale_ref[r, :] = square
            center_ref[r, :] = inner

    scale_ref[...] = jnp.zeros_like(scale_ref)
    center_ref[...] = jnp.zeros_like(center_ref)
    loads[3].wait()
    loads[4].wait()
    loads[5].wait()
    ticks(0, intra_pair, 0, finish_attn)

    strips = tokens // 128

    def packed(x):
        turned = jnp.sum(x.T, axis=0, keepdims=True)
        return [turned[:, n * 128 : (n + 1) * 128] for n in range(strips)]

    spare = -2 * strips % 8
    pieces = packed(scale_ref[...]) + packed(center_ref[...])
    if spare:
        pieces.append(jnp.zeros((spare, 128), F32))
    sums[...] = jnp.concatenate(pieces, axis=0)

    def tp_copy(d):
        return pltpu.make_async_remote_copy(
            src_ref=sums, dst_ref=sums_in.at[d - 1], send_sem=tp_send.at[d - 1],
            recv_sem=tp_recv.at[d - 1], device_id=(me, lax.rem(z + d, n_tp)), device_id_type=MESH,
        )

    for d in range(1, n_tp):
        tp_copy(d).start()
    total = sums[...]
    for d in range(1, n_tp):
        tp_copy(d).wait_recv()
        total = total + sums_in[d - 1]
    scale = lax.rsqrt(total[0:strips] / width + 1e-06)
    center = total[strips : 2 * strips] * scale / width
    for n in range(strips):
        r = slice(n * 128, (n + 1) * 128)
        scale_ref[r, :] = jnp.broadcast_to(scale[n : n + 1, :], (128, 128)).T
        center_ref[r, :] = jnp.broadcast_to(center[n : n + 1, :], (128, 128)).T

    def pointwise(h):
        weighted = None
        for i in range(nb):
            r = span_of(i)
            sc = scale_ref[r, :]
            s, d = sig[h, r, :], dnorm[h, r, :]
            normed = attn[h, r, :] * sc
            g = (sc * (d - normed * center_ref[r, :])).astype(BF16)
            grad[r, lane(h)] = g
            up[r, lane(h)] = (normed * s).astype(BF16)
            gate[r, lane(h)] = (d * normed * (1.0 - s)).astype(BF16)
            w = tn(grown[r, lane(h)], g)
            weighted = w if weighted is None else weighted + w
        own[1, h] = weighted

    def pointwise_pair(c):
        pair = (others(c), mine(c))
        for h in pair:
            pointwise(h)
        for h in pair:
            s0_copy(1, h).start()

    first_exchange(1, pointwise_pair, 3)

    def backward_pair(c):
        pair = (mine(c), others(c))
        work = [(e, i, j) for e in (0, 1) for i, j in tiles]

        def scores(e, i, j):
            return nt(grad[span_of(i), lane(pair[e])], v[span_of(j), lane(pair[e])])

        def add(parts, n, x):
            parts[n] = x if n not in parts else parts[n] + x

        ahead = scores(*work[0])
        dq, dk, dv = {}, {}, {}
        for n, (e, i, j) in enumerate(work):
            h = pair[e]
            s = ahead
            if n + 1 < len(work):
                ahead = scores(*work[n + 1])
            r = span_of(i)
            add(dv, (e, j), tn(grad[r, lane(h)], probs[h, tiles.index((i, j))]))
            pg = decayed(s, h, i, j)
            add(dk, (e, j), tn(q[r, lane(h)], pg))
            add(dq, (e, i), nn(pg, k[span_of(j), lane(h)]))
            if i == j:
                carried = jnp.exp2(cols[h, r, :]) * nt(grad[r, lane(h)], state[h])
                grown[r, lane(h)] = (dq[e, i] + carried).astype(BF16)
            if i == nb - 1:
                dkt[h, :, span_of(j)] = dk[e, j]
                dvt[h, :, span_of(j)] = dv[e, j]

    ticks(1, backward_pair, 1, lambda c: put(1, c, state_grad))

    for b in range(bits):
        sp_copy(b).wait_send()
    for d in (0, 1):
        for b in (0, 1):
            part = pl.ds(b * half, half)
            pltpu.make_async_remote_copy(
                src_ref=own.at[d, part], dst_ref=other.at[d, part], send_sem=s0_send.at[d],
                recv_sem=s0_recv.at[d, 0], device_id=partner(0), device_id_type=MESH,
            ).wait_send()

        def all_sent(s):
            pltpu.make_async_remote_copy(
                src_ref=sent.at[d, s], dst_ref=got.at[d, s], send_sem=st_send.at[d, s],
                recv_sem=st_recv.at[d, s, 0], device_id=partner(s + 1), device_id_type=MESH,
            ).wait_send()

        for s in range(chips - 1):
            all_sent(s)
        pl.when(takes(d, chips) == 0)(lambda: all_sent(chips - 1))
        pltpu.make_async_remote_copy(
            src_ref=edge.at[d], dst_ref=far.at[d], send_sem=fin_send.at[d],
            recv_sem=fin_recv.at[d, 0], device_id=partner(0), device_id_type=MESH,
        ).wait_send()

    for d in range(1, n_tp):
        tp_copy(d).wait_send()


def last_kernel(
    heads, dim, tokens,
    out_ref, gg_ref, dq_ref, k, v, dkt, dvt, state_grad, rows,
    out_hbm, dq_hbm, dk_hbm, dv_hbm, gg_hbm,
    dk, dv, sem, pair_sem,
):
    block = min(256, tokens)
    trips = heads // 2
    whole = [
        pltpu.make_async_copy(a, b, sem.at[i])
        for i, (a, b) in enumerate(((out_ref, out_hbm), (gg_ref, gg_hbm), (dq_ref, dq_hbm)))
    ]
    for c in whole:
        c.start()

    def strips(i):
        part = pl.ds(pl.multiple_of(i * 2 * dim, 2 * dim), 2 * dim)
        return [
            pltpu.make_async_copy(a.at[:, part], b.at[:, part], pair_sem.at[n])
            for n, (a, b) in enumerate(((dk, dk_hbm), (dv, dv_hbm)))
        ]

    @pl.loop(0, trips)
    def _(i):
        for h in (2 * i, 2 * i + 1):
            at = pl.ds(pl.multiple_of(h * dim, dim), dim)
            row = rows[pl.ds(h, 1), :]
            tail = jnp.exp2(row[:, tokens - 1 : tokens] - row)
            turned = state_grad[h].astype(F32).T.astype(BF16)
            for n in range(tokens // block):
                r = slice(n * block, (n + 1) * block)
                key = dkt[h, :, r] + tail[:, r] * nt(state_grad[h], v[r, at])
                value = dvt[h, :, r] + tail[:, r] * nt(turned, k[r, at])
                dk[r, at] = key.astype(BF16).T
                dv[r, at] = value.astype(BF16).T
        for c in strips(i):
            c.start()

    for n, (a, b) in enumerate(((dk, dk_hbm), (dv, dv_hbm))):
        pltpu.make_async_copy(a, b, pair_sem.at[n]).wait()
    for c in whole:
        c.wait()


def solution(mesh):
    n_seq, n_tp = mesh.shape["seq"], mesh.shape["tp"]

    def shards(queries, keys, values, gate, log_decay, out_grad):
        tokens, flat = queries.shape
        heads = log_decay.shape[1]
        dim = flat // heads
        half = heads // 2
        bits = n_seq.bit_length() - 1
        chips = bits - 1
        block = min(256, tokens)
        nb = tokens // block
        tile = (dim, dim)
        dma = pltpu.SemaphoreType.DMA
        peers = max(n_tp - 1, 1)
        sums = (-(-2 * (tokens // 128) // 8) * 8, 128)
        hbm = pl.BlockSpec(memory_space=pltpu.HBM)
        vmem = pl.BlockSpec(memory_space=pltpu.VMEM)
        big = pltpu.VMEM((tokens, flat), BF16)
        wide = pltpu.VMEM((heads, tokens, dim), F32)
        turned = pltpu.VMEM((heads, dim, tokens), F32)
        flops = 2 * tokens * tokens * flat * 5 + 2 * tokens * flat * dim * 7
        results = pl.pallas_call(
            functools.partial(kernel, n_seq, n_tp, heads, dim, tokens),
            out_shape=[
                big, big, big, big, big, turned, turned,
                pltpu.VMEM((heads, *tile), BF16), pltpu.VMEM((heads, tokens), F32),
            ],
            in_specs=[hbm] * 6,
            out_specs=[vmem] * 9,
            scratch_shapes=[
                pltpu.VMEM((heads, tokens), F32), big, wide, pltpu.VMEM((tokens, 128), BF16),
                pltpu.VMEM(tile, F32), wide, wide, wide, wide, big,
                pltpu.VMEM((heads, nb * (nb + 1) // 2, block, block), BF16),
                pltpu.VMEM((2, heads, *tile), F32),
                pltpu.VMEM((2, heads, *tile), F32),
                pltpu.VMEM((2, chips, half, *tile), F32),
                pltpu.VMEM((2, chips, half, *tile), F32),
                pltpu.VMEM((2, half, *tile), F32),
                pltpu.VMEM((2, half, *tile), F32),
                pltpu.VMEM((heads, *tile), BF16),
                pltpu.VMEM((bits, heads, dim), F32), pltpu.VMEM((bits, heads, dim), F32),
                pltpu.VMEM((2, bits, 3, heads, dim), F32),
                pltpu.VMEM(sums, F32), pltpu.VMEM((peers, *sums), F32),
                pltpu.VMEM((tokens, dim), F32), pltpu.VMEM((tokens, dim), F32),
                dma((6,)), dma((bits,)), dma((bits,)), dma((2,)), dma((2, heads)),
                dma((2, chips)), dma((2, chips, half)), dma((2,)), dma((2, half)),
                dma((peers,)), dma((peers,)),
            ],
            compiler_params=pltpu.CompilerParams(
                collective_id=0, has_side_effects=True, vmem_limit_bytes=43 << 20
            ),
            cost_estimate=pl.CostEstimate(
                flops=flops, bytes_accessed=tokens * flat * 10, transcendentals=0
            ),
        )(queries, keys, values, gate, log_decay.T, out_grad)
        return tuple(
            pl.pallas_call(
                functools.partial(last_kernel, heads, dim, tokens),
                out_shape=[jax.ShapeDtypeStruct((tokens, flat), BF16)] * 5,
                in_specs=[vmem] * 9,
                out_specs=[hbm] * 5,
                scratch_shapes=[big, big, dma((3,)), dma((2,))],
                compiler_params=pltpu.CompilerParams(vmem_limit_bytes=16 << 20),
                cost_estimate=pl.CostEstimate(
                    flops=4 * tokens * flat * dim, bytes_accessed=tokens * flat * 10, transcendentals=0
                ),
            )(*results)
        )

    spec = P("seq", "tp")
    return jax.shard_map(
        shards, mesh=mesh, in_specs=(spec,) * 6, out_specs=(spec,) * 5, check_vma=False
    )
```

```python
import functools

import jax
import jax.numpy as jnp
from jax import lax
from jax.experimental import pallas as pl
from jax.experimental.pallas import tpu as pltpu
from jax.sharding import PartitionSpec as P

MESH = pl.DeviceIdType.MESH
F32 = jnp.float32
BF16 = jnp.bfloat16
LOG2E = 1.4426950408889634
LOW = -1e9


def nt(a, b):
    return lax.dot_general(a, b, (((1,), (1,)), ((), ())), preferred_element_type=F32)


def tn(a, b):
    return lax.dot_general(a, b, (((0,), (0,)), ((), ())), preferred_element_type=F32)


def nn(a, b):
    return lax.dot_general(a, b, (((1,), (0,)), ((), ())), preferred_element_type=F32)


def three_parts(x):
    high = x.astype(BF16).astype(F32)
    rest = x - high
    middle = rest.astype(BF16).astype(F32)
    low = (rest - middle).astype(BF16).astype(F32)
    return high, middle, low


def stacked(x):
    parts = three_parts(x)
    spare = 128 - 3 * x.shape[0]
    return jnp.concatenate([*parts, jnp.zeros((spare, x.shape[1]), F32)], axis=0)


def kernel(
    n_seq, n_tp, heads, dim, tokens,
    q_hbm, k_hbm, v_hbm, gate_hbm, rate_hbm, up_hbm,
    up, gate, grown, k, v, dkt, dvt, state_grad, rows,
    rate, q, cols, split, bias, inside, attn, sig, dnorm, grad, probs,
    own, other, sent, got, edge, far, state, span, span_in, factor,
    sums, sums_in, scale_ref, center_ref,
    in_sem, sp_send, sp_recv, s0_send, s0_recv, st_send, st_recv, fin_send, fin_recv, tp_send, tp_recv,
):
    width = heads * dim * n_tp
    half = heads // 2
    bits = n_seq.bit_length() - 1
    chips = bits - 1
    block = min(256, tokens)
    nb = tokens // block
    me = lax.axis_index("seq")
    z = lax.axis_index("tp")
    core = lax.rem(me, 2)

    def bit_of(b):
        return lax.rem(me // (1 << b), 2)

    def partner(b):
        return (me + (1 << b) * (1 - 2 * bit_of(b)), z)

    def takes(d, b):
        return bit_of(b) if d == 0 else 1 - bit_of(b)

    def load(i, a, b):
        return pltpu.make_async_copy(a, b, in_sem.at[i])

    rate_load = load(0, rate_hbm, rate)
    q_load, up_load, gate_load = (
        load(1 + i, a, b) for i, (a, b) in enumerate(((q_hbm, q), (up_hbm, up), (gate_hbm, gate)))
    )
    soon = min(2, half)

    def kv_loads(lo, hi, at):
        out = []
        for start in (lo, half + lo):
            part = slice(start * dim, (start + hi - lo) * dim)
            for a, b in ((k_hbm, k), (v_hbm, v)):
                out.append(load(4 + at + len(out), a.at[:, part], b.at[:, part]))
        return out

    first_loads = kv_loads(0, soon, 0)
    more_loads = kv_loads(soon, half, 4) if soon < half else []
    rate_load.start()
    for c in first_loads + more_loads:
        c.start()

    barrier = pltpu.get_barrier_semaphore()
    for b in range(bits):
        pl.semaphore_signal(barrier, inc=1, device_id=partner(b), device_id_type=MESH)
    for d in range(1, n_tp):
        pl.semaphore_signal(
            barrier, inc=1, device_id=(me, lax.rem(z + d, n_tp)), device_id_type=MESH
        )

    def lane(h):
        return pl.ds(pl.multiple_of(h * dim, dim), dim)

    def mine(c):
        return core * half + c

    def others(c):
        return (1 - core) * half + c

    rate_load.wait()
    upto = (
        lax.broadcasted_iota(jnp.int32, (tokens, tokens), 0)
        <= lax.broadcasted_iota(jnp.int32, (tokens, tokens), 1)
    ).astype(BF16)
    parts = nn(stacked(rate[...]).astype(BF16), upto)
    across = parts[0:heads] + parts[heads : 2 * heads] + parts[2 * heads : 3 * heads]
    across = across * LOG2E
    rows[...] = across
    split[...] = stacked(across).T.astype(BF16)
    span[0] = jnp.broadcast_to(across[:, tokens - 1 : tokens], (heads, dim))
    q_load.start()
    corner = lax.broadcasted_iota(jnp.int32, (dim, dim), 0) >= lax.broadcasted_iota(
        jnp.int32, (dim, dim), 1
    )
    bias[...] = jnp.where(corner, 0.0, LOW)

    def cols_pair(c):
        pair = (mine(c), others(c))
        at = lax.broadcasted_iota(jnp.int32, (128, dim), 0)
        pick = jnp.concatenate(
            [
                ((at == h) | (at == h + heads) | (at == h + 2 * heads)).astype(F32).astype(BF16)
                for h in pair
            ],
            axis=1,
        )
        for r in (slice(n, n + 256) for n in range(0, tokens, 256)):
            wide = nn(split[r, :], pick)
            for n, h in enumerate(pair):
                cols[h, r, :] = wide[:, n * dim : (n + 1) * dim]

    crossed = chips == 2 and half % 2 == 0

    def sp_copy(b):
        return pltpu.make_async_remote_copy(
            src_ref=span.at[b], dst_ref=span_in.at[b], send_sem=sp_send.at[b],
            recv_sem=sp_recv.at[b], device_id=partner(b), device_id_type=MESH,
        )

    def aside_copy():
        return pltpu.make_async_remote_copy(
            src_ref=span_in.at[1], dst_ref=span_in.at[bits], send_sem=sp_send.at[bits],
            recv_sem=sp_recv.at[bits], device_id=partner(2), device_id_type=MESH,
        )

    def s0_copy(d, h):
        return pltpu.make_async_remote_copy(
            src_ref=own.at[d, h], dst_ref=other.at[d, h], send_sem=s0_send.at[d],
            recv_sem=s0_recv.at[d, h], device_id=partner(0), device_id_type=MESH,
        )

    def st_copy(d, s, c):
        return pltpu.make_async_remote_copy(
            src_ref=sent.at[d, s, c], dst_ref=got.at[d, s, c], send_sem=st_send.at[d, s],
            recv_sem=st_recv.at[d, s, c], device_id=partner(s + 1), device_id_type=MESH,
        )

    def fin_copy(d, c):
        return pltpu.make_async_remote_copy(
            src_ref=edge.at[d, c], dst_ref=far.at[d, c], send_sem=fin_send.at[d],
            recv_sem=fin_recv.at[d, c], device_id=partner(0), device_id_type=MESH,
        )

    def span_step(b):
        sp_copy(b).wait_recv()
        here, there = span[b], span_in[b]
        if b + 1 < bits:
            span[b + 1] = here + there
            sp_copy(b + 1).start()
        if crossed and b == 1:
            aside_copy().start()
        if crossed and b == 2:
            aside_copy().wait_recv()
            aside = span_in[bits]
            for d in (0, 1):
                f = takes(d, 1).astype(F32)
                factor[d, bits, 0] = jnp.exp2(aside + span[1])
                factor[d, bits, 1] = jnp.exp2(f * span_in[1] + (1.0 - f) * aside)
        for d in (0, 1):
            f = takes(d, b).astype(F32)
            factor[d, b, 0] = jnp.exp2(there * (1.0 - f))
            factor[d, b, 1] = jnp.exp2(here * f)
            if b == 0:
                factor[d, b, 2] = jnp.exp2(there * f)
            else:
                before = jnp.zeros((heads, dim), F32)
                for r in range(1, b):
                    before = before + takes(d, r).astype(F32) * span_in[r]
                factor[d, b, 2] = f * jnp.exp2(before)

    def row_of(d, b, n, h):
        return factor[d, b, n, pl.ds(h, 1), :]

    def send_level(d, s, c):
        if s == chips - 1:

            @pl.when(takes(d, s + 1) == 0)
            def _():
                st_copy(d, s, c).start()
        else:
            st_copy(d, s, c).start()

    def level0(d, c, crosses):
        h = mine(c)
        s0_copy(d, h).wait_recv()
        total = row_of(d, 0, 0, h) * own[d, h] + row_of(d, 0, 1, h) * other[d, h]
        if not crossed:
            sent[d, 0, c] = total
            send_level(d, 0, c)
        elif crosses:
            sent[d, 1, c] = total

            @pl.when(takes(d, 2) == 0)
            def _():
                st_copy(d, 1, c).start()
        else:
            sent[d, 0, c] = total

            @pl.when((takes(d, 1) == 0) | (takes(d, 2) == 0))
            def _():
                st_copy(d, 0, c).start()

    def even_first(d, c):
        h = mine(c)
        fx, fy = takes(d, 1), takes(d, 2)

        @pl.when((fx == 1) | (fy == 0))
        def _():
            st_copy(d, 0, c).wait_recv()
            theirs = got[d, 0, c]
            edge[d, c] = fx.astype(F32) * theirs

            @pl.when(fy == 0)
            def _():
                sent[d, 1, c] = row_of(d, 1, 0, h) * sent[d, 0, c] + row_of(d, 1, 1, h) * theirs
                st_copy(d, 1, c).start()

        @pl.when((fx == 0) & (fy == 1))
        def _():
            edge[d, c] = jnp.zeros((dim, dim), F32)

    def even_second(d, c):
        @pl.when(takes(d, 2) == 1)
        def _():
            st_copy(d, 1, c).wait_recv()
            edge[d, c] = edge[d, c] + row_of(d, 2, 2, mine(c)) * got[d, 1, c]

        fin_copy(d, c).start()

    def odd_first(d, c):
        fx, fy = takes(d, 1), takes(d, 2)

        @pl.when(fy == 1)
        def _():
            st_copy(d, 1, c).wait_recv()

        @pl.when((fx == 0) & (fy == 1))
        def _():
            sent[d, 0, c] = row_of(d, bits, 0, mine(c)) * got[d, 1, c] + sent[d, 1, c]

        @pl.when((fx == 1) & (fy == 1))
        def _():
            sent[d, 0, c] = got[d, 1, c]

        @pl.when((fx == 0) & (fy == 0))
        def _():
            sent[d, 0, c] = sent[d, 1, c]

        @pl.when((fx == 0) | (fy == 1))
        def _():
            st_copy(d, 0, c).start()

    def odd_second(d, c):
        fx, fy = takes(d, 1), takes(d, 2)

        @pl.when((fx == 1) | (fy == 1))
        def _():
            st_copy(d, 0, c).wait_recv()

        @pl.when(fy == 1)
        def _():
            edge[d, c] = got[d, 0, c] + row_of(d, bits, 1, mine(c)) * got[d, 1, c]

        @pl.when((fx == 1) & (fy == 0))
        def _():
            edge[d, c] = got[d, 0, c]

        @pl.when((fx == 0) & (fy == 0))
        def _():
            edge[d, c] = jnp.zeros((dim, dim), F32)

        fin_copy(d, c).start()

    def step(d, s, c):
        h = mine(c)

        def arrive():
            st_copy(d, s, c).wait_recv()
            theirs = got[d, s, c]
            on_top = row_of(d, s + 1, 2, h) * theirs
            edge[d, c] = on_top if s == 0 else edge[d, c] + on_top
            if s + 1 < chips:
                sent[d, s + 1, c] = (
                    row_of(d, s + 1, 0, h) * sent[d, s, c] + row_of(d, s + 1, 1, h) * theirs
                )

        if s + 1 < chips:
            arrive()
            send_level(d, s + 1, c)
            return
        pl.when(takes(d, s + 1) == 1)(arrive)
        if s == 0:

            @pl.when(takes(d, s + 1) == 0)
            def _():
                edge[d, c] = jnp.zeros((dim, dim), F32)

        fin_copy(d, c).start()

    def put(d, c, target):
        f = takes(d, 0).astype(F32)
        h = mine(c)
        target[h] = (row_of(d, 0, 2, h) * edge[d, c] + f * other[d, h]).astype(BF16)
        h = others(c)
        s0_copy(d, h).wait_recv()
        fin_copy(d, c).wait_recv()
        target[h] = (row_of(d, 0, 2, h) * far[d, c] + f * other[d, h]).astype(BF16)

    def local_pair(c):
        pair = (others(c), mine(c))
        scaled = []
        for h in pair:
            last = cols[h, tokens - 1 : tokens, :]
            scaled.append((k[:, lane(h)].astype(F32) * jnp.exp2(last - cols[h])).astype(BF16))
        for h, x in zip(pair, scaled):
            own[0, h] = tn(x, v[:, lane(h)])

    def local_and_next(c):
        local_pair(c)
        cols_pair(c + 1 - (c + 1) // half)

    def s0_start(d, c):
        for h in (others(c), mine(c)):
            s0_copy(d, h).start()

    def levels0(d, lo, hi, lag, body):
        count = 2 if crossed else 1

        @pl.loop(0, (hi - lo) // count)
        def _(n):
            for e in range(count):
                c = lo + n * count + e
                body(c)
                level0(d, c - lag, (e + lo - lag) % 2 == 1)

    def first_exchange(d, body, done):
        lead = min(2, half)

        @pl.loop(done, lead)
        def _(c):
            body(c)
            s0_start(d, c)

        if d == 0:
            span_step(0)

        def more(c):
            body(c)
            s0_start(d, c)

        levels0(d, lead, half, lead, more)
        if d == 0:
            span_step(1)
        levels0(d, half, half + lead, lead, lambda c: None)

    def ticks(d, body, finish):
        if crossed:
            trips = half // 2

            def first(m):
                even_first(d, 2 * m)
                odd_first(d, 2 * m + 1)

            def second(m):
                even_second(d, 2 * m)
                odd_second(d, 2 * m + 1)

            def third(m):
                finish(2 * m)
                finish(2 * m + 1)

            stages = [(0, first), (trips, second), (trips + 1, third)]
        else:
            trips = half
            stages = [(2 * s, functools.partial(step, d, s)) for s in range(chips)]
            stages.append((2 * chips - 1, finish))

        @pl.loop(0, max(half, trips + stages[-1][0]))
        def _(t):
            @pl.when(t < half)
            def _():
                body(t)

            for n, (lag, stage) in enumerate(stages):
                if d == 0 and 1 <= n + 1 < bits and n >= 1 and not crossed:

                    @pl.when(t == lag)
                    def _():
                        span_step(n + 1)

                if d == 0 and crossed and n == 0:

                    @pl.when(t == 0)
                    def _():
                        span_step(2)

                @pl.when((t >= lag) & (t < trips + lag))
                def _():
                    stage(t - lag)

    cols_pair(0)
    for c in first_loads:
        c.wait()
    local_and_next(0)
    pl.semaphore_wait(barrier, bits + n_tp - 1)
    sp_copy(0).start()
    s0_start(0, 0)
    for c in more_loads:
        c.wait()
    up_load.start()
    gate_load.start()
    first_exchange(0, local_and_next, 1)

    tiles = [(i, j) for i in range(nb) for j in range(i + 1)]
    sub = block // dim

    def span_of(i):
        return slice(i * block, (i + 1) * block)

    def decayed(s, h, i, j):
        row = rows[pl.ds(h, 1), j * block : (j + 1) * block]

        def parted(x, t, lo, hi):
            m = cols[h, j * block + hi - 1 : j * block + hi, :]
            width = (hi - lo) // dim
            right = jnp.exp2(jnp.concatenate([m] * width, axis=1) - row[:, lo:hi])
            left = jnp.exp2(cols[h, t : t + x.shape[0], :] - m)
            return (x * right) * jnp.concatenate([left] * width, axis=1)

        if i != j:
            return parted(s, i * block, 0, block).astype(BF16)
        lines = []
        for a in range(sub):
            t = slice(a * dim, (a + 1) * dim)
            line = []
            if a:
                for b in range(a):
                    line.append(
                        parted(s[t, b * dim : (b + 1) * dim], i * block + a * dim, b * dim, (b + 1) * dim)
                    )
            gap = cols[h, i * block + a * dim : i * block + (a + 1) * dim, :] - row[:, t]
            line.append(s[t, t] * jnp.exp2(gap + bias[...]))
            if a + 1 < sub:
                line.append(jnp.zeros((dim, (sub - 1 - a) * dim), F32))
            lines.append(jnp.concatenate([x.astype(BF16) for x in line], axis=1))
        return jnp.concatenate(lines, axis=0)

    def before_norm(h, i):
        r = span_of(i)
        grow = jnp.exp2(cols[h, r, :])
        grown[r, lane(h)] = (q[r, lane(h)].astype(F32) * grow).astype(BF16)
        s = jax.nn.sigmoid(gate[r, lane(h)].astype(F32))
        sig[h, r, :] = s
        dnorm[h, r, :] = up[r, lane(h)].astype(F32) * s

    def intra_pair(c):
        work = [(h, i, j) for h in (mine(c), others(c)) for i, j in tiles]

        def scores(h, i, j):
            return nt(q[span_of(i), lane(h)], k[span_of(j), lane(h)])

        ahead = scores(*work[0])
        total = None
        for n, (h, i, j) in enumerate(work):
            s = ahead
            if n + 1 < len(work):
                ahead = scores(*work[n + 1])
            p = decayed(s, h, i, j)
            probs[h, tiles.index((i, j))] = p
            o = nn(p, v[span_of(j), lane(h)])
            total = o if j == 0 else total + o
            if i == j:
                inside[h, span_of(i), :] = total
                before_norm(h, i)

    def finish_attn(c):
        put(0, c, state)
        for i in range(nb):
            r = span_of(i)
            square, inner = scale_ref[r, :], center_ref[r, :]
            for h in (mine(c), others(c)):
                a = inside[h, r, :] + nn(grown[r, lane(h)], state[h])
                attn[h, r, :] = a
                square = square + a * a
                inner = inner + dnorm[h, r, :] * a
            scale_ref[r, :] = square
            center_ref[r, :] = inner

    scale_ref[...] = jnp.zeros_like(scale_ref)
    center_ref[...] = jnp.zeros_like(center_ref)
    q_load.wait()
    up_load.wait()
    gate_load.wait()
    ticks(0, intra_pair, finish_attn)

    strips = tokens // 128

    def packed(x):
        turned = jnp.sum(x.T, axis=0, keepdims=True)
        return [turned[:, n * 128 : (n + 1) * 128] for n in range(strips)]

    spare = -2 * strips % 8
    pieces = packed(scale_ref[...]) + packed(center_ref[...])
    if spare:
        pieces.append(jnp.zeros((spare, 128), F32))
    sums[...] = jnp.concatenate(pieces, axis=0)

    def tp_copy(d):
        return pltpu.make_async_remote_copy(
            src_ref=sums, dst_ref=sums_in.at[d - 1], send_sem=tp_send.at[d - 1],
            recv_sem=tp_recv.at[d - 1], device_id=(me, lax.rem(z + d, n_tp)), device_id_type=MESH,
        )

    for d in range(1, n_tp):
        tp_copy(d).start()
    total = sums[...]
    for d in range(1, n_tp):
        tp_copy(d).wait_recv()
        total = total + sums_in[d - 1]
    scale = lax.rsqrt(total[0:strips] / width + 1e-06)
    center = total[strips : 2 * strips] * scale / width
    for n in range(strips):
        r = slice(n * 128, (n + 1) * 128)
        scale_ref[r, :] = jnp.broadcast_to(scale[n : n + 1, :], (128, 128)).T
        center_ref[r, :] = jnp.broadcast_to(center[n : n + 1, :], (128, 128)).T

    def pointwise(h):
        weighted = None
        for i in range(nb):
            r = span_of(i)
            sc = scale_ref[r, :]
            s, d = sig[h, r, :], dnorm[h, r, :]
            normed = attn[h, r, :] * sc
            g = (sc * (d - normed * center_ref[r, :])).astype(BF16)
            grad[r, lane(h)] = g
            up[r, lane(h)] = (normed * s).astype(BF16)
            gate[r, lane(h)] = (d * normed * (1.0 - s)).astype(BF16)
            w = tn(grown[r, lane(h)], g)
            weighted = w if weighted is None else weighted + w
        own[1, h] = weighted

    def pointwise_pair(c):
        pair = (others(c), mine(c))
        for h in pair:
            pointwise(h)

    first_exchange(1, pointwise_pair, 0)

    def backward_pair(c):
        pair = (mine(c), others(c))
        work = [(e, i, j) for e in (0, 1) for i, j in tiles]

        def scores(e, i, j):
            return nt(grad[span_of(i), lane(pair[e])], v[span_of(j), lane(pair[e])])

        def add(parts, n, x):
            parts[n] = x if n not in parts else parts[n] + x

        ahead = scores(*work[0])
        dq, dk, dv = {}, {}, {}
        for n, (e, i, j) in enumerate(work):
            h = pair[e]
            s = ahead
            if n + 1 < len(work):
                ahead = scores(*work[n + 1])
            r = span_of(i)
            add(dv, (e, j), tn(grad[r, lane(h)], probs[h, tiles.index((i, j))]))
            pg = decayed(s, h, i, j)
            add(dk, (e, j), tn(q[r, lane(h)], pg))
            add(dq, (e, i), nn(pg, k[span_of(j), lane(h)]))
            if i == j:
                carried = jnp.exp2(cols[h, r, :]) * nt(grad[r, lane(h)], state[h])
                grown[r, lane(h)] = (dq[e, i] + carried).astype(BF16)
            if i == nb - 1:
                dkt[h, :, span_of(j)] = dk[e, j]
                dvt[h, :, span_of(j)] = dv[e, j]

    ticks(1, backward_pair, lambda c: put(1, c, state_grad))

    for b in range(bits):
        sp_copy(b).wait_send()
    if crossed:
        aside_copy().wait_send()
    for d in (0, 1):
        for b in (0, 1):
            part = pl.ds(b * half, half)
            pltpu.make_async_remote_copy(
                src_ref=own.at[d, part], dst_ref=other.at[d, part], send_sem=s0_send.at[d],
                recv_sem=s0_recv.at[d, 0], device_id=partner(0), device_id_type=MESH,
            ).wait_send()

        def sent_all(s, count):
            part = pl.ds(0, count)
            pltpu.make_async_remote_copy(
                src_ref=sent.at[d, s, part], dst_ref=got.at[d, s, part], send_sem=st_send.at[d, s],
                recv_sem=st_recv.at[d, s, 0], device_id=partner(s + 1), device_id_type=MESH,
            ).wait_send()

        if crossed:
            pl.when(takes(d, 1) == 0)(lambda: sent_all(0, half))
            pl.when(takes(d, 1) == 1)(lambda: sent_all(0, half // 2))
        else:
            for s in range(chips - 1):
                sent_all(s, half)
        pl.when(takes(d, chips) == 0)(lambda: sent_all(chips - 1, half))
        pltpu.make_async_remote_copy(
            src_ref=edge.at[d], dst_ref=far.at[d], send_sem=fin_send.at[d],
            recv_sem=fin_recv.at[d, 0], device_id=partner(0), device_id_type=MESH,
        ).wait_send()

    for d in range(1, n_tp):
        tp_copy(d).wait_send()


def last_kernel(
    heads, dim, tokens,
    out_ref, gg_ref, dq_ref, k, v, dkt, dvt, state_grad, rows,
    out_hbm, dq_hbm, dk_hbm, dv_hbm, gg_hbm,
    dk, dv, sem, pair_sem,
):
    block = min(256, tokens)
    trips = heads // 2
    whole = [
        pltpu.make_async_copy(a, b, sem.at[i])
        for i, (a, b) in enumerate(((out_ref, out_hbm), (gg_ref, gg_hbm), (dq_ref, dq_hbm)))
    ]
    for c in whole:
        c.start()

    def strips(i):
        part = pl.ds(pl.multiple_of(i * 2 * dim, 2 * dim), 2 * dim)
        return [
            pltpu.make_async_copy(a.at[:, part], b.at[:, part], pair_sem.at[n])
            for n, (a, b) in enumerate(((dk, dk_hbm), (dv, dv_hbm)))
        ]

    @pl.loop(0, trips)
    def _(i):
        for h in (2 * i, 2 * i + 1):
            at = pl.ds(pl.multiple_of(h * dim, dim), dim)
            row = rows[pl.ds(h, 1), :]
            tail = jnp.exp2(row[:, tokens - 1 : tokens] - row)
            turned = state_grad[h].astype(F32).T.astype(BF16)
            for n in range(tokens // block):
                r = slice(n * block, (n + 1) * block)
                key = dkt[h, :, r] + tail[:, r] * nt(state_grad[h], v[r, at])
                value = dvt[h, :, r] + tail[:, r] * nt(turned, k[r, at])
                dk[r, at] = key.astype(BF16).T
                dv[r, at] = value.astype(BF16).T
        for c in strips(i):
            c.start()

    for n, (a, b) in enumerate(((dk, dk_hbm), (dv, dv_hbm))):
        pltpu.make_async_copy(a, b, pair_sem.at[n]).wait()
    for c in whole:
        c.wait()


def solution(mesh):
    n_seq, n_tp = mesh.shape["seq"], mesh.shape["tp"]

    def shards(queries, keys, values, gate, log_decay, out_grad):
        tokens, flat = queries.shape
        heads = log_decay.shape[1]
        dim = flat // heads
        half = heads // 2
        bits = n_seq.bit_length() - 1
        chips = bits - 1
        block = min(256, tokens)
        nb = tokens // block
        tile = (dim, dim)
        dma = pltpu.SemaphoreType.DMA
        peers = max(n_tp - 1, 1)
        sums = (-(-2 * (tokens // 128) // 8) * 8, 128)
        hbm = pl.BlockSpec(memory_space=pltpu.HBM)
        vmem = pl.BlockSpec(memory_space=pltpu.VMEM)
        big = pltpu.VMEM((tokens, flat), BF16)
        wide = pltpu.VMEM((heads, tokens, dim), F32)
        turned = pltpu.VMEM((heads, dim, tokens), F32)
        flops = 2 * tokens * tokens * flat * 5 + 2 * tokens * flat * dim * 7
        results = pl.pallas_call(
            functools.partial(kernel, n_seq, n_tp, heads, dim, tokens),
            out_shape=[
                big, big, big, big, big, turned, turned,
                pltpu.VMEM((heads, *tile), BF16), pltpu.VMEM((heads, tokens), F32),
            ],
            in_specs=[hbm] * 6,
            out_specs=[vmem] * 9,
            scratch_shapes=[
                pltpu.VMEM((heads, tokens), F32), big, wide, pltpu.VMEM((tokens, 128), BF16),
                pltpu.VMEM(tile, F32), wide, wide, wide, wide, big,
                pltpu.VMEM((heads, nb * (nb + 1) // 2, block, block), BF16),
                pltpu.VMEM((2, heads, *tile), F32),
                pltpu.VMEM((2, heads, *tile), F32),
                pltpu.VMEM((2, chips, half, *tile), F32),
                pltpu.VMEM((2, chips, half, *tile), F32),
                pltpu.VMEM((2, half, *tile), F32),
                pltpu.VMEM((2, half, *tile), F32),
                pltpu.VMEM((heads, *tile), BF16),
                pltpu.VMEM((bits, heads, dim), F32), pltpu.VMEM((bits + 1, heads, dim), F32),
                pltpu.VMEM((2, bits + 1, 3, heads, dim), F32),
                pltpu.VMEM(sums, F32), pltpu.VMEM((peers, *sums), F32),
                pltpu.VMEM((tokens, dim), F32), pltpu.VMEM((tokens, dim), F32),
                dma((12,)), dma((bits + 1,)), dma((bits + 1,)), dma((2,)), dma((2, heads)),
                dma((2, chips)), dma((2, chips, half)), dma((2,)), dma((2, half)),
                dma((peers,)), dma((peers,)),
            ],
            compiler_params=pltpu.CompilerParams(
                collective_id=0, has_side_effects=True, vmem_limit_bytes=43 << 20
            ),
            cost_estimate=pl.CostEstimate(
                flops=flops, bytes_accessed=tokens * flat * 10, transcendentals=0
            ),
        )(queries, keys, values, gate, log_decay.T, out_grad)
        return tuple(
            pl.pallas_call(
                functools.partial(last_kernel, heads, dim, tokens),
                out_shape=[jax.ShapeDtypeStruct((tokens, flat), BF16)] * 5,
                in_specs=[vmem] * 9,
                out_specs=[hbm] * 5,
                scratch_shapes=[big, big, dma((3,)), dma((2,))],
                compiler_params=pltpu.CompilerParams(vmem_limit_bytes=16 << 20),
                cost_estimate=pl.CostEstimate(
                    flops=4 * tokens * flat * dim, bytes_accessed=tokens * flat * 10, transcendentals=0
                ),
            )(*results)
        )

    spec = P("seq", "tp")
    return jax.shard_map(
        shards, mesh=mesh, in_specs=(spec,) * 6, out_specs=(spec,) * 5, check_vma=False
    )
```

```python
import functools

import jax
import jax.numpy as jnp
from jax import lax
from jax.experimental import pallas as pl
from jax.experimental.pallas import tpu as pltpu
from jax.sharding import PartitionSpec as P

MESH = pl.DeviceIdType.MESH
F32 = jnp.float32
BF16 = jnp.bfloat16
LOG2E = 1.4426950408889634
LOW = -1e9


def nt(a, b):
    return lax.dot_general(a, b, (((1,), (1,)), ((), ())), preferred_element_type=F32)


def tn(a, b):
    return lax.dot_general(a, b, (((0,), (0,)), ((), ())), preferred_element_type=F32)


def nn(a, b):
    return lax.dot_general(a, b, (((1,), (0,)), ((), ())), preferred_element_type=F32)


def t0(a, b):
    return lax.dot_general(a, b, (((0,), (1,)), ((), ())), preferred_element_type=F32)


def three_parts(x):
    high = x.astype(BF16).astype(F32)
    rest = x - high
    middle = rest.astype(BF16).astype(F32)
    low = (rest - middle).astype(BF16).astype(F32)
    return high, middle, low


def stacked(x):
    parts = three_parts(x)
    spare = 128 - 3 * x.shape[0]
    return jnp.concatenate([*parts, jnp.zeros((spare, x.shape[1]), F32)], axis=0)


def kernel(
    n_seq, n_tp, heads, dim, tokens,
    q_hbm, k_hbm, v_hbm, gate_hbm, rate_hbm, up_hbm,
    up, gate, grown, k, v, dkt, dvt, state_grad, rows,
    rate, q, cols, split, bias, inside, attn, sig, dnorm, grad, probs,
    own, other, sent, got, edge, far, state, span, span_in, factor,
    sums, sums_in, scale_ref, center_ref,
    in_sem, sp_send, sp_recv, s0_send, s0_recv, st_send, st_recv, fin_send, fin_recv, tp_send, tp_recv,
):
    width = heads * dim * n_tp
    half = heads // 2
    bits = n_seq.bit_length() - 1
    chips = bits - 1
    block = min(256, tokens)
    nb = tokens // block
    me = lax.axis_index("seq")
    z = lax.axis_index("tp")
    core = lax.rem(me, 2)

    def bit_of(b):
        return lax.rem(me // (1 << b), 2)

    def partner(b):
        return (me + (1 << b) * (1 - 2 * bit_of(b)), z)

    def takes(d, b):
        return bit_of(b) if d == 0 else 1 - bit_of(b)

    def load(i, a, b):
        return pltpu.make_async_copy(a, b, in_sem.at[i])

    rate_load = load(0, rate_hbm, rate)
    q_load, up_load, gate_load = (
        load(1 + i, a, b) for i, (a, b) in enumerate(((q_hbm, q), (up_hbm, up), (gate_hbm, gate)))
    )
    soon = min(2, half)

    def kv_loads(lo, hi, at):
        out = []
        for start in (lo, half + lo):
            part = slice(start * dim, (start + hi - lo) * dim)
            for a, b in ((k_hbm, k), (v_hbm, v)):
                out.append(load(4 + at + len(out), a.at[:, part], b.at[:, part]))
        return out

    first_loads = kv_loads(0, soon, 0)
    more_loads = kv_loads(soon, half, 4) if soon < half else []
    rate_load.start()
    for c in first_loads + more_loads:
        c.start()

    crossed = chips == 2 and half % 2 == 0
    barrier = pltpu.get_barrier_semaphore()
    if crossed:
        others_along = [(lax.rem(me + o, n_seq), z) for o in range(1, n_seq)]
    else:
        others_along = [partner(b) for b in range(bits)]
    for at in others_along:
        pl.semaphore_signal(barrier, inc=1, device_id=at, device_id_type=MESH)
    for d in range(1, n_tp):
        pl.semaphore_signal(
            barrier, inc=1, device_id=(me, lax.rem(z + d, n_tp)), device_id_type=MESH
        )

    def lane(h):
        return pl.ds(pl.multiple_of(h * dim, dim), dim)

    def mine(c):
        return core * half + c

    def others(c):
        return (1 - core) * half + c

    rate_load.wait()
    upto = (
        lax.broadcasted_iota(jnp.int32, (tokens, tokens), 0)
        <= lax.broadcasted_iota(jnp.int32, (tokens, tokens), 1)
    ).astype(BF16)
    parts = nn(stacked(rate[...]).astype(BF16), upto)
    across = parts[0:heads] + parts[heads : 2 * heads] + parts[2 * heads : 3 * heads]
    across = across * LOG2E
    rows[...] = across
    split[...] = stacked(across).T.astype(BF16)
    span[0] = jnp.broadcast_to(across[:, tokens - 1 : tokens], (heads, dim))
    q_load.start()
    corner = lax.broadcasted_iota(jnp.int32, (dim, dim), 0) >= lax.broadcasted_iota(
        jnp.int32, (dim, dim), 1
    )
    bias[...] = jnp.where(corner, 0.0, LOW)

    def cols_pair(c):
        pair = (mine(c), others(c))
        at = lax.broadcasted_iota(jnp.int32, (128, dim), 0)
        pick = jnp.concatenate(
            [
                ((at == h) | (at == h + heads) | (at == h + 2 * heads)).astype(F32).astype(BF16)
                for h in pair
            ],
            axis=1,
        )
        for r in (slice(n, n + 256) for n in range(0, tokens, 256)):
            wide = nn(split[r, :], pick)
            for n, h in enumerate(pair):
                cols[h, r, :] = wide[:, n * dim : (n + 1) * dim]

    def sp_copy(b):
        return pltpu.make_async_remote_copy(
            src_ref=span.at[b], dst_ref=span_in.at[b], send_sem=sp_send.at[b],
            recv_sem=sp_recv.at[b], device_id=partner(b), device_id_type=MESH,
        )

    def last_copy(o):
        return pltpu.make_async_remote_copy(
            src_ref=span.at[0], dst_ref=span_in.at[me], send_sem=sp_send.at[o],
            recv_sem=sp_recv.at[o], device_id=(lax.rem(me + o, n_seq), z), device_id_type=MESH,
        )

    def s0_copy(d, h):
        return pltpu.make_async_remote_copy(
            src_ref=own.at[d, h], dst_ref=other.at[d, h], send_sem=s0_send.at[d],
            recv_sem=s0_recv.at[d, h], device_id=partner(0), device_id_type=MESH,
        )

    def st_copy(d, s, c):
        return pltpu.make_async_remote_copy(
            src_ref=sent.at[d, s, c], dst_ref=got.at[d, s, c], send_sem=st_send.at[d, s],
            recv_sem=st_recv.at[d, s, c], device_id=partner(s + 1), device_id_type=MESH,
        )

    def fin_copy(d, c):
        return pltpu.make_async_remote_copy(
            src_ref=edge.at[d, c], dst_ref=far.at[d, c], send_sem=fin_send.at[d],
            recv_sem=fin_recv.at[d, c], device_id=partner(0), device_id_type=MESH,
        )

    def set_factors(b, here, there, before):
        for d in (0, 1):
            f = takes(d, b).astype(F32)
            factor[d, b, 0] = jnp.exp2(there * (1.0 - f))
            factor[d, b, 1] = jnp.exp2(here * f)
            factor[d, b, 2] = jnp.exp2(there * f) if b == 0 else f * jnp.exp2(before(d))

    def span_step(b):
        if crossed:
            return crossed_spans(b)
        sp_copy(b).wait_recv()
        here, there = span[b], span_in[b]
        if b + 1 < bits:
            span[b + 1] = here + there
            sp_copy(b + 1).start()

        def before(d):
            total = jnp.zeros((heads, dim), F32)
            for r in range(1, b):
                total = total + takes(d, r).astype(F32) * span_in[r]
            return total

        set_factors(b, here, there, before)

    def crossed_spans(b):
        if b == 0:
            o = 1 + (1 - core) * (n_seq - 2)
            last_copy(o).wait_recv()
            set_factors(0, span[0], span_in[partner(0)[0]], None)
            return
        for o in range(1, n_seq):
            if o == 1:
                pl.when(core == 0)(lambda: last_copy(1).wait_recv())
            elif o == n_seq - 1:
                pl.when(core == 1)(lambda: last_copy(n_seq - 1).wait_recv())
            else:
                last_copy(o).wait_recv()

        def chip(at):
            first = at - lax.rem(at, 2)
            return span_in[first] + span_in[first + 1]

        span_in[me] = span[0]
        mine_all, along_x, along_y = chip(me), chip(partner(1)[0]), chip(partner(2)[0])
        aside = chip(partner(1)[0] + partner(2)[0] - me)
        set_factors(1, mine_all, along_x, lambda d: jnp.zeros((heads, dim), F32))
        set_factors(
            2, mine_all + along_x, along_y + aside, lambda d: takes(d, 1).astype(F32) * along_x
        )
        for d in (0, 1):
            f = takes(d, 1).astype(F32)
            factor[d, bits, 0] = jnp.exp2(aside + mine_all)
            factor[d, bits, 1] = jnp.exp2(f * along_x + (1.0 - f) * aside)

    def row_of(d, b, n, h):
        return factor[d, b, n, pl.ds(h, 1), :]

    def send_level(d, s, c):
        if s == chips - 1:

            @pl.when(takes(d, s + 1) == 0)
            def _():
                st_copy(d, s, c).start()
        else:
            st_copy(d, s, c).start()

    def level0(d, c, crosses):
        h = mine(c)
        s0_copy(d, h).wait_recv()
        total = row_of(d, 0, 0, h) * own[d, h] + row_of(d, 0, 1, h) * other[d, h]
        if not crossed:
            sent[d, 0, c] = total
            send_level(d, 0, c)
        elif crosses:
            sent[d, 1, c] = total

            @pl.when(takes(d, 2) == 0)
            def _():
                st_copy(d, 1, c).start()
        else:
            sent[d, 0, c] = total

            @pl.when((takes(d, 1) == 0) | (takes(d, 2) == 0))
            def _():
                st_copy(d, 0, c).start()

    def even_first(d, c):
        h = mine(c)
        fx, fy = takes(d, 1), takes(d, 2)

        @pl.when((fx == 1) | (fy == 0))
        def _():
            st_copy(d, 0, c).wait_recv()
            theirs = got[d, 0, c]
            edge[d, c] = fx.astype(F32) * theirs

            @pl.when(fy == 0)
            def _():
                sent[d, 1, c] = row_of(d, 1, 0, h) * sent[d, 0, c] + row_of(d, 1, 1, h) * theirs
                st_copy(d, 1, c).start()

        @pl.when((fx == 0) & (fy == 1))
        def _():
            edge[d, c] = jnp.zeros((dim, dim), F32)

    def even_second(d, c):
        @pl.when(takes(d, 2) == 1)
        def _():
            st_copy(d, 1, c).wait_recv()
            edge[d, c] = edge[d, c] + row_of(d, 2, 2, mine(c)) * got[d, 1, c]

        fin_copy(d, c).start()

    def odd_first(d, c):
        fx, fy = takes(d, 1), takes(d, 2)

        @pl.when(fy == 1)
        def _():
            st_copy(d, 1, c).wait_recv()

        @pl.when((fx == 0) & (fy == 1))
        def _():
            sent[d, 0, c] = row_of(d, bits, 0, mine(c)) * got[d, 1, c] + sent[d, 1, c]

        @pl.when((fx == 1) & (fy == 1))
        def _():
            sent[d, 0, c] = got[d, 1, c]

        @pl.when((fx == 0) & (fy == 0))
        def _():
            sent[d, 0, c] = sent[d, 1, c]

        @pl.when((fx == 0) | (fy == 1))
        def _():
            st_copy(d, 0, c).start()

    def odd_second(d, c):
        fx, fy = takes(d, 1), takes(d, 2)

        @pl.when((fx == 1) | (fy == 1))
        def _():
            st_copy(d, 0, c).wait_recv()

        @pl.when(fy == 1)
        def _():
            edge[d, c] = got[d, 0, c] + row_of(d, bits, 1, mine(c)) * got[d, 1, c]

        @pl.when((fx == 1) & (fy == 0))
        def _():
            edge[d, c] = got[d, 0, c]

        @pl.when((fx == 0) & (fy == 0))
        def _():
            edge[d, c] = jnp.zeros((dim, dim), F32)

        fin_copy(d, c).start()

    def step(d, s, c):
        h = mine(c)

        def arrive():
            st_copy(d, s, c).wait_recv()
            theirs = got[d, s, c]
            on_top = row_of(d, s + 1, 2, h) * theirs
            edge[d, c] = on_top if s == 0 else edge[d, c] + on_top
            if s + 1 < chips:
                sent[d, s + 1, c] = (
                    row_of(d, s + 1, 0, h) * sent[d, s, c] + row_of(d, s + 1, 1, h) * theirs
                )

        if s + 1 < chips:
            arrive()
            send_level(d, s + 1, c)
            return
        pl.when(takes(d, s + 1) == 1)(arrive)
        if s == 0:

            @pl.when(takes(d, s + 1) == 0)
            def _():
                edge[d, c] = jnp.zeros((dim, dim), F32)

        fin_copy(d, c).start()

    def put(d, c, target):
        f = takes(d, 0).astype(F32)
        h = mine(c)
        target[h] = (row_of(d, 0, 2, h) * edge[d, c] + f * other[d, h]).astype(BF16)
        h = others(c)
        s0_copy(d, h).wait_recv()
        fin_copy(d, c).wait_recv()
        target[h] = (row_of(d, 0, 2, h) * far[d, c] + f * other[d, h]).astype(BF16)

    def local_pair(c):
        pair = (others(c), mine(c))
        scaled = []
        for h in pair:
            last = cols[h, tokens - 1 : tokens, :]
            scaled.append((k[:, lane(h)].astype(F32) * jnp.exp2(last - cols[h])).astype(BF16))
        for h, x in zip(pair, scaled):
            own[0, h] = tn(x, v[:, lane(h)])

    def local_and_next(c):
        local_pair(c)
        cols_pair(c + 1 - (c + 1) // half)

    def s0_start(d, c):
        for h in (others(c), mine(c)):
            s0_copy(d, h).start()

    def levels0(d, lo, hi, lag, body):
        count = 2 if crossed else 1

        @pl.loop(0, (hi - lo) // count)
        def _(n):
            for e in range(count):
                c = lo + n * count + e
                body(c)
                level0(d, c - lag, (e + lo - lag) % 2 == 1)

    def first_exchange(d, body, done):
        lead = min(2, half)

        @pl.loop(done, lead)
        def _(c):
            body(c)
            s0_start(d, c)

        if d == 0:
            span_step(0)

        def more(c):
            body(c)
            s0_start(d, c)

        levels0(d, lead, half, lead, more)
        levels0(d, half, half + lead, lead, lambda c: None)
        if d == 0:
            span_step(1)

    def ticks(d, body, finish):
        if crossed:
            trips = half // 2

            def first(m):
                even_first(d, 2 * m)
                odd_first(d, 2 * m + 1)

            def second(m):
                even_second(d, 2 * m)
                odd_second(d, 2 * m + 1)

            def third(m):
                finish(2 * m)
                finish(2 * m + 1)

            stages = [(0, first), (trips, second), (trips + 1, third)]
        else:
            trips = half
            stages = [(2 * s, functools.partial(step, d, s)) for s in range(chips)]
            stages.append((2 * chips - 1, finish))

        @pl.loop(0, max(half, trips + stages[-1][0]))
        def _(t):
            @pl.when(t < half)
            def _():
                body(t)

            for n, (lag, stage) in enumerate(stages):
                if d == 0 and 1 <= n + 1 < bits and n >= 1 and not crossed:

                    @pl.when(t == lag)
                    def _():
                        span_step(n + 1)

                @pl.when((t >= lag) & (t < trips + lag))
                def _():
                    stage(t - lag)

    cols_pair(0)
    for c in first_loads:
        c.wait()
    local_and_next(0)
    pl.semaphore_wait(barrier, len(others_along) + n_tp - 1)
    if crossed:
        for o in range(1, n_seq):
            last_copy(o).start()
    else:
        sp_copy(0).start()
    s0_start(0, 0)
    for c in more_loads:
        c.wait()
    up_load.start()
    gate_load.start()
    first_exchange(0, local_and_next, 1)

    tiles = [(i, j) for i in range(nb) for j in range(i + 1)]
    sub = block // dim

    def span_of(i):
        return slice(i * block, (i + 1) * block)

    def decayed(s, h, i, j):
        row = rows[pl.ds(h, 1), j * block : (j + 1) * block]

        def parted(x, t, lo, hi):
            m = cols[h, j * block + hi - 1 : j * block + hi, :]
            width = (hi - lo) // dim
            right = jnp.exp2(jnp.concatenate([m] * width, axis=1) - row[:, lo:hi])
            left = jnp.exp2(cols[h, t : t + x.shape[0], :] - m)
            return (x * right) * jnp.concatenate([left] * width, axis=1)

        if i != j:
            return parted(s, i * block, 0, block).astype(BF16)
        lines = []
        for a in range(sub):
            t = slice(a * dim, (a + 1) * dim)
            line = []
            if a:
                for b in range(a):
                    line.append(
                        parted(s[t, b * dim : (b + 1) * dim], i * block + a * dim, b * dim, (b + 1) * dim)
                    )
            gap = cols[h, i * block + a * dim : i * block + (a + 1) * dim, :] - row[:, t]
            line.append(s[t, t] * jnp.exp2(gap + bias[...]))
            if a + 1 < sub:
                line.append(jnp.zeros((dim, (sub - 1 - a) * dim), F32))
            lines.append(jnp.concatenate([x.astype(BF16) for x in line], axis=1))
        return jnp.concatenate(lines, axis=0)

    def before_norm(h, i):
        r = span_of(i)
        grow = jnp.exp2(cols[h, r, :])
        grown[r, lane(h)] = (q[r, lane(h)].astype(F32) * grow).astype(BF16)
        s = jax.nn.sigmoid(gate[r, lane(h)].astype(F32))
        sig[h, r, :] = s
        dnorm[h, r, :] = up[r, lane(h)].astype(F32) * s

    def intra_pair(c):
        work = [(h, i, j) for h in (mine(c), others(c)) for i, j in tiles]

        def scores(h, i, j):
            return nt(q[span_of(i), lane(h)], k[span_of(j), lane(h)])

        ahead = scores(*work[0])
        total = None
        for n, (h, i, j) in enumerate(work):
            s = ahead
            if n + 1 < len(work):
                ahead = scores(*work[n + 1])
            p = decayed(s, h, i, j)
            probs[h, tiles.index((i, j))] = p
            o = nn(p, v[span_of(j), lane(h)])
            total = o if j == 0 else total + o
            if i == j:
                inside[h, span_of(i), :] = total
                before_norm(h, i)

    def finish_attn(c):
        put(0, c, state)
        for i in range(nb):
            r = span_of(i)
            square, inner = scale_ref[r, :], center_ref[r, :]
            for h in (mine(c), others(c)):
                a = inside[h, r, :] + nn(grown[r, lane(h)], state[h])
                attn[h, r, :] = a
                square = square + a * a
                inner = inner + dnorm[h, r, :] * a
            scale_ref[r, :] = square
            center_ref[r, :] = inner

    scale_ref[...] = jnp.zeros_like(scale_ref)
    center_ref[...] = jnp.zeros_like(center_ref)
    q_load.wait()
    up_load.wait()
    gate_load.wait()
    ticks(0, intra_pair, finish_attn)

    strips = tokens // 128

    def packed(x):
        turned = jnp.sum(x.T, axis=0, keepdims=True)
        return [turned[:, n * 128 : (n + 1) * 128] for n in range(strips)]

    spare = -2 * strips % 8
    pieces = packed(scale_ref[...]) + packed(center_ref[...])
    if spare:
        pieces.append(jnp.zeros((spare, 128), F32))
    sums[...] = jnp.concatenate(pieces, axis=0)

    def tp_copy(d):
        return pltpu.make_async_remote_copy(
            src_ref=sums, dst_ref=sums_in.at[d - 1], send_sem=tp_send.at[d - 1],
            recv_sem=tp_recv.at[d - 1], device_id=(me, lax.rem(z + d, n_tp)), device_id_type=MESH,
        )

    for d in range(1, n_tp):
        tp_copy(d).start()
    total = sums[...]
    for d in range(1, n_tp):
        tp_copy(d).wait_recv()
        total = total + sums_in[d - 1]
    scale = lax.rsqrt(total[0:strips] / width + 1e-06)
    center = total[strips : 2 * strips] * scale / width
    for n in range(strips):
        r = slice(n * 128, (n + 1) * 128)
        scale_ref[r, :] = jnp.broadcast_to(scale[n : n + 1, :], (128, 128)).T
        center_ref[r, :] = jnp.broadcast_to(center[n : n + 1, :], (128, 128)).T

    def pointwise(h):
        weighted = None
        for i in range(nb):
            r = span_of(i)
            sc = scale_ref[r, :]
            s, d = sig[h, r, :], dnorm[h, r, :]
            normed = attn[h, r, :] * sc
            g = (sc * (d - normed * center_ref[r, :])).astype(BF16)
            grad[r, lane(h)] = g
            up[r, lane(h)] = (normed * s).astype(BF16)
            gate[r, lane(h)] = (d * normed * (1.0 - s)).astype(BF16)
            w = tn(grown[r, lane(h)], g)
            weighted = w if weighted is None else weighted + w
        own[1, h] = weighted

    def pointwise_pair(c):
        pair = (others(c), mine(c))
        for h in pair:
            pointwise(h)

    first_exchange(1, pointwise_pair, 0)

    def backward_pair(c):
        pair = (mine(c), others(c))
        work = [(e, i, j) for e in (0, 1) for i, j in tiles]

        def scores(e, i, j):
            return nt(grad[span_of(i), lane(pair[e])], v[span_of(j), lane(pair[e])])

        def add(parts, n, x):
            parts[n] = x if n not in parts else parts[n] + x

        ahead = scores(*work[0])
        dq, dk, dv = {}, {}, {}
        for n, (e, i, j) in enumerate(work):
            h = pair[e]
            s = ahead
            if n + 1 < len(work):
                ahead = scores(*work[n + 1])
            r = span_of(i)
            add(dv, (e, j), tn(grad[r, lane(h)], probs[h, tiles.index((i, j))]))
            pg = decayed(s, h, i, j)
            add(dk, (e, j), tn(q[r, lane(h)], pg))
            add(dq, (e, i), nn(pg, k[span_of(j), lane(h)]))
            if i == j:
                carried = jnp.exp2(cols[h, r, :]) * nt(grad[r, lane(h)], state[h])
                grown[r, lane(h)] = (dq[e, i] + carried).astype(BF16)
            if i == nb - 1:
                dkt[h, :, span_of(j)] = dk[e, j]
                dvt[h, :, span_of(j)] = dv[e, j]

    ticks(1, backward_pair, lambda c: put(1, c, state_grad))

    if crossed:
        for o in range(1, n_seq):
            last_copy(o).wait_send()
    else:
        for b in range(bits):
            sp_copy(b).wait_send()
    for d in (0, 1):
        for b in (0, 1):
            part = pl.ds(b * half, half)
            pltpu.make_async_remote_copy(
                src_ref=own.at[d, part], dst_ref=other.at[d, part], send_sem=s0_send.at[d],
                recv_sem=s0_recv.at[d, 0], device_id=partner(0), device_id_type=MESH,
            ).wait_send()

        def sent_all(s, count):
            part = pl.ds(0, count)
            pltpu.make_async_remote_copy(
                src_ref=sent.at[d, s, part], dst_ref=got.at[d, s, part], send_sem=st_send.at[d, s],
                recv_sem=st_recv.at[d, s, 0], device_id=partner(s + 1), device_id_type=MESH,
            ).wait_send()

        if crossed:
            pl.when(takes(d, 1) == 0)(lambda: sent_all(0, half))
            pl.when(takes(d, 1) == 1)(lambda: sent_all(0, half // 2))
        else:
            for s in range(chips - 1):
                sent_all(s, half)
        pl.when(takes(d, chips) == 0)(lambda: sent_all(chips - 1, half))
        pltpu.make_async_remote_copy(
            src_ref=edge.at[d], dst_ref=far.at[d], send_sem=fin_send.at[d],
            recv_sem=fin_recv.at[d, 0], device_id=partner(0), device_id_type=MESH,
        ).wait_send()

    for d in range(1, n_tp):
        tp_copy(d).wait_send()


def last_kernel(
    heads, dim, tokens,
    out_ref, gg_ref, dq_ref, k, v, dkt, dvt, state_grad, rows,
    out_hbm, dq_hbm, dk_hbm, dv_hbm, gg_hbm,
    dk, dv, sem, pair_sem,
):
    block = min(256, tokens)
    many = 4 if heads % 4 == 0 else 2
    trips = heads // many
    whole = [
        pltpu.make_async_copy(a, b, sem.at[i])
        for i, (a, b) in enumerate(((out_ref, out_hbm), (gg_ref, gg_hbm), (dq_ref, dq_hbm)))
    ]
    for c in whole:
        c.start()

    def strips(i):
        part = pl.ds(pl.multiple_of(i * many * dim, many * dim), many * dim)
        return [
            pltpu.make_async_copy(a.at[:, part], b.at[:, part], pair_sem.at[n])
            for n, (a, b) in enumerate(((dk, dk_hbm), (dv, dv_hbm)))
        ]

    @pl.loop(0, trips)
    def _(i):
        for h in [many * i + n for n in range(many)]:
            at = pl.ds(pl.multiple_of(h * dim, dim), dim)
            row = rows[pl.ds(h, 1), :]
            tail = jnp.exp2(row[:, tokens - 1 : tokens] - row)
            for n in range(tokens // block):
                r = slice(n * block, (n + 1) * block)
                key = dkt[h, :, r] + tail[:, r] * nt(state_grad[h], v[r, at])
                value = dvt[h, :, r] + tail[:, r] * t0(state_grad[h], k[r, at])
                dk[r, at] = key.astype(BF16).T
                dv[r, at] = value.astype(BF16).T
        for c in strips(i):
            c.start()

    for n, (a, b) in enumerate(((dk, dk_hbm), (dv, dv_hbm))):
        pltpu.make_async_copy(a, b, pair_sem.at[n]).wait()
    for c in whole:
        c.wait()


def solution(mesh):
    n_seq, n_tp = mesh.shape["seq"], mesh.shape["tp"]

    def shards(queries, keys, values, gate, log_decay, out_grad):
        tokens, flat = queries.shape
        heads = log_decay.shape[1]
        dim = flat // heads
        half = heads // 2
        bits = n_seq.bit_length() - 1
        chips = bits - 1
        block = min(256, tokens)
        nb = tokens // block
        tile = (dim, dim)
        dma = pltpu.SemaphoreType.DMA
        peers = max(n_tp - 1, 1)
        spans = n_seq if chips == 2 else bits
        sums = (-(-2 * (tokens // 128) // 8) * 8, 128)
        hbm = pl.BlockSpec(memory_space=pltpu.HBM)
        vmem = pl.BlockSpec(memory_space=pltpu.VMEM)
        big = pltpu.VMEM((tokens, flat), BF16)
        wide = pltpu.VMEM((heads, tokens, dim), F32)
        turned = pltpu.VMEM((heads, dim, tokens), F32)
        flops = 2 * tokens * tokens * flat * 5 + 2 * tokens * flat * dim * 7
        results = pl.pallas_call(
            functools.partial(kernel, n_seq, n_tp, heads, dim, tokens),
            out_shape=[
                big, big, big, big, big, turned, turned,
                pltpu.VMEM((heads, *tile), BF16), pltpu.VMEM((heads, tokens), F32),
            ],
            in_specs=[hbm] * 6,
            out_specs=[vmem] * 9,
            scratch_shapes=[
                pltpu.VMEM((heads, tokens), F32), big, wide, pltpu.VMEM((tokens, 128), BF16),
                pltpu.VMEM(tile, F32), wide, wide, wide, wide, big,
                pltpu.VMEM((heads, nb * (nb + 1) // 2, block, block), BF16),
                pltpu.VMEM((2, heads, *tile), F32),
                pltpu.VMEM((2, heads, *tile), F32),
                pltpu.VMEM((2, chips, half, *tile), F32),
                pltpu.VMEM((2, chips, half, *tile), F32),
                pltpu.VMEM((2, half, *tile), F32),
                pltpu.VMEM((2, half, *tile), F32),
                pltpu.VMEM((heads, *tile), BF16),
                pltpu.VMEM((bits, heads, dim), F32), pltpu.VMEM((n_seq, heads, dim), F32),
                pltpu.VMEM((2, bits + 1, 3, heads, dim), F32),
                pltpu.VMEM(sums, F32), pltpu.VMEM((peers, *sums), F32),
                pltpu.VMEM((tokens, dim), F32), pltpu.VMEM((tokens, dim), F32),
                dma((12,)), dma((spans,)), dma((spans,)), dma((2,)), dma((2, heads)),
                dma((2, chips)), dma((2, chips, half)), dma((2,)), dma((2, half)),
                dma((peers,)), dma((peers,)),
            ],
            compiler_params=pltpu.CompilerParams(
                collective_id=0, has_side_effects=True, vmem_limit_bytes=43 << 20
            ),
            cost_estimate=pl.CostEstimate(
                flops=flops, bytes_accessed=tokens * flat * 10, transcendentals=0
            ),
        )(queries, keys, values, gate, log_decay.T, out_grad)
        return tuple(
            pl.pallas_call(
                functools.partial(last_kernel, heads, dim, tokens),
                out_shape=[jax.ShapeDtypeStruct((tokens, flat), BF16)] * 5,
                in_specs=[vmem] * 9,
                out_specs=[hbm] * 5,
                scratch_shapes=[big, big, dma((3,)), dma((2,))],
                compiler_params=pltpu.CompilerParams(vmem_limit_bytes=16 << 20),
                cost_estimate=pl.CostEstimate(
                    flops=4 * tokens * flat * dim, bytes_accessed=tokens * flat * 10, transcendentals=0
                ),
            )(*results)
        )

    spec = P("seq", "tp")
    return jax.shard_map(
        shards, mesh=mesh, in_specs=(spec,) * 6, out_specs=(spec,) * 5, check_vma=False
    )
```

```python
import functools

import jax
import jax.numpy as jnp
from jax import lax
from jax.experimental import pallas as pl
from jax.experimental.pallas import tpu as pltpu
from jax.sharding import PartitionSpec as P

MESH = pl.DeviceIdType.MESH
F32 = jnp.float32
BF16 = jnp.bfloat16
LOG2E = 1.4426950408889634
LOW = -1e9


def nt(a, b):
    return lax.dot_general(a, b, (((1,), (1,)), ((), ())), preferred_element_type=F32)


def tn(a, b):
    return lax.dot_general(a, b, (((0,), (0,)), ((), ())), preferred_element_type=F32)


def nn(a, b):
    return lax.dot_general(a, b, (((1,), (0,)), ((), ())), preferred_element_type=F32)


def t0(a, b):
    return lax.dot_general(a, b, (((0,), (1,)), ((), ())), preferred_element_type=F32)


def three_parts(x):
    high = x.astype(BF16).astype(F32)
    rest = x - high
    middle = rest.astype(BF16).astype(F32)
    low = (rest - middle).astype(BF16).astype(F32)
    return high, middle, low


def stacked(x):
    parts = three_parts(x)
    spare = 128 - 3 * x.shape[0]
    return jnp.concatenate([*parts, jnp.zeros((spare, x.shape[1]), F32)], axis=0)


def kernel(
    n_seq, n_tp, heads, dim, tokens,
    q_hbm, k_hbm, v_hbm, gate_hbm, rate_hbm, up_hbm,
    up, gate, grown, k, v, dkt, dvt, state_grad, rows,
    rate, q, cols, split, bias, inside, attn, sig, dnorm, grad, probs,
    own, other, sent, got, edge, far, state, span, span_in, factor,
    sums, sums_in, scale_ref, center_ref,
    in_sem, sp_send, sp_recv, s0_send, s0_recv, st_send, st_recv, fin_send, fin_recv, tp_send, tp_recv,
):
    width = heads * dim * n_tp
    half = heads // 2
    bits = n_seq.bit_length() - 1
    chips = bits - 1
    block = min(256, tokens)
    nb = tokens // block
    me = lax.axis_index("seq")
    z = lax.axis_index("tp")
    core = lax.rem(me, 2)

    def bit_of(b):
        return lax.rem(me // (1 << b), 2)

    def partner(b):
        return (me + (1 << b) * (1 - 2 * bit_of(b)), z)

    def takes(d, b):
        return bit_of(b) if d == 0 else 1 - bit_of(b)

    def load(i, a, b):
        return pltpu.make_async_copy(a, b, in_sem.at[i])

    rate_load = load(0, rate_hbm, rate)
    q_load, up_load, gate_load = (
        load(1 + i, a, b) for i, (a, b) in enumerate(((q_hbm, q), (up_hbm, up), (gate_hbm, gate)))
    )
    soon = min(2, half)

    def kv_loads(lo, hi, at):
        out = []
        for start in (lo, half + lo):
            part = slice(start * dim, (start + hi - lo) * dim)
            for a, b in ((k_hbm, k), (v_hbm, v)):
                out.append(load(4 + at + len(out), a.at[:, part], b.at[:, part]))
        return out

    first_loads = kv_loads(0, soon, 0)
    more_loads = kv_loads(soon, half, 4) if soon < half else []
    rate_load.start()
    for c in first_loads + more_loads:
        c.start()

    crossed = chips == 2 and half % 2 == 0
    barrier = pltpu.get_barrier_semaphore()
    if crossed:
        others_along = [(lax.rem(me + o, n_seq), z) for o in range(1, n_seq)]
    else:
        others_along = [partner(b) for b in range(bits)]
    for at in others_along:
        pl.semaphore_signal(barrier, inc=1, device_id=at, device_id_type=MESH)
    for d in range(1, n_tp):
        pl.semaphore_signal(
            barrier, inc=1, device_id=(me, lax.rem(z + d, n_tp)), device_id_type=MESH
        )

    def lane(h):
        return pl.ds(pl.multiple_of(h * dim, dim), dim)

    def mine(c):
        return core * half + c

    def others(c):
        return (1 - core) * half + c

    rate_load.wait()
    upto = (
        lax.broadcasted_iota(jnp.int32, (tokens, tokens), 0)
        <= lax.broadcasted_iota(jnp.int32, (tokens, tokens), 1)
    ).astype(BF16)
    parts = nn(stacked(rate[...]).astype(BF16), upto)
    across = parts[0:heads] + parts[heads : 2 * heads] + parts[2 * heads : 3 * heads]
    across = across * LOG2E
    rows[...] = across
    split[...] = stacked(across).T.astype(BF16)
    span[0] = jnp.broadcast_to(across[:, tokens - 1 : tokens], (heads, dim))
    q_load.start()
    corner = lax.broadcasted_iota(jnp.int32, (dim, dim), 0) >= lax.broadcasted_iota(
        jnp.int32, (dim, dim), 1
    )
    bias[...] = jnp.where(corner, 0.0, LOW)

    def cols_pair(c):
        pair = (mine(c), others(c))
        at = lax.broadcasted_iota(jnp.int32, (128, dim), 0)
        pick = jnp.concatenate(
            [
                ((at == h) | (at == h + heads) | (at == h + 2 * heads)).astype(F32).astype(BF16)
                for h in pair
            ],
            axis=1,
        )
        for r in (slice(n, n + 256) for n in range(0, tokens, 256)):
            wide = nn(split[r, :], pick)
            for n, h in enumerate(pair):
                cols[h, r, :] = wide[:, n * dim : (n + 1) * dim]

    def sp_copy(b):
        return pltpu.make_async_remote_copy(
            src_ref=span.at[b], dst_ref=span_in.at[b], send_sem=sp_send.at[b],
            recv_sem=sp_recv.at[b], device_id=partner(b), device_id_type=MESH,
        )

    def last_copy(o):
        return pltpu.make_async_remote_copy(
            src_ref=span.at[0], dst_ref=span_in.at[me], send_sem=sp_send.at[o],
            recv_sem=sp_recv.at[o], device_id=(lax.rem(me + o, n_seq), z), device_id_type=MESH,
        )

    def s0_copy(d, h):
        return pltpu.make_async_remote_copy(
            src_ref=own.at[d, h], dst_ref=other.at[d, h], send_sem=s0_send.at[d],
            recv_sem=s0_recv.at[d, h], device_id=partner(0), device_id_type=MESH,
        )

    def st_copy(d, s, c):
        return pltpu.make_async_remote_copy(
            src_ref=sent.at[d, s, c], dst_ref=got.at[d, s, c], send_sem=st_send.at[d, s],
            recv_sem=st_recv.at[d, s, c], device_id=partner(s + 1), device_id_type=MESH,
        )

    def fin_copy(d, c):
        return pltpu.make_async_remote_copy(
            src_ref=edge.at[d, c], dst_ref=far.at[d, c], send_sem=fin_send.at[d],
            recv_sem=fin_recv.at[d, c], device_id=partner(0), device_id_type=MESH,
        )

    def set_factors(b, here, there, before):
        for d in (0, 1):
            f = takes(d, b).astype(F32)
            factor[d, b, 0] = jnp.exp2(there * (1.0 - f))
            factor[d, b, 1] = jnp.exp2(here * f)
            factor[d, b, 2] = jnp.exp2(there * f) if b == 0 else f * jnp.exp2(before(d))

    def span_step(b):
        if crossed:
            return crossed_spans(b)
        sp_copy(b).wait_recv()
        here, there = span[b], span_in[b]
        if b + 1 < bits:
            span[b + 1] = here + there
            sp_copy(b + 1).start()

        def before(d):
            total = jnp.zeros((heads, dim), F32)
            for r in range(1, b):
                total = total + takes(d, r).astype(F32) * span_in[r]
            return total

        set_factors(b, here, there, before)

    def crossed_spans(b):
        if b == 0:
            o = 1 + (1 - core) * (n_seq - 2)
            last_copy(o).wait_recv()
            set_factors(0, span[0], span_in[partner(0)[0]], None)
            return
        for o in range(1, n_seq):
            if o == 1:
                pl.when(core == 0)(lambda: last_copy(1).wait_recv())
            elif o == n_seq - 1:
                pl.when(core == 1)(lambda: last_copy(n_seq - 1).wait_recv())
            else:
                last_copy(o).wait_recv()

        def chip(at):
            first = at - lax.rem(at, 2)
            return span_in[first] + span_in[first + 1]

        span_in[me] = span[0]
        mine_all, along_x, along_y = chip(me), chip(partner(1)[0]), chip(partner(2)[0])
        aside = chip(partner(1)[0] + partner(2)[0] - me)
        set_factors(1, mine_all, along_x, lambda d: jnp.zeros((heads, dim), F32))
        set_factors(
            2, mine_all + along_x, along_y + aside, lambda d: takes(d, 1).astype(F32) * along_x
        )
        for d in (0, 1):
            f = takes(d, 1).astype(F32)
            factor[d, bits, 0] = jnp.exp2(aside + mine_all)
            factor[d, bits, 1] = jnp.exp2(f * along_x + (1.0 - f) * aside)

    def row_of(d, b, n, h):
        return factor[d, b, n, pl.ds(h, 1), :]

    def send_level(d, s, c):
        if s == chips - 1:

            @pl.when(takes(d, s + 1) == 0)
            def _():
                st_copy(d, s, c).start()
        else:
            st_copy(d, s, c).start()

    def level0(d, c, crosses):
        h = mine(c)
        s0_copy(d, h).wait_recv()
        total = row_of(d, 0, 0, h) * own[d, h] + row_of(d, 0, 1, h) * other[d, h]
        if not crossed:
            sent[d, 0, c] = total
            send_level(d, 0, c)
        elif crosses:
            sent[d, 1, c] = total

            @pl.when(takes(d, 2) == 0)
            def _():
                st_copy(d, 1, c).start()
        else:
            sent[d, 0, c] = total

            @pl.when((takes(d, 1) == 0) | (takes(d, 2) == 0))
            def _():
                st_copy(d, 0, c).start()

    def even_first(d, c):
        h = mine(c)
        fx, fy = takes(d, 1), takes(d, 2)

        @pl.when((fx == 1) | (fy == 0))
        def _():
            st_copy(d, 0, c).wait_recv()
            theirs = got[d, 0, c]
            edge[d, c] = fx.astype(F32) * theirs

            @pl.when(fy == 0)
            def _():
                sent[d, 1, c] = row_of(d, 1, 0, h) * sent[d, 0, c] + row_of(d, 1, 1, h) * theirs
                st_copy(d, 1, c).start()

        @pl.when((fx == 0) & (fy == 1))
        def _():
            edge[d, c] = jnp.zeros((dim, dim), F32)

    def even_second(d, c):
        @pl.when(takes(d, 2) == 1)
        def _():
            st_copy(d, 1, c).wait_recv()
            edge[d, c] = edge[d, c] + row_of(d, 2, 2, mine(c)) * got[d, 1, c]

        fin_copy(d, c).start()

    def odd_first(d, c):
        fx, fy = takes(d, 1), takes(d, 2)

        @pl.when(fy == 1)
        def _():
            st_copy(d, 1, c).wait_recv()

        @pl.when((fx == 0) & (fy == 1))
        def _():
            sent[d, 0, c] = row_of(d, bits, 0, mine(c)) * got[d, 1, c] + sent[d, 1, c]

        @pl.when((fx == 1) & (fy == 1))
        def _():
            sent[d, 0, c] = got[d, 1, c]

        @pl.when((fx == 0) & (fy == 0))
        def _():
            sent[d, 0, c] = sent[d, 1, c]

        @pl.when((fx == 0) | (fy == 1))
        def _():
            st_copy(d, 0, c).start()

    def odd_second(d, c):
        fx, fy = takes(d, 1), takes(d, 2)

        @pl.when((fx == 1) | (fy == 1))
        def _():
            st_copy(d, 0, c).wait_recv()

        @pl.when(fy == 1)
        def _():
            edge[d, c] = got[d, 0, c] + row_of(d, bits, 1, mine(c)) * got[d, 1, c]

        @pl.when((fx == 1) & (fy == 0))
        def _():
            edge[d, c] = got[d, 0, c]

        @pl.when((fx == 0) & (fy == 0))
        def _():
            edge[d, c] = jnp.zeros((dim, dim), F32)

        fin_copy(d, c).start()

    def step(d, s, c):
        h = mine(c)

        def arrive():
            st_copy(d, s, c).wait_recv()
            theirs = got[d, s, c]
            on_top = row_of(d, s + 1, 2, h) * theirs
            edge[d, c] = on_top if s == 0 else edge[d, c] + on_top
            if s + 1 < chips:
                sent[d, s + 1, c] = (
                    row_of(d, s + 1, 0, h) * sent[d, s, c] + row_of(d, s + 1, 1, h) * theirs
                )

        if s + 1 < chips:
            arrive()
            send_level(d, s + 1, c)
            return
        pl.when(takes(d, s + 1) == 1)(arrive)
        if s == 0:

            @pl.when(takes(d, s + 1) == 0)
            def _():
                edge[d, c] = jnp.zeros((dim, dim), F32)

        fin_copy(d, c).start()

    def put(d, c, target):
        f = takes(d, 0).astype(F32)
        h = mine(c)
        target[h] = (row_of(d, 0, 2, h) * edge[d, c] + f * other[d, h]).astype(BF16)
        h = others(c)
        s0_copy(d, h).wait_recv()
        fin_copy(d, c).wait_recv()
        target[h] = (row_of(d, 0, 2, h) * far[d, c] + f * other[d, h]).astype(BF16)

    def local_pair(c):
        pair = (others(c), mine(c))
        scaled = []
        for h in pair:
            last = cols[h, tokens - 1 : tokens, :]
            scaled.append((k[:, lane(h)].astype(F32) * jnp.exp2(last - cols[h])).astype(BF16))
        for h, x in zip(pair, scaled):
            own[0, h] = tn(x, v[:, lane(h)])

    def local_and_next(c):
        local_pair(c)
        cols_pair(c + 1 - (c + 1) // half)

    def s0_start(d, c):
        for h in (others(c), mine(c)):
            s0_copy(d, h).start()

    def levels0(d, lo, hi, lag, body):
        count = 2 if crossed else 1

        @pl.loop(0, (hi - lo) // count)
        def _(n):
            for e in range(count):
                c = lo + n * count + e
                body(c)
                level0(d, c - lag, (e + lo - lag) % 2 == 1)

    def first_exchange(d, body, done):
        lead = min(2, half)

        @pl.loop(done, lead)
        def _(c):
            body(c)
            s0_start(d, c)

        if d == 0:
            span_step(0)

        def more(c):
            body(c)
            s0_start(d, c)

        levels0(d, lead, half, lead, more)
        levels0(d, half, half + lead, lead, lambda c: None)
        if d == 0:
            span_step(1)

    def ticks(d, body, finish):
        if crossed:
            trips = half // 2

            def first(m):
                even_first(d, 2 * m)
                odd_first(d, 2 * m + 1)

            def second(m):
                even_second(d, 2 * m)
                odd_second(d, 2 * m + 1)

            def third(m):
                finish(2 * m, 2 * m + 1)

            stages = [(0, first), (trips, second), (trips + 1, third)]
        else:
            trips = half
            stages = [(2 * s, functools.partial(step, d, s)) for s in range(chips)]
            stages.append((2 * chips - 1, finish))

        @pl.loop(0, max(half, trips + stages[-1][0]))
        def _(t):
            @pl.when(t < half)
            def _():
                body(t)

            for n, (lag, stage) in enumerate(stages):
                if d == 0 and 1 <= n + 1 < bits and n >= 1 and not crossed:

                    @pl.when(t == lag)
                    def _():
                        span_step(n + 1)

                @pl.when((t >= lag) & (t < trips + lag))
                def _():
                    stage(t - lag)

    cols_pair(0)
    for c in first_loads:
        c.wait()
    local_and_next(0)
    pl.semaphore_wait(barrier, len(others_along) + n_tp - 1)
    if crossed:
        for o in range(1, n_seq):
            last_copy(o).start()
    else:
        sp_copy(0).start()
    s0_start(0, 0)
    for c in more_loads:
        c.wait()
    up_load.start()
    gate_load.start()
    first_exchange(0, local_and_next, 1)

    tiles = [(i, j) for i in range(nb) for j in range(i + 1)]
    sub = block // dim

    def span_of(i):
        return slice(i * block, (i + 1) * block)

    def decayed(s, h, i, j):
        row = rows[pl.ds(h, 1), j * block : (j + 1) * block]

        def parted(x, t, lo, hi):
            m = cols[h, j * block + hi - 1 : j * block + hi, :]
            width = (hi - lo) // dim
            right = jnp.exp2(jnp.concatenate([m] * width, axis=1) - row[:, lo:hi])
            left = jnp.exp2(cols[h, t : t + x.shape[0], :] - m)
            return (x * right) * jnp.concatenate([left] * width, axis=1)

        if i != j:
            return parted(s, i * block, 0, block).astype(BF16)
        lines = []
        for a in range(sub):
            t = slice(a * dim, (a + 1) * dim)
            line = []
            if a:
                for b in range(a):
                    line.append(
                        parted(s[t, b * dim : (b + 1) * dim], i * block + a * dim, b * dim, (b + 1) * dim)
                    )
            gap = cols[h, i * block + a * dim : i * block + (a + 1) * dim, :] - row[:, t]
            line.append(s[t, t] * jnp.exp2(gap + bias[...]))
            if a + 1 < sub:
                line.append(jnp.zeros((dim, (sub - 1 - a) * dim), F32))
            lines.append(jnp.concatenate([x.astype(BF16) for x in line], axis=1))
        return jnp.concatenate(lines, axis=0)

    def before_norm(h, i):
        r = span_of(i)
        s = jax.nn.sigmoid(gate[r, lane(h)].astype(F32))
        sig[h, r, :] = s
        dnorm[h, r, :] = up[r, lane(h)].astype(F32) * s

    def intra_pair(c):
        work = [(h, i, j) for h in (mine(c), others(c)) for i, j in tiles]

        def scores(h, i, j):
            return nt(q[span_of(i), lane(h)], k[span_of(j), lane(h)])

        ahead = scores(*work[0])
        total = None
        for n, (h, i, j) in enumerate(work):
            s = ahead
            if n + 1 < len(work):
                ahead = scores(*work[n + 1])
            p = decayed(s, h, i, j)
            probs[h, tiles.index((i, j))] = p
            o = nn(p, v[span_of(j), lane(h)])
            total = o if j == 0 else total + o
            if i == j:
                inside[h, span_of(i), :] = total
                before_norm(h, i)

    def finish_attn(*chunks):
        for c in chunks:
            put(0, c, state)
        for r in (slice(n, n + 128) for n in range(0, tokens, 128)):
            square, inner = scale_ref[r, :], center_ref[r, :]
            for h in [h for c in chunks for h in (mine(c), others(c))]:
                a = inside[h, r, :] + jnp.exp2(cols[h, r, :]) * nn(q[r, lane(h)], state[h])
                attn[h, r, :] = a
                square = square + a * a
                inner = inner + dnorm[h, r, :] * a
            scale_ref[r, :] = square
            center_ref[r, :] = inner

    scale_ref[...] = jnp.zeros_like(scale_ref)
    center_ref[...] = jnp.zeros_like(center_ref)
    q_load.wait()
    up_load.wait()
    gate_load.wait()
    ticks(0, intra_pair, finish_attn)

    strips = tokens // 128

    def packed(x):
        turned = jnp.sum(x.T, axis=0, keepdims=True)
        return [turned[:, n * 128 : (n + 1) * 128] for n in range(strips)]

    spare = -2 * strips % 8
    pieces = packed(scale_ref[...]) + packed(center_ref[...])
    if spare:
        pieces.append(jnp.zeros((spare, 128), F32))
    sums[...] = jnp.concatenate(pieces, axis=0)

    def tp_copy(d):
        return pltpu.make_async_remote_copy(
            src_ref=sums, dst_ref=sums_in.at[d - 1], send_sem=tp_send.at[d - 1],
            recv_sem=tp_recv.at[d - 1], device_id=(me, lax.rem(z + d, n_tp)), device_id_type=MESH,
        )

    for d in range(1, n_tp):
        tp_copy(d).start()

    @pl.loop(0, heads)
    def _(h):
        grow = jnp.exp2(cols[h])
        grown[:, lane(h)] = (q[:, lane(h)].astype(F32) * grow).astype(BF16)

    total = sums[...]
    for d in range(1, n_tp):
        tp_copy(d).wait_recv()
        total = total + sums_in[d - 1]
    scale = lax.rsqrt(total[0:strips] / width + 1e-06)
    center = total[strips : 2 * strips] * scale / width
    for n in range(strips):
        r = slice(n * 128, (n + 1) * 128)
        scale_ref[r, :] = jnp.broadcast_to(scale[n : n + 1, :], (128, 128)).T
        center_ref[r, :] = jnp.broadcast_to(center[n : n + 1, :], (128, 128)).T

    def grad_pair(c):
        for h in (others(c), mine(c)):
            weighted = None
            for i in range(nb):
                r = span_of(i)
                sc = scale_ref[r, :]
                g = (sc * (dnorm[h, r, :] - attn[h, r, :] * sc * center_ref[r, :])).astype(BF16)
                grad[r, lane(h)] = g
                w = tn(grown[r, lane(h)], g)
                weighted = w if weighted is None else weighted + w
            own[1, h] = weighted

    def outputs(h):
        for i in range(nb):
            r = span_of(i)
            s = sig[h, r, :]
            normed = attn[h, r, :] * scale_ref[r, :]
            up[r, lane(h)] = (normed * s).astype(BF16)
            gate[r, lane(h)] = (dnorm[h, r, :] * normed * (1.0 - s)).astype(BF16)

    first_exchange(1, grad_pair, 0)
    pl.loop(0, heads)(outputs)

    def backward_pair(c):
        pair = (mine(c), others(c))
        work = [(e, i, j) for e in (0, 1) for i, j in tiles]

        def scores(e, i, j):
            return nt(grad[span_of(i), lane(pair[e])], v[span_of(j), lane(pair[e])])

        def add(parts, n, x):
            parts[n] = x if n not in parts else parts[n] + x

        ahead = scores(*work[0])
        dq, dk, dv = {}, {}, {}
        for n, (e, i, j) in enumerate(work):
            h = pair[e]
            s = ahead
            if n + 1 < len(work):
                ahead = scores(*work[n + 1])
            r = span_of(i)
            add(dv, (e, j), tn(grad[r, lane(h)], probs[h, tiles.index((i, j))]))
            pg = decayed(s, h, i, j)
            add(dk, (e, j), tn(q[r, lane(h)], pg))
            add(dq, (e, i), nn(pg, k[span_of(j), lane(h)]))
            if i == j:
                carried = jnp.exp2(cols[h, r, :]) * nt(grad[r, lane(h)], state[h])
                grown[r, lane(h)] = (dq[e, i] + carried).astype(BF16)
            if i == nb - 1:
                dkt[h, :, span_of(j)] = dk[e, j]
                dvt[h, :, span_of(j)] = dv[e, j]

    def put_grads(*chunks):
        for c in chunks:
            put(1, c, state_grad)

    ticks(1, backward_pair, put_grads)

    if crossed:
        for o in range(1, n_seq):
            last_copy(o).wait_send()
    else:
        for b in range(bits):
            sp_copy(b).wait_send()
    for d in (0, 1):
        for b in (0, 1):
            part = pl.ds(b * half, half)
            pltpu.make_async_remote_copy(
                src_ref=own.at[d, part], dst_ref=other.at[d, part], send_sem=s0_send.at[d],
                recv_sem=s0_recv.at[d, 0], device_id=partner(0), device_id_type=MESH,
            ).wait_send()

        def sent_all(s, count):
            part = pl.ds(0, count)
            pltpu.make_async_remote_copy(
                src_ref=sent.at[d, s, part], dst_ref=got.at[d, s, part], send_sem=st_send.at[d, s],
                recv_sem=st_recv.at[d, s, 0], device_id=partner(s + 1), device_id_type=MESH,
            ).wait_send()

        if crossed:
            pl.when(takes(d, 1) == 0)(lambda: sent_all(0, half))
            pl.when(takes(d, 1) == 1)(lambda: sent_all(0, half // 2))
        else:
            for s in range(chips - 1):
                sent_all(s, half)
        pl.when(takes(d, chips) == 0)(lambda: sent_all(chips - 1, half))
        pltpu.make_async_remote_copy(
            src_ref=edge.at[d], dst_ref=far.at[d], send_sem=fin_send.at[d],
            recv_sem=fin_recv.at[d, 0], device_id=partner(0), device_id_type=MESH,
        ).wait_send()

    for d in range(1, n_tp):
        tp_copy(d).wait_send()


def last_kernel(
    heads, dim, tokens,
    out_ref, gg_ref, dq_ref, k, v, dkt, dvt, state_grad, rows,
    out_hbm, dq_hbm, dk_hbm, dv_hbm, gg_hbm,
    dk, dv, sem, pair_sem,
):
    block = min(256, tokens)
    many = 4 if heads % 4 == 0 else 2
    trips = heads // many
    whole = [
        pltpu.make_async_copy(a, b, sem.at[i])
        for i, (a, b) in enumerate(((out_ref, out_hbm), (gg_ref, gg_hbm), (dq_ref, dq_hbm)))
    ]
    for c in whole:
        c.start()

    def strips(i):
        part = pl.ds(pl.multiple_of(i * many * dim, many * dim), many * dim)
        return [
            pltpu.make_async_copy(a.at[:, part], b.at[:, part], pair_sem.at[n])
            for n, (a, b) in enumerate(((dk, dk_hbm), (dv, dv_hbm)))
        ]

    @pl.loop(0, trips)
    def _(i):
        for h in [many * i + n for n in range(many)]:
            at = pl.ds(pl.multiple_of(h * dim, dim), dim)
            row = rows[pl.ds(h, 1), :]
            tail = jnp.exp2(row[:, tokens - 1 : tokens] - row)
            for n in range(tokens // block):
                r = slice(n * block, (n + 1) * block)
                key = dkt[h, :, r] + tail[:, r] * nt(state_grad[h], v[r, at])
                value = dvt[h, :, r] + tail[:, r] * t0(state_grad[h], k[r, at])
                dk[r, at] = key.astype(BF16).T
                dv[r, at] = value.astype(BF16).T
        for c in strips(i):
            c.start()

    for n, (a, b) in enumerate(((dk, dk_hbm), (dv, dv_hbm))):
        pltpu.make_async_copy(a, b, pair_sem.at[n]).wait()
    for c in whole:
        c.wait()


def solution(mesh):
    n_seq, n_tp = mesh.shape["seq"], mesh.shape["tp"]

    def shards(queries, keys, values, gate, log_decay, out_grad):
        tokens, flat = queries.shape
        heads = log_decay.shape[1]
        dim = flat // heads
        half = heads // 2
        bits = n_seq.bit_length() - 1
        chips = bits - 1
        block = min(256, tokens)
        nb = tokens // block
        tile = (dim, dim)
        dma = pltpu.SemaphoreType.DMA
        peers = max(n_tp - 1, 1)
        spans = n_seq if chips == 2 else bits
        sums = (-(-2 * (tokens // 128) // 8) * 8, 128)
        hbm = pl.BlockSpec(memory_space=pltpu.HBM)
        vmem = pl.BlockSpec(memory_space=pltpu.VMEM)
        big = pltpu.VMEM((tokens, flat), BF16)
        wide = pltpu.VMEM((heads, tokens, dim), F32)
        turned = pltpu.VMEM((heads, dim, tokens), F32)
        flops = 2 * tokens * tokens * flat * 5 + 2 * tokens * flat * dim * 7
        results = pl.pallas_call(
            functools.partial(kernel, n_seq, n_tp, heads, dim, tokens),
            out_shape=[
                big, big, big, big, big, turned, turned,
                pltpu.VMEM((heads, *tile), BF16), pltpu.VMEM((heads, tokens), F32),
            ],
            in_specs=[hbm] * 6,
            out_specs=[vmem] * 9,
            scratch_shapes=[
                pltpu.VMEM((heads, tokens), F32), big, wide, pltpu.VMEM((tokens, 128), BF16),
                pltpu.VMEM(tile, F32), wide, wide, wide, wide, big,
                pltpu.VMEM((heads, nb * (nb + 1) // 2, block, block), BF16),
                pltpu.VMEM((2, heads, *tile), F32),
                pltpu.VMEM((2, heads, *tile), F32),
                pltpu.VMEM((2, chips, half, *tile), F32),
                pltpu.VMEM((2, chips, half, *tile), F32),
                pltpu.VMEM((2, half, *tile), F32),
                pltpu.VMEM((2, half, *tile), F32),
                pltpu.VMEM((heads, *tile), BF16),
                pltpu.VMEM((bits, heads, dim), F32), pltpu.VMEM((n_seq, heads, dim), F32),
                pltpu.VMEM((2, bits + 1, 3, heads, dim), F32),
                pltpu.VMEM(sums, F32), pltpu.VMEM((peers, *sums), F32),
                pltpu.VMEM((tokens, dim), F32), pltpu.VMEM((tokens, dim), F32),
                dma((12,)), dma((spans,)), dma((spans,)), dma((2,)), dma((2, heads)),
                dma((2, chips)), dma((2, chips, half)), dma((2,)), dma((2, half)),
                dma((peers,)), dma((peers,)),
            ],
            compiler_params=pltpu.CompilerParams(
                collective_id=0, has_side_effects=True, vmem_limit_bytes=43 << 20
            ),
            cost_estimate=pl.CostEstimate(
                flops=flops, bytes_accessed=tokens * flat * 10, transcendentals=0
            ),
        )(queries, keys, values, gate, log_decay.T, out_grad)
        return tuple(
            pl.pallas_call(
                functools.partial(last_kernel, heads, dim, tokens),
                out_shape=[jax.ShapeDtypeStruct((tokens, flat), BF16)] * 5,
                in_specs=[vmem] * 9,
                out_specs=[hbm] * 5,
                scratch_shapes=[big, big, dma((3,)), dma((2,))],
                compiler_params=pltpu.CompilerParams(vmem_limit_bytes=16 << 20),
                cost_estimate=pl.CostEstimate(
                    flops=4 * tokens * flat * dim, bytes_accessed=tokens * flat * 10, transcendentals=0
                ),
            )(*results)
        )

    spec = P("seq", "tp")
    return jax.shard_map(
        shards, mesh=mesh, in_specs=(spec,) * 6, out_specs=(spec,) * 5, check_vma=False
    )
```

```python
import functools

import jax
import jax.numpy as jnp
from jax import lax
from jax.experimental import pallas as pl
from jax.experimental.pallas import tpu as pltpu
from jax.sharding import PartitionSpec as P

MESH = pl.DeviceIdType.MESH
F32 = jnp.float32
BF16 = jnp.bfloat16
LOG2E = 1.4426950408889634
LOW = -1e9


def nt(a, b):
    return lax.dot_general(a, b, (((1,), (1,)), ((), ())), preferred_element_type=F32)


def tn(a, b):
    return lax.dot_general(a, b, (((0,), (0,)), ((), ())), preferred_element_type=F32)


def nn(a, b):
    return lax.dot_general(a, b, (((1,), (0,)), ((), ())), preferred_element_type=F32)


def t0(a, b):
    return lax.dot_general(a, b, (((0,), (1,)), ((), ())), preferred_element_type=F32)


def three_parts(x):
    high = x.astype(BF16).astype(F32)
    rest = x - high
    middle = rest.astype(BF16).astype(F32)
    low = (rest - middle).astype(BF16).astype(F32)
    return high, middle, low


def stacked(x):
    parts = three_parts(x)
    spare = 128 - 3 * x.shape[0]
    return jnp.concatenate([*parts, jnp.zeros((spare, x.shape[1]), F32)], axis=0)


def kernel(
    n_seq, n_tp, heads, dim, tokens,
    q_hbm, k_hbm, v_hbm, gate_hbm, rate_hbm, up_hbm,
    up, gate, grown, k, v, dkt, dvt, state_grad, rows,
    rate, q, cols, split, bias, inside, attn, sig, dnorm, grad, probs,
    own, other, sent, got, edge, far, state, span, span_in, factor,
    sums, sums_in, scale_ref, center_ref,
    in_sem, sp_send, sp_recv, s0_send, s0_recv, st_send, st_recv, fin_send, fin_recv, tp_send, tp_recv,
):
    width = heads * dim * n_tp
    half = heads // 2
    bits = n_seq.bit_length() - 1
    chips = bits - 1
    block = min(256, tokens)
    nb = tokens // block
    me = lax.axis_index("seq")
    z = lax.axis_index("tp")
    core = lax.rem(me, 2)

    def bit_of(b):
        return lax.rem(me // (1 << b), 2)

    def partner(b):
        return (me + (1 << b) * (1 - 2 * bit_of(b)), z)

    def takes(d, b):
        return bit_of(b) if d == 0 else 1 - bit_of(b)

    def load(i, a, b):
        return pltpu.make_async_copy(a, b, in_sem.at[i])

    rate_load = load(0, rate_hbm, rate)
    q_load, up_load, gate_load = (
        load(1 + i, a, b) for i, (a, b) in enumerate(((q_hbm, q), (up_hbm, up), (gate_hbm, gate)))
    )
    soon = min(2, half)

    def kv_loads(lo, hi, at):
        out = []
        for start in (lo, half + lo):
            part = slice(start * dim, (start + hi - lo) * dim)
            for a, b in ((k_hbm, k), (v_hbm, v)):
                out.append(load(4 + at + len(out), a.at[:, part], b.at[:, part]))
        return out

    first_loads = kv_loads(0, soon, 0)
    more_loads = kv_loads(soon, half, 4) if soon < half else []
    rate_load.start()
    crossed = chips == 2 and half % 2 == 0
    barrier = pltpu.get_barrier_semaphore()
    if crossed:
        others_along = [(lax.rem(me + o, n_seq), z) for o in range(1, n_seq)]
    else:
        others_along = [partner(b) for b in range(bits)]
    for at in others_along:
        pl.semaphore_signal(barrier, inc=1, device_id=at, device_id_type=MESH)
    for d in range(1, n_tp):
        pl.semaphore_signal(
            barrier, inc=1, device_id=(me, lax.rem(z + d, n_tp)), device_id_type=MESH
        )
    for c in first_loads + more_loads:
        c.start()

    def lane(h):
        return pl.ds(pl.multiple_of(h * dim, dim), dim)

    def mine(c):
        return core * half + c

    def others(c):
        return (1 - core) * half + c

    rate_load.wait()
    upto = (
        lax.broadcasted_iota(jnp.int32, (tokens, tokens), 0)
        <= lax.broadcasted_iota(jnp.int32, (tokens, tokens), 1)
    ).astype(BF16)
    parts = nn(stacked(rate[...]).astype(BF16), upto)
    across = parts[0:heads] + parts[heads : 2 * heads] + parts[2 * heads : 3 * heads]
    across = across * LOG2E
    rows[...] = across
    split[...] = stacked(across).T.astype(BF16)
    span[0] = jnp.broadcast_to(across[:, tokens - 1 : tokens], (heads, dim))
    q_load.start()
    corner = lax.broadcasted_iota(jnp.int32, (dim, dim), 0) >= lax.broadcasted_iota(
        jnp.int32, (dim, dim), 1
    )
    bias[...] = jnp.where(corner, 0.0, LOW)

    def cols_pair(c):
        pair = (mine(c), others(c))
        at = lax.broadcasted_iota(jnp.int32, (128, dim), 0)
        pick = jnp.concatenate(
            [
                ((at == h) | (at == h + heads) | (at == h + 2 * heads)).astype(F32).astype(BF16)
                for h in pair
            ],
            axis=1,
        )
        for r in (slice(n, n + 256) for n in range(0, tokens, 256)):
            wide = nn(split[r, :], pick)
            for n, h in enumerate(pair):
                cols[h, r, :] = wide[:, n * dim : (n + 1) * dim]

    def sp_copy(b):
        return pltpu.make_async_remote_copy(
            src_ref=span.at[b], dst_ref=span_in.at[b], send_sem=sp_send.at[b],
            recv_sem=sp_recv.at[b], device_id=partner(b), device_id_type=MESH,
        )

    def last_copy(o):
        return pltpu.make_async_remote_copy(
            src_ref=span.at[0], dst_ref=span_in.at[me], send_sem=sp_send.at[o],
            recv_sem=sp_recv.at[o], device_id=(lax.rem(me + o, n_seq), z), device_id_type=MESH,
        )

    def s0_copy(d, h):
        return pltpu.make_async_remote_copy(
            src_ref=own.at[d, h], dst_ref=other.at[d, h], send_sem=s0_send.at[d],
            recv_sem=s0_recv.at[d, h], device_id=partner(0), device_id_type=MESH,
        )

    def st_copy(d, s, c):
        return pltpu.make_async_remote_copy(
            src_ref=sent.at[d, s, c], dst_ref=got.at[d, s, c], send_sem=st_send.at[d, s],
            recv_sem=st_recv.at[d, s, c], device_id=partner(s + 1), device_id_type=MESH,
        )

    def fin_copy(d, c):
        return pltpu.make_async_remote_copy(
            src_ref=edge.at[d, c], dst_ref=far.at[d, c], send_sem=fin_send.at[d],
            recv_sem=fin_recv.at[d, c], device_id=partner(0), device_id_type=MESH,
        )

    def set_factors(b, here, there, before):
        for d in (0, 1):
            f = takes(d, b).astype(F32)
            factor[d, b, 0] = jnp.exp2(there * (1.0 - f))
            factor[d, b, 1] = jnp.exp2(here * f)
            factor[d, b, 2] = jnp.exp2(there * f) if b == 0 else f * jnp.exp2(before(d))

    def span_step(b):
        if crossed:
            return crossed_spans(b)
        sp_copy(b).wait_recv()
        here, there = span[b], span_in[b]
        if b + 1 < bits:
            span[b + 1] = here + there
            sp_copy(b + 1).start()

        def before(d):
            total = jnp.zeros((heads, dim), F32)
            for r in range(1, b):
                total = total + takes(d, r).astype(F32) * span_in[r]
            return total

        set_factors(b, here, there, before)

    def crossed_spans(b):
        if b == 0:
            o = 1 + (1 - core) * (n_seq - 2)
            last_copy(o).wait_recv()
            set_factors(0, span[0], span_in[partner(0)[0]], None)
            return
        for o in range(1, n_seq):
            if o == 1:
                pl.when(core == 0)(lambda: last_copy(1).wait_recv())
            elif o == n_seq - 1:
                pl.when(core == 1)(lambda: last_copy(n_seq - 1).wait_recv())
            else:
                last_copy(o).wait_recv()

        def chip(at):
            first = at - lax.rem(at, 2)
            return span_in[first] + span_in[first + 1]

        span_in[me] = span[0]
        mine_all, along_x, along_y = chip(me), chip(partner(1)[0]), chip(partner(2)[0])
        aside = chip(partner(1)[0] + partner(2)[0] - me)
        set_factors(1, mine_all, along_x, lambda d: jnp.zeros((heads, dim), F32))
        set_factors(
            2, mine_all + along_x, along_y + aside, lambda d: takes(d, 1).astype(F32) * along_x
        )
        for d in (0, 1):
            f = takes(d, 1).astype(F32)
            factor[d, bits, 0] = jnp.exp2(aside + mine_all)
            factor[d, bits, 1] = jnp.exp2(f * along_x + (1.0 - f) * aside)

    def row_of(d, b, n, h):
        return factor[d, b, n, pl.ds(h, 1), :]

    def send_level(d, s, c):
        if s == chips - 1:

            @pl.when(takes(d, s + 1) == 0)
            def _():
                st_copy(d, s, c).start()
        else:
            st_copy(d, s, c).start()

    def level0(d, c, crosses):
        h = mine(c)
        s0_copy(d, h).wait_recv()
        total = row_of(d, 0, 0, h) * own[d, h] + row_of(d, 0, 1, h) * other[d, h]
        if not crossed:
            sent[d, 0, c] = total
            send_level(d, 0, c)
        elif crosses:
            sent[d, 1, c] = total

            @pl.when(takes(d, 2) == 0)
            def _():
                st_copy(d, 1, c).start()
        else:
            sent[d, 0, c] = total

            @pl.when((takes(d, 1) == 0) | (takes(d, 2) == 0))
            def _():
                st_copy(d, 0, c).start()

    def even_first(d, c):
        h = mine(c)
        fx, fy = takes(d, 1), takes(d, 2)

        @pl.when((fx == 1) | (fy == 0))
        def _():
            st_copy(d, 0, c).wait_recv()
            theirs = got[d, 0, c]
            edge[d, c] = fx.astype(F32) * theirs

            @pl.when(fy == 0)
            def _():
                sent[d, 1, c] = row_of(d, 1, 0, h) * sent[d, 0, c] + row_of(d, 1, 1, h) * theirs
                st_copy(d, 1, c).start()

        @pl.when((fx == 0) & (fy == 1))
        def _():
            edge[d, c] = jnp.zeros((dim, dim), F32)

    def even_second(d, c):
        @pl.when(takes(d, 2) == 1)
        def _():
            st_copy(d, 1, c).wait_recv()
            edge[d, c] = edge[d, c] + row_of(d, 2, 2, mine(c)) * got[d, 1, c]

        fin_copy(d, c).start()

    def odd_first(d, c):
        fx, fy = takes(d, 1), takes(d, 2)

        @pl.when(fy == 1)
        def _():
            st_copy(d, 1, c).wait_recv()

        @pl.when((fx == 0) & (fy == 1))
        def _():
            sent[d, 0, c] = row_of(d, bits, 0, mine(c)) * got[d, 1, c] + sent[d, 1, c]

        @pl.when((fx == 1) & (fy == 1))
        def _():
            sent[d, 0, c] = got[d, 1, c]

        @pl.when((fx == 0) & (fy == 0))
        def _():
            sent[d, 0, c] = sent[d, 1, c]

        @pl.when((fx == 0) | (fy == 1))
        def _():
            st_copy(d, 0, c).start()

    def odd_second(d, c):
        fx, fy = takes(d, 1), takes(d, 2)

        @pl.when((fx == 1) | (fy == 1))
        def _():
            st_copy(d, 0, c).wait_recv()

        @pl.when(fy == 1)
        def _():
            edge[d, c] = got[d, 0, c] + row_of(d, bits, 1, mine(c)) * got[d, 1, c]

        @pl.when((fx == 1) & (fy == 0))
        def _():
            edge[d, c] = got[d, 0, c]

        @pl.when((fx == 0) & (fy == 0))
        def _():
            edge[d, c] = jnp.zeros((dim, dim), F32)

        fin_copy(d, c).start()

    def step(d, s, c):
        h = mine(c)

        def arrive():
            st_copy(d, s, c).wait_recv()
            theirs = got[d, s, c]
            on_top = row_of(d, s + 1, 2, h) * theirs
            edge[d, c] = on_top if s == 0 else edge[d, c] + on_top
            if s + 1 < chips:
                sent[d, s + 1, c] = (
                    row_of(d, s + 1, 0, h) * sent[d, s, c] + row_of(d, s + 1, 1, h) * theirs
                )

        if s + 1 < chips:
            arrive()
            send_level(d, s + 1, c)
            return
        pl.when(takes(d, s + 1) == 1)(arrive)
        if s == 0:

            @pl.when(takes(d, s + 1) == 0)
            def _():
                edge[d, c] = jnp.zeros((dim, dim), F32)

        fin_copy(d, c).start()

    def put(d, c, target):
        f = takes(d, 0).astype(F32)
        h = mine(c)
        target[h] = (row_of(d, 0, 2, h) * edge[d, c] + f * other[d, h]).astype(BF16)
        h = others(c)
        s0_copy(d, h).wait_recv()
        fin_copy(d, c).wait_recv()
        target[h] = (row_of(d, 0, 2, h) * far[d, c] + f * other[d, h]).astype(BF16)

    def local(*some):
        scaled = []
        for h in some:
            last = cols[h, tokens - 1 : tokens, :]
            scaled.append((k[:, lane(h)].astype(F32) * jnp.exp2(last - cols[h])).astype(BF16))
        for h, x in zip(some, scaled):
            own[0, h] = tn(x, v[:, lane(h)])

    def local_and_next(c):
        local(others(c), mine(c))
        cols_pair(c + 1 - (c + 1) // half)

    def levels0(d, lo, hi, lag, body):
        count = 2 if crossed else 1

        @pl.loop(0, (hi - lo) // count)
        def _(n):
            for e in range(count):
                c = lo + n * count + e
                body(c)
                level0(d, c - lag, (e + lo - lag) % 2 == 1)

    def first_exchange(d, body, done):
        for n, h in enumerate([others(0), others(1), mine(0), mine(1)]):
            if n >= done:
                body(h)
                s0_copy(d, h).start()
        if d == 0:
            cols_pair(2 - 2 // half)
            span_step(0)

        def more(c):
            if d == 0:
                local_and_next(c)
            else:
                body(others(c), mine(c))
            for h in (others(c), mine(c)):
                s0_copy(d, h).start()

        levels0(d, 2, half, 2, more)
        levels0(d, half, half + 2, 2, lambda c: None)
        if d == 0:
            span_step(1)

    def ticks(d, body, finish):
        if crossed:
            trips = half // 2

            def first(m):
                even_first(d, 2 * m)
                odd_first(d, 2 * m + 1)

            def second(m):
                even_second(d, 2 * m)
                odd_second(d, 2 * m + 1)

            def third(m):
                finish(2 * m, 2 * m + 1)

            stages = [(0, first), (trips, second), (trips + 1, third)]
        else:
            trips = half
            stages = [(2 * s, functools.partial(step, d, s)) for s in range(chips)]
            stages.append((2 * chips - 1, finish))

        @pl.loop(0, max(half, trips + stages[-1][0]))
        def _(t):
            @pl.when(t < half)
            def _():
                body(t)

            for n, (lag, stage) in enumerate(stages):
                if d == 0 and 1 <= n + 1 < bits and n >= 1 and not crossed:

                    @pl.when(t == lag)
                    def _():
                        span_step(n + 1)

                @pl.when((t >= lag) & (t < trips + lag))
                def _():
                    stage(t - lag)

    cols_pair(0)
    for c in first_loads:
        c.wait()
    local(others(0))
    pl.semaphore_wait(barrier, len(others_along) + n_tp - 1)
    s0_copy(0, others(0)).start()
    if crossed:
        for o in range(1, n_seq):
            last_copy(o).start()
    else:
        sp_copy(0).start()
    cols_pair(1)
    for c in more_loads:
        c.wait()
    up_load.start()
    gate_load.start()
    first_exchange(0, local, 1)

    tiles = [(i, j) for i in range(nb) for j in range(i + 1)]
    sub = block // dim

    def span_of(i):
        return slice(i * block, (i + 1) * block)

    def decayed(s, h, i, j):
        row = rows[pl.ds(h, 1), j * block : (j + 1) * block]

        def parted(x, t, lo, hi):
            m = cols[h, j * block + hi - 1 : j * block + hi, :]
            width = (hi - lo) // dim
            right = jnp.exp2(jnp.concatenate([m] * width, axis=1) - row[:, lo:hi])
            left = jnp.exp2(cols[h, t : t + x.shape[0], :] - m)
            return (x * right) * jnp.concatenate([left] * width, axis=1)

        if i != j:
            return parted(s, i * block, 0, block).astype(BF16)
        lines = []
        for a in range(sub):
            t = slice(a * dim, (a + 1) * dim)
            line = []
            if a:
                for b in range(a):
                    line.append(
                        parted(s[t, b * dim : (b + 1) * dim], i * block + a * dim, b * dim, (b + 1) * dim)
                    )
            gap = cols[h, i * block + a * dim : i * block + (a + 1) * dim, :] - row[:, t]
            line.append(s[t, t] * jnp.exp2(gap + bias[...]))
            if a + 1 < sub:
                line.append(jnp.zeros((dim, (sub - 1 - a) * dim), F32))
            lines.append(jnp.concatenate([x.astype(BF16) for x in line], axis=1))
        return jnp.concatenate(lines, axis=0)

    def before_norm(h, i):
        r = span_of(i)
        s = jax.nn.sigmoid(gate[r, lane(h)].astype(F32))
        sig[h, r, :] = s
        dnorm[h, r, :] = up[r, lane(h)].astype(F32) * s

    def intra_pair(c):
        work = [(h, i, j) for h in (mine(c), others(c)) for i, j in tiles]

        def scores(h, i, j):
            return nt(q[span_of(i), lane(h)], k[span_of(j), lane(h)])

        ahead = scores(*work[0])
        total = None
        for n, (h, i, j) in enumerate(work):
            s = ahead
            if n + 1 < len(work):
                ahead = scores(*work[n + 1])
            p = decayed(s, h, i, j)
            probs[h, tiles.index((i, j))] = p
            o = nn(p, v[span_of(j), lane(h)])
            total = o if j == 0 else total + o
            if i == j:
                inside[h, span_of(i), :] = total
                before_norm(h, i)

    def finish_attn(*chunks):
        for c in chunks:
            put(0, c, state)
        for r in (slice(n, n + 128) for n in range(0, tokens, 128)):
            square, inner = scale_ref[r, :], center_ref[r, :]
            for h in [h for c in chunks for h in (mine(c), others(c))]:
                a = inside[h, r, :] + jnp.exp2(cols[h, r, :]) * nn(q[r, lane(h)], state[h])
                attn[h, r, :] = a
                square = square + a * a
                inner = inner + dnorm[h, r, :] * a
            scale_ref[r, :] = square
            center_ref[r, :] = inner

    scale_ref[...] = jnp.zeros_like(scale_ref)
    center_ref[...] = jnp.zeros_like(center_ref)
    q_load.wait()
    up_load.wait()
    gate_load.wait()
    ticks(0, intra_pair, finish_attn)

    strips = tokens // 128

    def packed(x):
        turned = jnp.sum(x.T, axis=0, keepdims=True)
        return [turned[:, n * 128 : (n + 1) * 128] for n in range(strips)]

    spare = -2 * strips % 8
    pieces = packed(scale_ref[...]) + packed(center_ref[...])
    if spare:
        pieces.append(jnp.zeros((spare, 128), F32))
    sums[...] = jnp.concatenate(pieces, axis=0)

    def tp_copy(d):
        return pltpu.make_async_remote_copy(
            src_ref=sums, dst_ref=sums_in.at[d - 1], send_sem=tp_send.at[d - 1],
            recv_sem=tp_recv.at[d - 1], device_id=(me, lax.rem(z + d, n_tp)), device_id_type=MESH,
        )

    for d in range(1, n_tp):
        tp_copy(d).start()

    def all_sent(d):
        for b in (0, 1):
            part = pl.ds(b * half, half)
            pltpu.make_async_remote_copy(
                src_ref=own.at[d, part], dst_ref=other.at[d, part], send_sem=s0_send.at[d],
                recv_sem=s0_recv.at[d, 0], device_id=partner(0), device_id_type=MESH,
            ).wait_send()

        def sent_all(s, count):
            part = pl.ds(0, count)
            pltpu.make_async_remote_copy(
                src_ref=sent.at[d, s, part], dst_ref=got.at[d, s, part], send_sem=st_send.at[d, s],
                recv_sem=st_recv.at[d, s, 0], device_id=partner(s + 1), device_id_type=MESH,
            ).wait_send()

        if crossed:
            pl.when(takes(d, 1) == 0)(lambda: sent_all(0, half))
            pl.when(takes(d, 1) == 1)(lambda: sent_all(0, half // 2))
        else:
            for s in range(chips - 1):
                sent_all(s, half)
        pl.when(takes(d, chips) == 0)(lambda: sent_all(chips - 1, half))
        pltpu.make_async_remote_copy(
            src_ref=edge.at[d], dst_ref=far.at[d], send_sem=fin_send.at[d],
            recv_sem=fin_recv.at[d, 0], device_id=partner(0), device_id_type=MESH,
        ).wait_send()

    @pl.loop(0, heads)
    def _(h):
        grow = jnp.exp2(cols[h])
        grown[:, lane(h)] = (q[:, lane(h)].astype(F32) * grow).astype(BF16)

    all_sent(0)
    if crossed:
        for o in range(1, n_seq):
            last_copy(o).wait_send()
    else:
        for b in range(bits):
            sp_copy(b).wait_send()
    total = sums[...]
    for d in range(1, n_tp):
        tp_copy(d).wait_recv()
        total = total + sums_in[d - 1]
    scale = lax.rsqrt(total[0:strips] / width + 1e-06)
    center = total[strips : 2 * strips] * scale / width
    for n in range(strips):
        r = slice(n * 128, (n + 1) * 128)
        scale_ref[r, :] = jnp.broadcast_to(scale[n : n + 1, :], (128, 128)).T
        center_ref[r, :] = jnp.broadcast_to(center[n : n + 1, :], (128, 128)).T

    def grads(*some):
        for h in some:
            weighted = None
            for i in range(nb):
                r = span_of(i)
                sc = scale_ref[r, :]
                g = (sc * (dnorm[h, r, :] - attn[h, r, :] * sc * center_ref[r, :])).astype(BF16)
                grad[r, lane(h)] = g
                w = tn(grown[r, lane(h)], g)
                weighted = w if weighted is None else weighted + w
            own[1, h] = weighted

    def outputs(h):
        for i in range(nb):
            r = span_of(i)
            s = sig[h, r, :]
            normed = attn[h, r, :] * scale_ref[r, :]
            up[r, lane(h)] = (normed * s).astype(BF16)
            gate[r, lane(h)] = (dnorm[h, r, :] * normed * (1.0 - s)).astype(BF16)

    first_exchange(1, grads, 0)
    pl.loop(0, heads)(outputs)

    def backward_pair(c):
        pair = (mine(c), others(c))
        work = [(e, i, j) for e in (0, 1) for i, j in tiles]

        def scores(e, i, j):
            return nt(grad[span_of(i), lane(pair[e])], v[span_of(j), lane(pair[e])])

        def add(parts, n, x):
            parts[n] = x if n not in parts else parts[n] + x

        ahead = scores(*work[0])
        dq, dk, dv = {}, {}, {}
        for n, (e, i, j) in enumerate(work):
            h = pair[e]
            s = ahead
            if n + 1 < len(work):
                ahead = scores(*work[n + 1])
            r = span_of(i)
            add(dv, (e, j), tn(grad[r, lane(h)], probs[h, tiles.index((i, j))]))
            pg = decayed(s, h, i, j)
            add(dk, (e, j), tn(q[r, lane(h)], pg))
            add(dq, (e, i), nn(pg, k[span_of(j), lane(h)]))
            if i == j:
                carried = jnp.exp2(cols[h, r, :]) * nt(grad[r, lane(h)], state[h])
                grown[r, lane(h)] = (dq[e, i] + carried).astype(BF16)
            if i == nb - 1:
                dkt[h, :, span_of(j)] = dk[e, j]
                dvt[h, :, span_of(j)] = dv[e, j]

    def put_grads(*chunks):
        for c in chunks:
            put(1, c, state_grad)

    ticks(1, backward_pair, put_grads)

    all_sent(1)
    for d in range(1, n_tp):
        tp_copy(d).wait_send()


def last_kernel(
    heads, dim, tokens,
    out_ref, gg_ref, dq_ref, k, v, dkt, dvt, state_grad, rows,
    out_hbm, dq_hbm, dk_hbm, dv_hbm, gg_hbm,
    dk, dv, sem, pair_sem,
):
    block = min(256, tokens)
    many = 4 if heads % 4 == 0 else 2
    trips = heads // many
    whole = [
        pltpu.make_async_copy(a, b, sem.at[i])
        for i, (a, b) in enumerate(((out_ref, out_hbm), (gg_ref, gg_hbm), (dq_ref, dq_hbm)))
    ]
    for c in whole:
        c.start()

    def strips(i):
        part = pl.ds(pl.multiple_of(i * many * dim, many * dim), many * dim)
        return [
            pltpu.make_async_copy(a.at[:, part], b.at[:, part], pair_sem.at[n])
            for n, (a, b) in enumerate(((dk, dk_hbm), (dv, dv_hbm)))
        ]

    @pl.loop(0, trips)
    def _(i):
        for h in [many * i + n for n in range(many)]:
            at = pl.ds(pl.multiple_of(h * dim, dim), dim)
            row = rows[pl.ds(h, 1), :]
            tail = jnp.exp2(row[:, tokens - 1 : tokens] - row)
            for n in range(tokens // block):
                r = slice(n * block, (n + 1) * block)
                key = dkt[h, :, r] + tail[:, r] * nt(state_grad[h], v[r, at])
                value = dvt[h, :, r] + tail[:, r] * t0(state_grad[h], k[r, at])
                dk[r, at] = key.astype(BF16).T
                dv[r, at] = value.astype(BF16).T
        for c in strips(i):
            c.start()

    for n, (a, b) in enumerate(((dk, dk_hbm), (dv, dv_hbm))):
        pltpu.make_async_copy(a, b, pair_sem.at[n]).wait()
    for c in whole:
        c.wait()


def solution(mesh):
    n_seq, n_tp = mesh.shape["seq"], mesh.shape["tp"]

    def shards(queries, keys, values, gate, log_decay, out_grad):
        tokens, flat = queries.shape
        heads = log_decay.shape[1]
        dim = flat // heads
        half = heads // 2
        bits = n_seq.bit_length() - 1
        chips = bits - 1
        block = min(256, tokens)
        nb = tokens // block
        tile = (dim, dim)
        dma = pltpu.SemaphoreType.DMA
        peers = max(n_tp - 1, 1)
        spans = n_seq if chips == 2 else bits
        sums = (-(-2 * (tokens // 128) // 8) * 8, 128)
        hbm = pl.BlockSpec(memory_space=pltpu.HBM)
        vmem = pl.BlockSpec(memory_space=pltpu.VMEM)
        big = pltpu.VMEM((tokens, flat), BF16)
        wide = pltpu.VMEM((heads, tokens, dim), F32)
        turned = pltpu.VMEM((heads, dim, tokens), F32)
        flops = 2 * tokens * tokens * flat * 5 + 2 * tokens * flat * dim * 7
        results = pl.pallas_call(
            functools.partial(kernel, n_seq, n_tp, heads, dim, tokens),
            out_shape=[
                big, big, big, big, big, turned, turned,
                pltpu.VMEM((heads, *tile), BF16), pltpu.VMEM((heads, tokens), F32),
            ],
            in_specs=[hbm] * 6,
            out_specs=[vmem] * 9,
            scratch_shapes=[
                pltpu.VMEM((heads, tokens), F32), big, wide, pltpu.VMEM((tokens, 128), BF16),
                pltpu.VMEM(tile, F32), wide, wide, wide, wide, big,
                pltpu.VMEM((heads, nb * (nb + 1) // 2, block, block), BF16),
                pltpu.VMEM((2, heads, *tile), F32),
                pltpu.VMEM((2, heads, *tile), F32),
                pltpu.VMEM((2, chips, half, *tile), F32),
                pltpu.VMEM((2, chips, half, *tile), F32),
                pltpu.VMEM((2, half, *tile), F32),
                pltpu.VMEM((2, half, *tile), F32),
                pltpu.VMEM((heads, *tile), BF16),
                pltpu.VMEM((bits, heads, dim), F32), pltpu.VMEM((n_seq, heads, dim), F32),
                pltpu.VMEM((2, bits + 1, 3, heads, dim), F32),
                pltpu.VMEM(sums, F32), pltpu.VMEM((peers, *sums), F32),
                pltpu.VMEM((tokens, dim), F32), pltpu.VMEM((tokens, dim), F32),
                dma((12,)), dma((spans,)), dma((spans,)), dma((2,)), dma((2, heads)),
                dma((2, chips)), dma((2, chips, half)), dma((2,)), dma((2, half)),
                dma((peers,)), dma((peers,)),
            ],
            compiler_params=pltpu.CompilerParams(
                collective_id=0, has_side_effects=True, vmem_limit_bytes=43 << 20
            ),
            cost_estimate=pl.CostEstimate(
                flops=flops, bytes_accessed=tokens * flat * 10, transcendentals=0
            ),
        )(queries, keys, values, gate, log_decay.T, out_grad)
        return tuple(
            pl.pallas_call(
                functools.partial(last_kernel, heads, dim, tokens),
                out_shape=[jax.ShapeDtypeStruct((tokens, flat), BF16)] * 5,
                in_specs=[vmem] * 9,
                out_specs=[hbm] * 5,
                scratch_shapes=[big, big, dma((3,)), dma((2,))],
                compiler_params=pltpu.CompilerParams(vmem_limit_bytes=16 << 20),
                cost_estimate=pl.CostEstimate(
                    flops=4 * tokens * flat * dim, bytes_accessed=tokens * flat * 10, transcendentals=0
                ),
            )(*results)
        )

    spec = P("seq", "tp")
    return jax.shard_map(
        shards, mesh=mesh, in_specs=(spec,) * 6, out_specs=(spec,) * 5, check_vma=False
    )
```

```python
import functools

import jax
import jax.numpy as jnp
from jax import lax
from jax.experimental import pallas as pl
from jax.experimental.pallas import tpu as pltpu
from jax.sharding import PartitionSpec as P

MESH = pl.DeviceIdType.MESH
F32 = jnp.float32
BF16 = jnp.bfloat16
LOG2E = 1.4426950408889634
LOW = -1e9


def nt(a, b):
    return lax.dot_general(a, b, (((1,), (1,)), ((), ())), preferred_element_type=F32)


def tn(a, b):
    return lax.dot_general(a, b, (((0,), (0,)), ((), ())), preferred_element_type=F32)


def nn(a, b):
    return lax.dot_general(a, b, (((1,), (0,)), ((), ())), preferred_element_type=F32)


def t0(a, b):
    return lax.dot_general(a, b, (((0,), (1,)), ((), ())), preferred_element_type=F32)


def three_parts(x):
    high = x.astype(BF16).astype(F32)
    rest = x - high
    middle = rest.astype(BF16).astype(F32)
    low = (rest - middle).astype(BF16).astype(F32)
    return high, middle, low


def stacked(x):
    parts = three_parts(x)
    spare = 128 - 3 * x.shape[0]
    return jnp.concatenate([*parts, jnp.zeros((spare, x.shape[1]), F32)], axis=0)


def kernel(
    n_seq, n_tp, heads, dim, tokens,
    q_hbm, k_hbm, v_hbm, gate_hbm, rate_hbm, up_hbm,
    up, gate, grown, k, v, dkt, dvt, state_grad, rows,
    rate, q, cols, split, bias, inside, attn, sig, dnorm, grad, probs,
    own, other, sent, got, edge, far, state, span, span_in, factor,
    sums, sums_in, scale_ref, center_ref,
    in_sem, sp_send, sp_recv, s0_send, s0_recv, st_send, st_recv, fin_send, fin_recv, tp_send, tp_recv,
):
    width = heads * dim * n_tp
    half = heads // 2
    bits = n_seq.bit_length() - 1
    chips = bits - 1
    block = min(256, tokens)
    nb = tokens // block
    me = lax.axis_index("seq")
    z = lax.axis_index("tp")
    core = lax.rem(me, 2)

    def bit_of(b):
        return lax.rem(me // (1 << b), 2)

    def partner(b):
        return (me + (1 << b) * (1 - 2 * bit_of(b)), z)

    def takes(d, b):
        return bit_of(b) if d == 0 else 1 - bit_of(b)

    def load(i, a, b):
        return pltpu.make_async_copy(a, b, in_sem.at[i])

    rate_load = load(0, rate_hbm, rate)
    q_load, up_load, gate_load = (
        load(1 + i, a, b) for i, (a, b) in enumerate(((q_hbm, q), (up_hbm, up), (gate_hbm, gate)))
    )
    soon = min(2, half)

    def kv_loads(lo, hi, at):
        starts, waits = [], []
        for n, (a, b) in enumerate(((k_hbm, k), (v_hbm, v))):
            for start in (lo, half + lo):
                part = slice(start * dim, (start + hi - lo) * dim)
                starts.append(load(at + n, a.at[:, part], b.at[:, part]))
            both = slice(0, 2 * (hi - lo) * dim)
            waits.append(load(at + n, a.at[:, both], b.at[:, both]))
        return starts, waits

    first_loads, first_waits = kv_loads(0, soon, 4)
    more_loads, more_waits = kv_loads(soon, half, 6) if soon < half else ([], [])
    rate_load.start()
    crossed = chips == 2 and half % 2 == 0
    group = 2 if crossed else 1
    barrier = pltpu.get_barrier_semaphore()
    if crossed:
        others_along = [(lax.rem(me + o, n_seq), z) for o in range(1, n_seq)]
    else:
        others_along = [partner(b) for b in range(bits)]
    for at in others_along:
        pl.semaphore_signal(barrier, inc=1, device_id=at, device_id_type=MESH)
    for d in range(1, n_tp):
        pl.semaphore_signal(
            barrier, inc=1, device_id=(me, lax.rem(z + d, n_tp)), device_id_type=MESH
        )
    for c in first_loads + more_loads:
        c.start()

    def lane(h):
        return pl.ds(pl.multiple_of(h * dim, dim), dim)

    def mine(c):
        return core * half + c

    def others(c):
        return (1 - core) * half + c

    rate_load.wait()
    upto = (
        lax.broadcasted_iota(jnp.int32, (tokens, tokens), 0)
        <= lax.broadcasted_iota(jnp.int32, (tokens, tokens), 1)
    ).astype(BF16)
    parts = nn(stacked(rate[...]).astype(BF16), upto)
    across = parts[0:heads] + parts[heads : 2 * heads] + parts[2 * heads : 3 * heads]
    across = across * LOG2E
    rows[...] = across
    split[...] = stacked(across).T.astype(BF16)
    span[0] = jnp.broadcast_to(across[:, tokens - 1 : tokens], (heads, dim))
    q_load.start()
    corner = lax.broadcasted_iota(jnp.int32, (dim, dim), 0) >= lax.broadcasted_iota(
        jnp.int32, (dim, dim), 1
    )
    bias[...] = jnp.where(corner, 0.0, LOW)

    def cols_pair(c):
        pair = (mine(c), others(c))
        at = lax.broadcasted_iota(jnp.int32, (128, dim), 0)
        pick = jnp.concatenate(
            [
                ((at == h) | (at == h + heads) | (at == h + 2 * heads)).astype(F32).astype(BF16)
                for h in pair
            ],
            axis=1,
        )
        for r in (slice(n, n + 256) for n in range(0, tokens, 256)):
            wide = nn(split[r, :], pick)
            for n, h in enumerate(pair):
                cols[h, r, :] = wide[:, n * dim : (n + 1) * dim]

    def sp_copy(b):
        return pltpu.make_async_remote_copy(
            src_ref=span.at[b], dst_ref=span_in.at[b], send_sem=sp_send.at[b],
            recv_sem=sp_recv.at[b], device_id=partner(b), device_id_type=MESH,
        )

    def last_copy(o):
        if o == 1:
            slot = core
        elif o == n_seq - 1:
            slot = 1 - core
        else:
            slot = 1
        return pltpu.make_async_remote_copy(
            src_ref=span.at[0], dst_ref=span_in.at[me], send_sem=sp_send.at[0],
            recv_sem=sp_recv.at[slot], device_id=(lax.rem(me + o, n_seq), z), device_id_type=MESH,
        )

    def lasts(count, slot):
        part = span_in.at[pl.ds(0, count)]
        return pltpu.make_async_remote_copy(
            src_ref=part, dst_ref=part, send_sem=sp_send.at[0], recv_sem=sp_recv.at[slot],
            device_id=partner(0), device_id_type=MESH,
        )

    def s0_copy(d, h, slot, count=1):
        part = pl.ds(h, count)
        return pltpu.make_async_remote_copy(
            src_ref=own.at[d, part], dst_ref=other.at[d, part], send_sem=s0_send.at[d],
            recv_sem=s0_recv.at[d, slot], device_id=partner(0), device_id_type=MESH,
        )

    def s0_start(d, c, needed):
        if needed:
            s0_copy(d, others(c), c).start()
        else:
            s0_copy(d, mine(c), half).start()

    def st_copy(d, s, c):
        return pltpu.make_async_remote_copy(
            src_ref=sent.at[d, s, c], dst_ref=got.at[d, s, c], send_sem=st_send.at[d, s],
            recv_sem=st_recv.at[d, s, c], device_id=partner(s + 1), device_id_type=MESH,
        )

    def fin_copy(d, c):
        return pltpu.make_async_remote_copy(
            src_ref=edge.at[d, c], dst_ref=far.at[d, c], send_sem=fin_send.at[d],
            recv_sem=fin_recv.at[d, c // group], device_id=partner(0), device_id_type=MESH,
        )

    def set_factors(b, here, there, before):
        for d in (0, 1):
            f = takes(d, b).astype(F32)
            factor[d, b, 0] = jnp.exp2(there * (1.0 - f))
            factor[d, b, 1] = jnp.exp2(here * f)
            factor[d, b, 2] = jnp.exp2(there * f) if b == 0 else f * jnp.exp2(before(d))

    def span_step(b):
        if crossed:
            return crossed_spans(b)
        sp_copy(b).wait_recv()
        here, there = span[b], span_in[b]
        if b + 1 < bits:
            span[b + 1] = here + there
            sp_copy(b + 1).start()

        def before(d):
            total = jnp.zeros((heads, dim), F32)
            for r in range(1, b):
                total = total + takes(d, r).astype(F32) * span_in[r]
            return total

        set_factors(b, here, there, before)

    def crossed_spans(b):
        if b == 0:
            lasts(1, 0).wait_recv()
            set_factors(0, span[0], span_in[partner(0)[0]], None)
            return
        lasts(n_seq - 2, 1).wait_recv()

        def chip(at):
            first = at - lax.rem(at, 2)
            return span_in[first] + span_in[first + 1]

        span_in[me] = span[0]
        mine_all, along_x, along_y = chip(me), chip(partner(1)[0]), chip(partner(2)[0])
        aside = chip(partner(1)[0] + partner(2)[0] - me)
        set_factors(1, mine_all, along_x, lambda d: jnp.zeros((heads, dim), F32))
        set_factors(
            2, mine_all + along_x, along_y + aside, lambda d: takes(d, 1).astype(F32) * along_x
        )
        for d in (0, 1):
            f = takes(d, 1).astype(F32)
            factor[d, bits, 0] = jnp.exp2(aside + mine_all)
            factor[d, bits, 1] = jnp.exp2(f * along_x + (1.0 - f) * aside)

    def row_of(d, b, n, h):
        return factor[d, b, n, pl.ds(h, 1), :]

    def send_level(d, s, c):
        if s == chips - 1:

            @pl.when(takes(d, s + 1) == 0)
            def _():
                st_copy(d, s, c).start()
        else:
            st_copy(d, s, c).start()

    def level0(d, c, crosses):
        h = mine(c)
        s0_copy(d, h, c).wait_recv()
        total = row_of(d, 0, 0, h) * own[d, h] + row_of(d, 0, 1, h) * other[d, h]
        if not crossed:
            sent[d, 0, c] = total
            send_level(d, 0, c)
        elif crosses:
            sent[d, 1, c] = total

            @pl.when(takes(d, 2) == 0)
            def _():
                st_copy(d, 1, c).start()
        else:
            sent[d, 0, c] = total

            @pl.when((takes(d, 1) == 0) | (takes(d, 2) == 0))
            def _():
                st_copy(d, 0, c).start()

    def even_first(d, c):
        h = mine(c)
        fx, fy = takes(d, 1), takes(d, 2)

        @pl.when((fx == 1) | (fy == 0))
        def _():
            st_copy(d, 0, c).wait_recv()
            theirs = got[d, 0, c]
            edge[d, c] = fx.astype(F32) * theirs

            @pl.when(fy == 0)
            def _():
                sent[d, 1, c] = row_of(d, 1, 0, h) * sent[d, 0, c] + row_of(d, 1, 1, h) * theirs
                st_copy(d, 1, c).start()

        @pl.when((fx == 0) & (fy == 1))
        def _():
            edge[d, c] = jnp.zeros((dim, dim), F32)

    def even_second(d, c):
        @pl.when(takes(d, 2) == 1)
        def _():
            st_copy(d, 1, c).wait_recv()
            edge[d, c] = edge[d, c] + row_of(d, 2, 2, mine(c)) * got[d, 1, c]

        fin_copy(d, c).start()

    def odd_first(d, c):
        fx, fy = takes(d, 1), takes(d, 2)

        @pl.when(fy == 1)
        def _():
            st_copy(d, 1, c).wait_recv()

        @pl.when((fx == 0) & (fy == 1))
        def _():
            sent[d, 0, c] = row_of(d, bits, 0, mine(c)) * got[d, 1, c] + sent[d, 1, c]

        @pl.when((fx == 1) & (fy == 1))
        def _():
            sent[d, 0, c] = got[d, 1, c]

        @pl.when((fx == 0) & (fy == 0))
        def _():
            sent[d, 0, c] = sent[d, 1, c]

        @pl.when((fx == 0) | (fy == 1))
        def _():
            st_copy(d, 0, c).start()

    def odd_second(d, c):
        fx, fy = takes(d, 1), takes(d, 2)

        @pl.when((fx == 1) | (fy == 1))
        def _():
            st_copy(d, 0, c).wait_recv()

        @pl.when(fy == 1)
        def _():
            edge[d, c] = got[d, 0, c] + row_of(d, bits, 1, mine(c)) * got[d, 1, c]

        @pl.when((fx == 1) & (fy == 0))
        def _():
            edge[d, c] = got[d, 0, c]

        @pl.when((fx == 0) & (fy == 0))
        def _():
            edge[d, c] = jnp.zeros((dim, dim), F32)

        fin_copy(d, c).start()

    def step(d, s, c):
        h = mine(c)

        def arrive():
            st_copy(d, s, c).wait_recv()
            theirs = got[d, s, c]
            on_top = row_of(d, s + 1, 2, h) * theirs
            edge[d, c] = on_top if s == 0 else edge[d, c] + on_top
            if s + 1 < chips:
                sent[d, s + 1, c] = (
                    row_of(d, s + 1, 0, h) * sent[d, s, c] + row_of(d, s + 1, 1, h) * theirs
                )

        if s + 1 < chips:
            arrive()
            send_level(d, s + 1, c)
            return
        pl.when(takes(d, s + 1) == 1)(arrive)
        if s == 0:

            @pl.when(takes(d, s + 1) == 0)
            def _():
                edge[d, c] = jnp.zeros((dim, dim), F32)

        fin_copy(d, c).start()

    def put(d, chunks, target):
        f = takes(d, 0).astype(F32)
        pltpu.make_async_remote_copy(
            src_ref=edge.at[d, pl.ds(chunks[0], group)], dst_ref=far.at[d, pl.ds(chunks[0], group)],
            send_sem=fin_send.at[d], recv_sem=fin_recv.at[d, chunks[0] // group],
            device_id=partner(0), device_id_type=MESH,
        ).wait_recv()
        for c in chunks:
            for h, end in ((mine(c), edge), (others(c), far)):
                target[h] = (row_of(d, 0, 2, h) * end[d, c] + f * other[d, h]).astype(BF16)

    def local(*some):
        scaled = []
        for h in some:
            last = cols[h, tokens - 1 : tokens, :]
            scaled.append((k[:, lane(h)].astype(F32) * jnp.exp2(last - cols[h])).astype(BF16))
        for h, x in zip(some, scaled):
            own[0, h] = tn(x, v[:, lane(h)])

    def local_and_next(c):
        local(others(c), mine(c))
        cols_pair(c + 1 - (c + 1) // half)

    def levels0(d, lo, hi, lag, body):
        count = 2 if crossed else 1

        @pl.loop(0, (hi - lo) // count)
        def _(n):
            for e in range(count):
                c = lo + n * count + e
                body(c)
                level0(d, c - lag, (e + lo - lag) % 2 == 1)

    def first_exchange(d, body, done):
        for n, (c, needed) in enumerate(((0, True), (1, True), (0, False), (1, False))):
            if n >= done:
                body(others(c) if needed else mine(c))
                s0_start(d, c, needed)
        if d == 0:
            cols_pair(2 - 2 // half)
            span_step(0)

        def more(c):
            if d == 0:
                local_and_next(c)
            else:
                body(others(c), mine(c))
            for needed in (True, False):
                s0_start(d, c, needed)

        levels0(d, 2, half, 2, more)
        levels0(d, half, half + 2, 2, lambda c: None)
        if d == 0:
            span_step(1)
        s0_copy(d, (1 - core) * half, half, half).wait_recv()

    def ticks(d, body, finish):
        if crossed:
            trips = half // 2

            def first(m):
                even_first(d, 2 * m)
                odd_first(d, 2 * m + 1)

            def second(m):
                even_second(d, 2 * m)
                odd_second(d, 2 * m + 1)

            def third(m):
                finish(2 * m, 2 * m + 1)

            stages = [(0, first), (trips, second), (trips + 1, third)]
        else:
            trips = half
            stages = [(2 * s, functools.partial(step, d, s)) for s in range(chips)]
            stages.append((2 * chips - 1, finish))

        @pl.loop(0, max(half, trips + stages[-1][0]))
        def _(t):
            @pl.when(t < half)
            def _():
                body(t)

            for n, (lag, stage) in enumerate(stages):
                if d == 0 and 1 <= n + 1 < bits and n >= 1 and not crossed:

                    @pl.when(t == lag)
                    def _():
                        span_step(n + 1)

                @pl.when((t >= lag) & (t < trips + lag))
                def _():
                    stage(t - lag)

    cols_pair(0)
    for c in first_waits:
        c.wait()
    local(others(0))
    pl.semaphore_wait(barrier, len(others_along) + n_tp - 1)
    s0_start(0, 0, True)
    if crossed:
        for o in range(1, n_seq):
            last_copy(o).start()
    else:
        sp_copy(0).start()
    cols_pair(1)
    for c in more_waits:
        c.wait()
    up_load.start()
    gate_load.start()
    first_exchange(0, local, 1)

    tiles = [(i, j) for i in range(nb) for j in range(i + 1)]
    sub = block // dim

    def span_of(i):
        return slice(i * block, (i + 1) * block)

    def decayed(s, h, i, j):
        row = rows[pl.ds(h, 1), j * block : (j + 1) * block]

        def parted(x, t, lo, hi):
            m = cols[h, j * block + hi - 1 : j * block + hi, :]
            width = (hi - lo) // dim
            right = jnp.exp2(jnp.concatenate([m] * width, axis=1) - row[:, lo:hi])
            left = jnp.exp2(cols[h, t : t + x.shape[0], :] - m)
            return (x * right) * jnp.concatenate([left] * width, axis=1)

        if i != j:
            return parted(s, i * block, 0, block).astype(BF16)
        lines = []
        for a in range(sub):
            t = slice(a * dim, (a + 1) * dim)
            line = []
            if a:
                for b in range(a):
                    line.append(
                        parted(s[t, b * dim : (b + 1) * dim], i * block + a * dim, b * dim, (b + 1) * dim)
                    )
            gap = cols[h, i * block + a * dim : i * block + (a + 1) * dim, :] - row[:, t]
            line.append(s[t, t] * jnp.exp2(gap + bias[...]))
            if a + 1 < sub:
                line.append(jnp.zeros((dim, (sub - 1 - a) * dim), F32))
            lines.append(jnp.concatenate([x.astype(BF16) for x in line], axis=1))
        return jnp.concatenate(lines, axis=0)

    def before_norm(h, i):
        r = span_of(i)
        s = jax.nn.sigmoid(gate[r, lane(h)].astype(F32))
        sig[h, r, :] = s
        dnorm[h, r, :] = up[r, lane(h)].astype(F32) * s

    def intra_pair(c):
        work = [(h, i, j) for h in (mine(c), others(c)) for i, j in tiles]

        def scores(h, i, j):
            return nt(q[span_of(i), lane(h)], k[span_of(j), lane(h)])

        ahead = scores(*work[0])
        total = None
        for n, (h, i, j) in enumerate(work):
            s = ahead
            if n + 1 < len(work):
                ahead = scores(*work[n + 1])
            p = decayed(s, h, i, j)
            probs[h, tiles.index((i, j))] = p
            o = nn(p, v[span_of(j), lane(h)])
            total = o if j == 0 else total + o
            if i == j:
                inside[h, span_of(i), :] = total
                before_norm(h, i)

    def finish_attn(*chunks):
        put(0, chunks, state)
        for r in (slice(n, n + 128) for n in range(0, tokens, 128)):
            square, inner = scale_ref[r, :], center_ref[r, :]
            for h in [h for c in chunks for h in (mine(c), others(c))]:
                a = inside[h, r, :] + jnp.exp2(cols[h, r, :]) * nn(q[r, lane(h)], state[h])
                attn[h, r, :] = a
                square = square + a * a
                inner = inner + dnorm[h, r, :] * a
            scale_ref[r, :] = square
            center_ref[r, :] = inner

    scale_ref[...] = jnp.zeros_like(scale_ref)
    center_ref[...] = jnp.zeros_like(center_ref)
    q_load.wait()
    up_load.wait()
    gate_load.wait()
    ticks(0, intra_pair, finish_attn)

    strips = tokens // 128

    def packed(x):
        turned = jnp.sum(x.T, axis=0, keepdims=True)
        return [turned[:, n * 128 : (n + 1) * 128] for n in range(strips)]

    spare = -2 * strips % 8
    pieces = packed(scale_ref[...]) + packed(center_ref[...])
    if spare:
        pieces.append(jnp.zeros((spare, 128), F32))
    sums[...] = jnp.concatenate(pieces, axis=0)

    def tp_copy(d):
        return pltpu.make_async_remote_copy(
            src_ref=sums, dst_ref=sums_in.at[d - 1], send_sem=tp_send.at[0],
            recv_sem=tp_recv.at[0], device_id=(me, lax.rem(z + d, n_tp)), device_id_type=MESH,
        )

    for d in range(1, n_tp):
        tp_copy(d).start()

    def all_sent(d):
        for b in (0, 1):
            s0_copy(d, b * half, 0, half).wait_send()

        def sent_all(s, count):
            part = pl.ds(0, count)
            pltpu.make_async_remote_copy(
                src_ref=sent.at[d, s, part], dst_ref=got.at[d, s, part], send_sem=st_send.at[d, s],
                recv_sem=st_recv.at[d, s, 0], device_id=partner(s + 1), device_id_type=MESH,
            ).wait_send()

        if crossed:
            pl.when(takes(d, 1) == 0)(lambda: sent_all(0, half))
            pl.when(takes(d, 1) == 1)(lambda: sent_all(0, half // 2))
        else:
            for s in range(chips - 1):
                sent_all(s, half)
        pl.when(takes(d, chips) == 0)(lambda: sent_all(chips - 1, half))
        pltpu.make_async_remote_copy(
            src_ref=edge.at[d], dst_ref=far.at[d], send_sem=fin_send.at[d],
            recv_sem=fin_recv.at[d, 0], device_id=partner(0), device_id_type=MESH,
        ).wait_send()

    @pl.loop(0, heads)
    def _(h):
        grow = jnp.exp2(cols[h])
        grown[:, lane(h)] = (q[:, lane(h)].astype(F32) * grow).astype(BF16)

    all_sent(0)
    if crossed:
        lasts(n_seq - 1, 0).wait_send()
    else:
        for b in range(bits):
            sp_copy(b).wait_send()
    total = sums[...]
    every = pltpu.make_async_remote_copy(
        src_ref=sums_in, dst_ref=sums_in, send_sem=tp_send.at[0], recv_sem=tp_recv.at[0],
        device_id=partner(0), device_id_type=MESH,
    )
    if n_tp > 1:
        every.wait_recv()
    for d in range(1, n_tp):
        total = total + sums_in[d - 1]
    scale = lax.rsqrt(total[0:strips] / width + 1e-06)
    center = total[strips : 2 * strips] * scale / width
    for n in range(strips):
        r = slice(n * 128, (n + 1) * 128)
        scale_ref[r, :] = jnp.broadcast_to(scale[n : n + 1, :], (128, 128)).T
        center_ref[r, :] = jnp.broadcast_to(center[n : n + 1, :], (128, 128)).T

    def grads(*some):
        for h in some:
            weighted = None
            for i in range(nb):
                r = span_of(i)
                sc = scale_ref[r, :]
                g = (sc * (dnorm[h, r, :] - attn[h, r, :] * sc * center_ref[r, :])).astype(BF16)
                grad[r, lane(h)] = g
                w = tn(grown[r, lane(h)], g)
                weighted = w if weighted is None else weighted + w
            own[1, h] = weighted

    def outputs(h):
        for i in range(nb):
            r = span_of(i)
            s = sig[h, r, :]
            normed = attn[h, r, :] * scale_ref[r, :]
            up[r, lane(h)] = (normed * s).astype(BF16)
            gate[r, lane(h)] = (dnorm[h, r, :] * normed * (1.0 - s)).astype(BF16)

    first_exchange(1, grads, 0)
    pl.loop(0, heads)(outputs)

    def backward_pair(c):
        pair = (mine(c), others(c))
        work = [(e, i, j) for e in (0, 1) for i, j in tiles]

        def scores(e, i, j):
            return nt(grad[span_of(i), lane(pair[e])], v[span_of(j), lane(pair[e])])

        def add(parts, n, x):
            parts[n] = x if n not in parts else parts[n] + x

        ahead = scores(*work[0])
        dq, dk, dv = {}, {}, {}
        for n, (e, i, j) in enumerate(work):
            h = pair[e]
            s = ahead
            if n + 1 < len(work):
                ahead = scores(*work[n + 1])
            r = span_of(i)
            add(dv, (e, j), tn(grad[r, lane(h)], probs[h, tiles.index((i, j))]))
            pg = decayed(s, h, i, j)
            add(dk, (e, j), tn(q[r, lane(h)], pg))
            add(dq, (e, i), nn(pg, k[span_of(j), lane(h)]))
            if i == j:
                carried = jnp.exp2(cols[h, r, :]) * nt(grad[r, lane(h)], state[h])
                grown[r, lane(h)] = (dq[e, i] + carried).astype(BF16)
            if i == nb - 1:
                dkt[h, :, span_of(j)] = dk[e, j]
                dvt[h, :, span_of(j)] = dv[e, j]

    def put_grads(*chunks):
        put(1, chunks, state_grad)

    ticks(1, backward_pair, put_grads)

    all_sent(1)
    if n_tp > 1:
        every.wait_send()


def last_kernel(
    heads, dim, tokens,
    out_ref, gg_ref, dq_ref, k, v, dkt, dvt, state_grad, rows,
    out_hbm, dq_hbm, dk_hbm, dv_hbm, gg_hbm,
    dk, dv, sem, pair_sem,
):
    block = min(256, tokens)
    many = 4 if heads % 4 == 0 else 2
    trips = heads // many
    whole = [
        pltpu.make_async_copy(a, b, sem.at[i])
        for i, (a, b) in enumerate(((out_ref, out_hbm), (gg_ref, gg_hbm), (dq_ref, dq_hbm)))
    ]
    for c in whole:
        c.start()

    def strips(i):
        part = pl.ds(pl.multiple_of(i * many * dim, many * dim), many * dim)
        return [
            pltpu.make_async_copy(a.at[:, part], b.at[:, part], pair_sem.at[n])
            for n, (a, b) in enumerate(((dk, dk_hbm), (dv, dv_hbm)))
        ]

    @pl.loop(0, trips)
    def _(i):
        for h in [many * i + n for n in range(many)]:
            at = pl.ds(pl.multiple_of(h * dim, dim), dim)
            row = rows[pl.ds(h, 1), :]
            tail = jnp.exp2(row[:, tokens - 1 : tokens] - row)
            for n in range(tokens // block):
                r = slice(n * block, (n + 1) * block)
                key = dkt[h, :, r] + tail[:, r] * nt(state_grad[h], v[r, at])
                value = dvt[h, :, r] + tail[:, r] * t0(state_grad[h], k[r, at])
                dk[r, at] = key.astype(BF16).T
                dv[r, at] = value.astype(BF16).T
        for c in strips(i):
            c.start()

    for n, (a, b) in enumerate(((dk, dk_hbm), (dv, dv_hbm))):
        pltpu.make_async_copy(a, b, pair_sem.at[n]).wait()
    for c in whole:
        c.wait()


def solution(mesh):
    n_seq, n_tp = mesh.shape["seq"], mesh.shape["tp"]

    def shards(queries, keys, values, gate, log_decay, out_grad):
        tokens, flat = queries.shape
        heads = log_decay.shape[1]
        dim = flat // heads
        half = heads // 2
        bits = n_seq.bit_length() - 1
        chips = bits - 1
        block = min(256, tokens)
        nb = tokens // block
        tile = (dim, dim)
        dma = pltpu.SemaphoreType.DMA
        peers = max(n_tp - 1, 1)
        crossed = chips == 2 and half % 2 == 0
        spans = 2 if crossed else bits
        ends = half // 2 if crossed else half
        sums = (-(-2 * (tokens // 128) // 8) * 8, 128)
        hbm = pl.BlockSpec(memory_space=pltpu.HBM)
        vmem = pl.BlockSpec(memory_space=pltpu.VMEM)
        big = pltpu.VMEM((tokens, flat), BF16)
        wide = pltpu.VMEM((heads, tokens, dim), F32)
        turned = pltpu.VMEM((heads, dim, tokens), F32)
        flops = 2 * tokens * tokens * flat * 5 + 2 * tokens * flat * dim * 7
        results = pl.pallas_call(
            functools.partial(kernel, n_seq, n_tp, heads, dim, tokens),
            out_shape=[
                big, big, big, big, big, turned, turned,
                pltpu.VMEM((heads, *tile), BF16), pltpu.VMEM((heads, tokens), F32),
            ],
            in_specs=[hbm] * 6,
            out_specs=[vmem] * 9,
            scratch_shapes=[
                pltpu.VMEM((heads, tokens), F32), big, wide, pltpu.VMEM((tokens, 128), BF16),
                pltpu.VMEM(tile, F32), wide, wide, wide, wide, big,
                pltpu.VMEM((heads, nb * (nb + 1) // 2, block, block), BF16),
                pltpu.VMEM((2, heads, *tile), F32),
                pltpu.VMEM((2, heads, *tile), F32),
                pltpu.VMEM((2, chips, half, *tile), F32),
                pltpu.VMEM((2, chips, half, *tile), F32),
                pltpu.VMEM((2, half, *tile), F32),
                pltpu.VMEM((2, half, *tile), F32),
                pltpu.VMEM((heads, *tile), BF16),
                pltpu.VMEM((bits, heads, dim), F32), pltpu.VMEM((n_seq, heads, dim), F32),
                pltpu.VMEM((2, bits + 1, 3, heads, dim), F32),
                pltpu.VMEM(sums, F32), pltpu.VMEM((peers, *sums), F32),
                pltpu.VMEM((tokens, dim), F32), pltpu.VMEM((tokens, dim), F32),
                dma((8,)), dma((spans,)), dma((spans,)), dma((2,)), dma((2, half + 1)),
                dma((2, chips)), dma((2, chips, half)), dma((2,)), dma((2, ends)),
                dma((1,)), dma((1,)),
            ],
            compiler_params=pltpu.CompilerParams(
                collective_id=0, has_side_effects=True, vmem_limit_bytes=43 << 20
            ),
            cost_estimate=pl.CostEstimate(
                flops=flops, bytes_accessed=tokens * flat * 10, transcendentals=0
            ),
        )(queries, keys, values, gate, log_decay.T, out_grad)
        return tuple(
            pl.pallas_call(
                functools.partial(last_kernel, heads, dim, tokens),
                out_shape=[jax.ShapeDtypeStruct((tokens, flat), BF16)] * 5,
                in_specs=[vmem] * 9,
                out_specs=[hbm] * 5,
                scratch_shapes=[big, big, dma((3,)), dma((2,))],
                compiler_params=pltpu.CompilerParams(vmem_limit_bytes=16 << 20),
                cost_estimate=pl.CostEstimate(
                    flops=4 * tokens * flat * dim, bytes_accessed=tokens * flat * 10, transcendentals=0
                ),
            )(*results)
        )

    spec = P("seq", "tp")
    return jax.shard_map(
        shards, mesh=mesh, in_specs=(spec,) * 6, out_specs=(spec,) * 5, check_vma=False
    )
```

```python
import functools

import jax
import jax.numpy as jnp
from jax import lax
from jax.experimental import pallas as pl
from jax.experimental.pallas import tpu as pltpu
from jax.sharding import PartitionSpec as P

MESH = pl.DeviceIdType.MESH
F32 = jnp.float32
BF16 = jnp.bfloat16
LOG2E = 1.4426950408889634
LOW = -1e9


def nt(a, b):
    return lax.dot_general(a, b, (((1,), (1,)), ((), ())), preferred_element_type=F32)


def tn(a, b):
    return lax.dot_general(a, b, (((0,), (0,)), ((), ())), preferred_element_type=F32)


def nn(a, b):
    return lax.dot_general(a, b, (((1,), (0,)), ((), ())), preferred_element_type=F32)


def t0(a, b):
    return lax.dot_general(a, b, (((0,), (1,)), ((), ())), preferred_element_type=F32)


def three_parts(x):
    high = x.astype(BF16).astype(F32)
    rest = x - high
    middle = rest.astype(BF16).astype(F32)
    low = (rest - middle).astype(BF16).astype(F32)
    return high, middle, low


def stacked(x):
    parts = three_parts(x)
    spare = 128 - 3 * x.shape[0]
    return jnp.concatenate([*parts, jnp.zeros((spare, x.shape[1]), F32)], axis=0)


def kernel(
    n_seq, n_tp, heads, dim, tokens,
    q_hbm, k_hbm, v_hbm, gate_hbm, rate_hbm, up_hbm,
    up, gate, grown, k, v, dkt, dvt, state_grad, rows,
    rate, q, cols, split, bias, inside, attn, sig, dnorm, grad, probs,
    own, other, sent, got, edge, far, state, span, span_in, factor,
    sums, sums_in, scale_ref, center_ref,
    in_sem, sp_send, sp_recv, s0_send, s0_recv, st_send, st_recv, fin_send, fin_recv, tp_send, tp_recv,
):
    width = heads * dim * n_tp
    half = heads // 2
    bits = n_seq.bit_length() - 1
    chips = bits - 1
    block = min(256, tokens)
    nb = tokens // block
    me = lax.axis_index("seq")
    z = lax.axis_index("tp")
    core = lax.rem(me, 2)

    def bit_of(b):
        return lax.rem(me // (1 << b), 2)

    def partner(b):
        return (me + (1 << b) * (1 - 2 * bit_of(b)), z)

    def takes(d, b):
        return bit_of(b) if d == 0 else 1 - bit_of(b)

    def load(i, a, b):
        return pltpu.make_async_copy(a, b, in_sem.at[i])

    rate_load = load(0, rate_hbm, rate)
    q_load, up_load, gate_load = (
        load(1 + i, a, b) for i, (a, b) in enumerate(((q_hbm, q), (up_hbm, up), (gate_hbm, gate)))
    )
    soon = min(2, half)

    def kv_loads(lo, hi, at):
        starts, waits = [], []
        for n, (a, b) in enumerate(((k_hbm, k), (v_hbm, v))):
            for start in (lo, half + lo):
                part = slice(start * dim, (start + hi - lo) * dim)
                starts.append(load(at + n, a.at[:, part], b.at[:, part]))
            both = slice(0, 2 * (hi - lo) * dim)
            waits.append(load(at + n, a.at[:, both], b.at[:, both]))
        return starts, waits

    first_loads, first_waits = kv_loads(0, soon, 4)
    more_loads, more_waits = kv_loads(soon, half, 6) if soon < half else ([], [])
    rate_load.start()
    crossed = chips == 2 and half % 2 == 0
    group = 2 if crossed else 1
    barrier = pltpu.get_barrier_semaphore()
    if crossed:
        others_along = [(lax.rem(me + o, n_seq), z) for o in range(1, n_seq)]
    else:
        others_along = [partner(b) for b in range(bits)]
    for at in others_along:
        pl.semaphore_signal(barrier, inc=1, device_id=at, device_id_type=MESH)
    for d in range(1, n_tp):
        pl.semaphore_signal(
            barrier, inc=1, device_id=(me, lax.rem(z + d, n_tp)), device_id_type=MESH
        )
    for c in first_loads + more_loads:
        c.start()

    def lane(h):
        return pl.ds(pl.multiple_of(h * dim, dim), dim)

    def mine(c):
        return core * half + c

    def others(c):
        return (1 - core) * half + c

    rate_load.wait()
    upto = (
        lax.broadcasted_iota(jnp.int32, (tokens, tokens), 0)
        <= lax.broadcasted_iota(jnp.int32, (tokens, tokens), 1)
    ).astype(BF16)
    parts = nn(stacked(rate[...]).astype(BF16), upto)
    across = parts[0:heads] + parts[heads : 2 * heads] + parts[2 * heads : 3 * heads]
    across = across * LOG2E
    rows[...] = across
    split[...] = stacked(across).T.astype(BF16)
    span[0] = jnp.broadcast_to(across[:, tokens - 1 : tokens], (heads, dim))
    q_load.start()
    corner = lax.broadcasted_iota(jnp.int32, (dim, dim), 0) >= lax.broadcasted_iota(
        jnp.int32, (dim, dim), 1
    )
    bias[...] = jnp.where(corner, 0.0, LOW)

    def cols_pair(c):
        pair = (mine(c), others(c))
        at = lax.broadcasted_iota(jnp.int32, (128, dim), 0)
        pick = jnp.concatenate(
            [
                ((at == h) | (at == h + heads) | (at == h + 2 * heads)).astype(F32).astype(BF16)
                for h in pair
            ],
            axis=1,
        )
        for r in (slice(n, n + 256) for n in range(0, tokens, 256)):
            wide = nn(split[r, :], pick)
            for n, h in enumerate(pair):
                cols[h, r, :] = wide[:, n * dim : (n + 1) * dim]

    def sp_copy(b):
        return pltpu.make_async_remote_copy(
            src_ref=span.at[b], dst_ref=span_in.at[b], send_sem=sp_send.at[b],
            recv_sem=sp_recv.at[b], device_id=partner(b), device_id_type=MESH,
        )

    def last_copy(o):
        if o == 1:
            slot = core
        elif o == n_seq - 1:
            slot = 1 - core
        else:
            slot = 1
        return pltpu.make_async_remote_copy(
            src_ref=span.at[0], dst_ref=span_in.at[me], send_sem=sp_send.at[0],
            recv_sem=sp_recv.at[slot], device_id=(lax.rem(me + o, n_seq), z), device_id_type=MESH,
        )

    def lasts(count, slot):
        part = span_in.at[pl.ds(0, count)]
        return pltpu.make_async_remote_copy(
            src_ref=part, dst_ref=part, send_sem=sp_send.at[0], recv_sem=sp_recv.at[slot],
            device_id=partner(0), device_id_type=MESH,
        )

    def s0_copy(d, h, slot, count=1):
        part = pl.ds(h, count)
        return pltpu.make_async_remote_copy(
            src_ref=own.at[d, part], dst_ref=other.at[d, part], send_sem=s0_send.at[d],
            recv_sem=s0_recv.at[d, slot], device_id=partner(0), device_id_type=MESH,
        )

    def s0_start(d, c, needed):
        if needed:
            s0_copy(d, others(c), c).start()
        else:
            s0_copy(d, mine(c), half).start()

    def st_copy(d, s, c):
        return pltpu.make_async_remote_copy(
            src_ref=sent.at[d, s, c], dst_ref=got.at[d, s, c], send_sem=st_send.at[d, s],
            recv_sem=st_recv.at[d, s, c], device_id=partner(s + 1), device_id_type=MESH,
        )

    def fin_copy(d, c):
        return pltpu.make_async_remote_copy(
            src_ref=edge.at[d, c], dst_ref=far.at[d, c], send_sem=fin_send.at[d],
            recv_sem=fin_recv.at[d, c // group], device_id=partner(0), device_id_type=MESH,
        )

    def set_factors(b, here, there, before):
        for d in (0, 1):
            f = takes(d, b).astype(F32)
            factor[d, b, 0] = jnp.exp2(there * (1.0 - f))
            factor[d, b, 1] = jnp.exp2(here * f)
            factor[d, b, 2] = jnp.exp2(there * f) if b == 0 else f * jnp.exp2(before(d))

    def span_step(b):
        if crossed:
            return crossed_spans(b)
        sp_copy(b).wait_recv()
        here, there = span[b], span_in[b]
        if b + 1 < bits:
            span[b + 1] = here + there
            sp_copy(b + 1).start()

        def before(d):
            total = jnp.zeros((heads, dim), F32)
            for r in range(1, b):
                total = total + takes(d, r).astype(F32) * span_in[r]
            return total

        set_factors(b, here, there, before)

    def crossed_spans(b):
        if b == 0:
            lasts(1, 0).wait_recv()
            set_factors(0, span[0], span_in[partner(0)[0]], None)
            return
        lasts(n_seq - 2, 1).wait_recv()

        def chip(at):
            first = at - lax.rem(at, 2)
            return span_in[first] + span_in[first + 1]

        span_in[me] = span[0]
        mine_all, along_x, along_y = chip(me), chip(partner(1)[0]), chip(partner(2)[0])
        aside = chip(partner(1)[0] + partner(2)[0] - me)
        set_factors(1, mine_all, along_x, lambda d: jnp.zeros((heads, dim), F32))
        set_factors(
            2, mine_all + along_x, along_y + aside, lambda d: takes(d, 1).astype(F32) * along_x
        )
        for d in (0, 1):
            f = takes(d, 1).astype(F32)
            factor[d, bits, 0] = jnp.exp2(aside + mine_all)
            factor[d, bits, 1] = jnp.exp2(f * along_x + (1.0 - f) * aside)

    def row_of(d, b, n, h):
        return factor[d, b, n, pl.ds(h, 1), :]

    def send_level(d, s, c):
        if s == chips - 1:

            @pl.when(takes(d, s + 1) == 0)
            def _():
                st_copy(d, s, c).start()
        else:
            st_copy(d, s, c).start()

    def level0(d, c, crosses):
        h = mine(c)
        s0_copy(d, h, c).wait_recv()
        total = row_of(d, 0, 0, h) * own[d, h] + row_of(d, 0, 1, h) * other[d, h]
        if not crossed:
            sent[d, 0, c] = total
            send_level(d, 0, c)
        elif crosses:
            sent[d, 1, c] = total

            @pl.when(takes(d, 2) == 0)
            def _():
                st_copy(d, 1, c).start()
        else:
            sent[d, 0, c] = total

            @pl.when((takes(d, 1) == 0) | (takes(d, 2) == 0))
            def _():
                st_copy(d, 0, c).start()

    def even_first(d, c):
        h = mine(c)
        fx, fy = takes(d, 1), takes(d, 2)

        @pl.when((fx == 1) | (fy == 0))
        def _():
            st_copy(d, 0, c).wait_recv()
            theirs = got[d, 0, c]
            edge[d, c] = fx.astype(F32) * theirs

            @pl.when(fy == 0)
            def _():
                sent[d, 1, c] = row_of(d, 1, 0, h) * sent[d, 0, c] + row_of(d, 1, 1, h) * theirs
                st_copy(d, 1, c).start()

        @pl.when((fx == 0) & (fy == 1))
        def _():
            edge[d, c] = jnp.zeros((dim, dim), F32)

    def even_second(d, c):
        @pl.when(takes(d, 2) == 1)
        def _():
            st_copy(d, 1, c).wait_recv()
            edge[d, c] = edge[d, c] + row_of(d, 2, 2, mine(c)) * got[d, 1, c]

        fin_copy(d, c).start()

    def odd_first(d, c):
        fx, fy = takes(d, 1), takes(d, 2)

        @pl.when(fy == 1)
        def _():
            st_copy(d, 1, c).wait_recv()

        @pl.when((fx == 0) & (fy == 1))
        def _():
            sent[d, 0, c] = row_of(d, bits, 0, mine(c)) * got[d, 1, c] + sent[d, 1, c]

        @pl.when((fx == 1) & (fy == 1))
        def _():
            sent[d, 0, c] = got[d, 1, c]

        @pl.when((fx == 0) & (fy == 0))
        def _():
            sent[d, 0, c] = sent[d, 1, c]

        @pl.when((fx == 0) | (fy == 1))
        def _():
            st_copy(d, 0, c).start()

    def odd_second(d, c):
        fx, fy = takes(d, 1), takes(d, 2)

        @pl.when((fx == 1) | (fy == 1))
        def _():
            st_copy(d, 0, c).wait_recv()

        @pl.when(fy == 1)
        def _():
            edge[d, c] = got[d, 0, c] + row_of(d, bits, 1, mine(c)) * got[d, 1, c]

        @pl.when((fx == 1) & (fy == 0))
        def _():
            edge[d, c] = got[d, 0, c]

        @pl.when((fx == 0) & (fy == 0))
        def _():
            edge[d, c] = jnp.zeros((dim, dim), F32)

        fin_copy(d, c).start()

    def step(d, s, c):
        h = mine(c)

        def arrive():
            st_copy(d, s, c).wait_recv()
            theirs = got[d, s, c]
            on_top = row_of(d, s + 1, 2, h) * theirs
            edge[d, c] = on_top if s == 0 else edge[d, c] + on_top
            if s + 1 < chips:
                sent[d, s + 1, c] = (
                    row_of(d, s + 1, 0, h) * sent[d, s, c] + row_of(d, s + 1, 1, h) * theirs
                )

        if s + 1 < chips:
            arrive()
            send_level(d, s + 1, c)
            return
        pl.when(takes(d, s + 1) == 1)(arrive)
        if s == 0:

            @pl.when(takes(d, s + 1) == 0)
            def _():
                edge[d, c] = jnp.zeros((dim, dim), F32)

        fin_copy(d, c).start()

    def put(d, chunks, target):
        f = takes(d, 0).astype(F32)
        pltpu.make_async_remote_copy(
            src_ref=edge.at[d, pl.ds(chunks[0], group)], dst_ref=far.at[d, pl.ds(chunks[0], group)],
            send_sem=fin_send.at[d], recv_sem=fin_recv.at[d, chunks[0] // group],
            device_id=partner(0), device_id_type=MESH,
        ).wait_recv()
        for c in chunks:
            for h, end in ((mine(c), edge), (others(c), far)):
                target[h] = (row_of(d, 0, 2, h) * end[d, c] + f * other[d, h]).astype(BF16)

    def local(*some):
        scaled = []
        for h in some:
            last = cols[h, tokens - 1 : tokens, :]
            scaled.append((k[:, lane(h)].astype(F32) * jnp.exp2(last - cols[h])).astype(BF16))
        for h, x in zip(some, scaled):
            own[0, h] = tn(x, v[:, lane(h)])

    def next_cols(c):
        cols_pair(c - (c // half) * (c - half + 1))

    def first_exchange(d, body, done):
        for n, (c, needed) in enumerate(((0, True), (1, True), (0, False), (1, False))):
            if n >= done:
                body(others(c) if needed else mine(c))
                s0_start(d, c, needed)
        if d == 0:
            for c in range(group):
                next_cols(2 + c)
            span_step(0)

        @pl.loop(0, (half - 2) // group)
        def _(n):
            some = [2 + n * group + e for e in range(group)]
            body(*(h for c in some for h in (others(c), mine(c))))
            if d == 0:
                for c in some:
                    next_cols(c + group)
            for needed in (True, False):
                for c in some:
                    s0_start(d, c, needed)
            for e, c in enumerate(some):
                level0(d, c - 2, e == 1)

        if d == 0:
            span_step(1)

    def last_levels0(d):
        for e, c in enumerate((half - 2, half - 1)):
            level0(d, c, e == 1)
        s0_copy(d, (1 - core) * half, half, half).wait_recv()

    def ticks(d, body, finish):
        if crossed:
            trips = half // 2

            def first(m):
                even_first(d, 2 * m)
                odd_first(d, 2 * m + 1)

            def second(m):
                even_second(d, 2 * m)
                odd_second(d, 2 * m + 1)

            def third(m):
                finish(2 * m, 2 * m + 1)

            stages = [(0, first), (trips, second), (trips + 1, third)]
        else:
            trips = half
            stages = [(2 * s, functools.partial(step, d, s)) for s in range(chips)]
            stages.append((2 * chips - 1, finish))

        @pl.loop(0, max(half, trips + stages[-1][0]))
        def _(t):
            @pl.when(t < half)
            def _():
                body(t)

            @pl.when(t == 0)
            def _():
                last_levels0(d)

            for n, (lag, stage) in enumerate(stages):
                if d == 0 and 1 <= n + 1 < bits and n >= 1 and not crossed:

                    @pl.when(t == lag)
                    def _():
                        span_step(n + 1)

                @pl.when((t >= lag) & (t < trips + lag))
                def _():
                    stage(t - lag)

    cols_pair(0)
    for c in first_waits:
        c.wait()
    local(others(0))
    pl.semaphore_wait(barrier, len(others_along) + n_tp - 1)
    s0_start(0, 0, True)
    if crossed:
        for o in range(1, n_seq):
            last_copy(o).start()
    else:
        sp_copy(0).start()
    cols_pair(1)
    for c in more_waits:
        c.wait()
    up_load.start()
    gate_load.start()
    first_exchange(0, local, 1)

    tiles = [(i, j) for i in range(nb) for j in range(i + 1)]
    sub = block // dim

    def span_of(i):
        return slice(i * block, (i + 1) * block)

    def decayed(s, h, i, j):
        row = rows[pl.ds(h, 1), j * block : (j + 1) * block]

        def parted(x, t, lo, hi):
            m = cols[h, j * block + hi - 1 : j * block + hi, :]
            width = (hi - lo) // dim
            right = jnp.exp2(jnp.concatenate([m] * width, axis=1) - row[:, lo:hi])
            left = jnp.exp2(cols[h, t : t + x.shape[0], :] - m)
            return (x * right) * jnp.concatenate([left] * width, axis=1)

        if i != j:
            return parted(s, i * block, 0, block).astype(BF16)
        lines = []
        for a in range(sub):
            t = slice(a * dim, (a + 1) * dim)
            line = []
            if a:
                for b in range(a):
                    line.append(
                        parted(s[t, b * dim : (b + 1) * dim], i * block + a * dim, b * dim, (b + 1) * dim)
                    )
            gap = cols[h, i * block + a * dim : i * block + (a + 1) * dim, :] - row[:, t]
            line.append(s[t, t] * jnp.exp2(gap + bias[...]))
            if a + 1 < sub:
                line.append(jnp.zeros((dim, (sub - 1 - a) * dim), F32))
            lines.append(jnp.concatenate([x.astype(BF16) for x in line], axis=1))
        return jnp.concatenate(lines, axis=0)

    def before_norm(h, i):
        r = span_of(i)
        s = jax.nn.sigmoid(gate[r, lane(h)].astype(F32))
        sig[h, r, :] = s
        dnorm[h, r, :] = up[r, lane(h)].astype(F32) * s

    def intra_pair(c):
        work = [(h, i, j) for h in (mine(c), others(c)) for i, j in tiles]

        def scores(h, i, j):
            return nt(q[span_of(i), lane(h)], k[span_of(j), lane(h)])

        ahead = scores(*work[0])
        total = None
        for n, (h, i, j) in enumerate(work):
            s = ahead
            if n + 1 < len(work):
                ahead = scores(*work[n + 1])
            p = decayed(s, h, i, j)
            probs[h, tiles.index((i, j))] = p
            o = nn(p, v[span_of(j), lane(h)])
            total = o if j == 0 else total + o
            if i == j:
                inside[h, span_of(i), :] = total
                before_norm(h, i)

    def finish_attn(*chunks):
        put(0, chunks, state)
        for r in (slice(n, n + 128) for n in range(0, tokens, 128)):
            square, inner = scale_ref[r, :], center_ref[r, :]
            for h in [h for c in chunks for h in (mine(c), others(c))]:
                a = inside[h, r, :] + jnp.exp2(cols[h, r, :]) * nn(q[r, lane(h)], state[h])
                attn[h, r, :] = a
                square = square + a * a
                inner = inner + dnorm[h, r, :] * a
            scale_ref[r, :] = square
            center_ref[r, :] = inner

    scale_ref[...] = jnp.zeros_like(scale_ref)
    center_ref[...] = jnp.zeros_like(center_ref)
    q_load.wait()
    up_load.wait()
    gate_load.wait()
    ticks(0, intra_pair, finish_attn)

    strips = tokens // 128

    def packed(x):
        turned = jnp.sum(x.T, axis=0, keepdims=True)
        return [turned[:, n * 128 : (n + 1) * 128] for n in range(strips)]

    spare = -2 * strips % 8
    pieces = packed(scale_ref[...]) + packed(center_ref[...])
    if spare:
        pieces.append(jnp.zeros((spare, 128), F32))
    sums[...] = jnp.concatenate(pieces, axis=0)

    def tp_copy(d):
        return pltpu.make_async_remote_copy(
            src_ref=sums, dst_ref=sums_in.at[d - 1], send_sem=tp_send.at[0],
            recv_sem=tp_recv.at[0], device_id=(me, lax.rem(z + d, n_tp)), device_id_type=MESH,
        )

    for d in range(1, n_tp):
        tp_copy(d).start()

    def all_sent(d):
        for b in (0, 1):
            s0_copy(d, b * half, 0, half).wait_send()

        def sent_all(s, count):
            part = pl.ds(0, count)
            pltpu.make_async_remote_copy(
                src_ref=sent.at[d, s, part], dst_ref=got.at[d, s, part], send_sem=st_send.at[d, s],
                recv_sem=st_recv.at[d, s, 0], device_id=partner(s + 1), device_id_type=MESH,
            ).wait_send()

        if crossed:
            pl.when(takes(d, 1) == 0)(lambda: sent_all(0, half))
            pl.when(takes(d, 1) == 1)(lambda: sent_all(0, half // 2))
        else:
            for s in range(chips - 1):
                sent_all(s, half)
        pl.when(takes(d, chips) == 0)(lambda: sent_all(chips - 1, half))
        pltpu.make_async_remote_copy(
            src_ref=edge.at[d], dst_ref=far.at[d], send_sem=fin_send.at[d],
            recv_sem=fin_recv.at[d, 0], device_id=partner(0), device_id_type=MESH,
        ).wait_send()

    @pl.loop(0, heads)
    def _(h):
        grow = jnp.exp2(cols[h])
        grown[:, lane(h)] = (q[:, lane(h)].astype(F32) * grow).astype(BF16)

    all_sent(0)
    if crossed:
        lasts(n_seq - 1, 0).wait_send()
    else:
        for b in range(bits):
            sp_copy(b).wait_send()
    total = sums[...]
    every = pltpu.make_async_remote_copy(
        src_ref=sums_in, dst_ref=sums_in, send_sem=tp_send.at[0], recv_sem=tp_recv.at[0],
        device_id=partner(0), device_id_type=MESH,
    )
    if n_tp > 1:
        every.wait_recv()
    for d in range(1, n_tp):
        total = total + sums_in[d - 1]
    scale = lax.rsqrt(total[0:strips] / width + 1e-06)
    center = total[strips : 2 * strips] * scale / width
    for n in range(strips):
        r = slice(n * 128, (n + 1) * 128)
        scale_ref[r, :] = jnp.broadcast_to(scale[n : n + 1, :], (128, 128)).T
        center_ref[r, :] = jnp.broadcast_to(center[n : n + 1, :], (128, 128)).T

    def grads(*some):
        for h in some:
            weighted = None
            for i in range(nb):
                r = span_of(i)
                sc = scale_ref[r, :]
                g = (sc * (dnorm[h, r, :] - attn[h, r, :] * sc * center_ref[r, :])).astype(BF16)
                grad[r, lane(h)] = g
                w = tn(grown[r, lane(h)], g)
                weighted = w if weighted is None else weighted + w
            own[1, h] = weighted

    def outputs(h):
        for i in range(nb):
            r = span_of(i)
            s = sig[h, r, :]
            normed = attn[h, r, :] * scale_ref[r, :]
            up[r, lane(h)] = (normed * s).astype(BF16)
            gate[r, lane(h)] = (dnorm[h, r, :] * normed * (1.0 - s)).astype(BF16)

    first_exchange(1, grads, 0)
    pl.loop(0, heads)(outputs)

    def backward_pair(c):
        pair = (mine(c), others(c))
        work = [(e, i, j) for e in (0, 1) for i, j in tiles]

        def scores(e, i, j):
            return nt(grad[span_of(i), lane(pair[e])], v[span_of(j), lane(pair[e])])

        def add(parts, n, x):
            parts[n] = x if n not in parts else parts[n] + x

        ahead = scores(*work[0])
        dq, dk, dv = {}, {}, {}
        for n, (e, i, j) in enumerate(work):
            h = pair[e]
            s = ahead
            if n + 1 < len(work):
                ahead = scores(*work[n + 1])
            r = span_of(i)
            add(dv, (e, j), tn(grad[r, lane(h)], probs[h, tiles.index((i, j))]))
            pg = decayed(s, h, i, j)
            add(dk, (e, j), tn(q[r, lane(h)], pg))
            add(dq, (e, i), nn(pg, k[span_of(j), lane(h)]))
            if i == j:
                carried = jnp.exp2(cols[h, r, :]) * nt(grad[r, lane(h)], state[h])
                grown[r, lane(h)] = (dq[e, i] + carried).astype(BF16)
            if i == nb - 1:
                dkt[h, :, span_of(j)] = dk[e, j]
                dvt[h, :, span_of(j)] = dv[e, j]

    def put_grads(*chunks):
        put(1, chunks, state_grad)

    ticks(1, backward_pair, put_grads)

    all_sent(1)
    if n_tp > 1:
        every.wait_send()


def last_kernel(
    heads, dim, tokens,
    out_ref, gg_ref, dq_ref, k, v, dkt, dvt, state_grad, rows,
    out_hbm, dq_hbm, dk_hbm, dv_hbm, gg_hbm,
    dk, dv, sem, pair_sem,
):
    block = min(256, tokens)
    many = 4 if heads % 4 == 0 else 2
    trips = heads // many
    whole = [
        pltpu.make_async_copy(a, b, sem.at[i])
        for i, (a, b) in enumerate(((out_ref, out_hbm), (gg_ref, gg_hbm), (dq_ref, dq_hbm)))
    ]
    for c in whole:
        c.start()

    def strips(i):
        part = pl.ds(pl.multiple_of(i * many * dim, many * dim), many * dim)
        return [
            pltpu.make_async_copy(a.at[:, part], b.at[:, part], pair_sem.at[n])
            for n, (a, b) in enumerate(((dk, dk_hbm), (dv, dv_hbm)))
        ]

    @pl.loop(0, trips)
    def _(i):
        for h in [many * i + n for n in range(many)]:
            at = pl.ds(pl.multiple_of(h * dim, dim), dim)
            row = rows[pl.ds(h, 1), :]
            tail = jnp.exp2(row[:, tokens - 1 : tokens] - row)
            for n in range(tokens // block):
                r = slice(n * block, (n + 1) * block)
                key = dkt[h, :, r] + tail[:, r] * nt(state_grad[h], v[r, at])
                value = dvt[h, :, r] + tail[:, r] * t0(state_grad[h], k[r, at])
                dk[r, at] = key.astype(BF16).T
                dv[r, at] = value.astype(BF16).T
        for c in strips(i):
            c.start()

    for n, (a, b) in enumerate(((dk, dk_hbm), (dv, dv_hbm))):
        pltpu.make_async_copy(a, b, pair_sem.at[n]).wait()
    for c in whole:
        c.wait()


def solution(mesh):
    n_seq, n_tp = mesh.shape["seq"], mesh.shape["tp"]

    def shards(queries, keys, values, gate, log_decay, out_grad):
        tokens, flat = queries.shape
        heads = log_decay.shape[1]
        dim = flat // heads
        half = heads // 2
        bits = n_seq.bit_length() - 1
        chips = bits - 1
        block = min(256, tokens)
        nb = tokens // block
        tile = (dim, dim)
        dma = pltpu.SemaphoreType.DMA
        peers = max(n_tp - 1, 1)
        crossed = chips == 2 and half % 2 == 0
        spans = 2 if crossed else bits
        ends = half // 2 if crossed else half
        sums = (-(-2 * (tokens // 128) // 8) * 8, 128)
        hbm = pl.BlockSpec(memory_space=pltpu.HBM)
        vmem = pl.BlockSpec(memory_space=pltpu.VMEM)
        big = pltpu.VMEM((tokens, flat), BF16)
        wide = pltpu.VMEM((heads, tokens, dim), F32)
        turned = pltpu.VMEM((heads, dim, tokens), F32)
        flops = 2 * tokens * tokens * flat * 5 + 2 * tokens * flat * dim * 7
        results = pl.pallas_call(
            functools.partial(kernel, n_seq, n_tp, heads, dim, tokens),
            out_shape=[
                big, big, big, big, big, turned, turned,
                pltpu.VMEM((heads, *tile), BF16), pltpu.VMEM((heads, tokens), F32),
            ],
            in_specs=[hbm] * 6,
            out_specs=[vmem] * 9,
            scratch_shapes=[
                pltpu.VMEM((heads, tokens), F32), big, wide, pltpu.VMEM((tokens, 128), BF16),
                pltpu.VMEM(tile, F32), wide, wide, wide, wide, big,
                pltpu.VMEM((heads, nb * (nb + 1) // 2, block, block), BF16),
                pltpu.VMEM((2, heads, *tile), F32),
                pltpu.VMEM((2, heads, *tile), F32),
                pltpu.VMEM((2, chips, half, *tile), F32),
                pltpu.VMEM((2, chips, half, *tile), F32),
                pltpu.VMEM((2, half, *tile), F32),
                pltpu.VMEM((2, half, *tile), F32),
                pltpu.VMEM((heads, *tile), BF16),
                pltpu.VMEM((bits, heads, dim), F32), pltpu.VMEM((n_seq, heads, dim), F32),
                pltpu.VMEM((2, bits + 1, 3, heads, dim), F32),
                pltpu.VMEM(sums, F32), pltpu.VMEM((peers, *sums), F32),
                pltpu.VMEM((tokens, dim), F32), pltpu.VMEM((tokens, dim), F32),
                dma((8,)), dma((spans,)), dma((spans,)), dma((2,)), dma((2, half + 1)),
                dma((2, chips)), dma((2, chips, half)), dma((2,)), dma((2, ends)),
                dma((1,)), dma((1,)),
            ],
            compiler_params=pltpu.CompilerParams(
                collective_id=0, has_side_effects=True, vmem_limit_bytes=43 << 20
            ),
            cost_estimate=pl.CostEstimate(
                flops=flops, bytes_accessed=tokens * flat * 10, transcendentals=0
            ),
        )(queries, keys, values, gate, log_decay.T, out_grad)
        return tuple(
            pl.pallas_call(
                functools.partial(last_kernel, heads, dim, tokens),
                out_shape=[jax.ShapeDtypeStruct((tokens, flat), BF16)] * 5,
                in_specs=[vmem] * 9,
                out_specs=[hbm] * 5,
                scratch_shapes=[big, big, dma((3,)), dma((2,))],
                compiler_params=pltpu.CompilerParams(vmem_limit_bytes=16 << 20),
                cost_estimate=pl.CostEstimate(
                    flops=4 * tokens * flat * dim, bytes_accessed=tokens * flat * 10, transcendentals=0
                ),
            )(*results)
        )

    spec = P("seq", "tp")
    return jax.shard_map(
        shards, mesh=mesh, in_specs=(spec,) * 6, out_specs=(spec,) * 5, check_vma=False
    )
```

```python
import functools

import jax
import jax.numpy as jnp
from jax import lax
from jax.experimental import pallas as pl
from jax.experimental.pallas import tpu as pltpu
from jax.sharding import PartitionSpec as P

MESH = pl.DeviceIdType.MESH
F32 = jnp.float32
BF16 = jnp.bfloat16
LOG2E = 1.4426950408889634
LOW = -1e9


def nt(a, b):
    return lax.dot_general(a, b, (((1,), (1,)), ((), ())), preferred_element_type=F32)


def tn(a, b):
    return lax.dot_general(a, b, (((0,), (0,)), ((), ())), preferred_element_type=F32)


def nn(a, b):
    return lax.dot_general(a, b, (((1,), (0,)), ((), ())), preferred_element_type=F32)


def t0(a, b):
    return lax.dot_general(a, b, (((0,), (1,)), ((), ())), preferred_element_type=F32)


def three_parts(x):
    high = x.astype(BF16).astype(F32)
    rest = x - high
    middle = rest.astype(BF16).astype(F32)
    low = (rest - middle).astype(BF16).astype(F32)
    return high, middle, low


def stacked(x):
    parts = three_parts(x)
    spare = 128 - 3 * x.shape[0]
    return jnp.concatenate([*parts, jnp.zeros((spare, x.shape[1]), F32)], axis=0)


def kernel(
    n_seq, n_tp, heads, dim, tokens,
    q_hbm, k_hbm, v_hbm, gate_hbm, rate_hbm, up_hbm,
    up, gate, grown, k, v, dkt, dvt, state_grad, rows,
    rate, q, cols, split, bias, inside, attn, sig, dnorm, grad, probs,
    own, other, sent, got, edge, far, state, span, span_in, factor,
    sums, sums_in, scale_ref, center_ref,
    in_sem, sp_send, sp_recv, s0_send, s0_recv, st_send, st_recv, fin_send, fin_recv, tp_send, tp_recv,
):
    width = heads * dim * n_tp
    half = heads // 2
    bits = n_seq.bit_length() - 1
    chips = bits - 1
    block = min(256, tokens)
    nb = tokens // block
    me = lax.axis_index("seq")
    z = lax.axis_index("tp")
    core = lax.rem(me, 2)

    def bit_of(b):
        return lax.rem(me // (1 << b), 2)

    def partner(b):
        return (me + (1 << b) * (1 - 2 * bit_of(b)), z)

    def takes(d, b):
        return bit_of(b) if d == 0 else 1 - bit_of(b)

    def load(i, a, b):
        return pltpu.make_async_copy(a, b, in_sem.at[i])

    rate_load = load(0, rate_hbm, rate)
    q_load, up_load, gate_load = (
        load(1 + i, a, b) for i, (a, b) in enumerate(((q_hbm, q), (up_hbm, up), (gate_hbm, gate)))
    )
    soon = min(2, half)

    def kv_loads(lo, hi, at):
        starts, waits = [], []
        for n, (a, b) in enumerate(((k_hbm, k), (v_hbm, v))):
            for start in (lo, half + lo):
                part = slice(start * dim, (start + hi - lo) * dim)
                starts.append(load(at + n, a.at[:, part], b.at[:, part]))
            both = slice(0, 2 * (hi - lo) * dim)
            waits.append(load(at + n, a.at[:, both], b.at[:, both]))
        return starts, waits

    first_loads, first_waits = kv_loads(0, soon, 4)
    more_loads, more_waits = kv_loads(soon, half, 6) if soon < half else ([], [])
    rate_load.start()
    crossed = chips == 2 and half % 2 == 0
    group = 2 if crossed else 1
    barrier = pltpu.get_barrier_semaphore()
    if crossed:
        others_along = [(lax.rem(me + o, n_seq), z) for o in range(1, n_seq)]
    else:
        others_along = [partner(b) for b in range(bits)]
    for at in others_along:
        pl.semaphore_signal(barrier, inc=1, device_id=at, device_id_type=MESH)
    for d in range(1, n_tp):
        pl.semaphore_signal(
            barrier, inc=1, device_id=(me, lax.rem(z + d, n_tp)), device_id_type=MESH
        )
    for c in first_loads + more_loads:
        c.start()

    def lane(h):
        return pl.ds(pl.multiple_of(h * dim, dim), dim)

    def mine(c):
        return core * half + c

    def others(c):
        return (1 - core) * half + c

    rate_load.wait()
    upto = (
        lax.broadcasted_iota(jnp.int32, (tokens, tokens), 0)
        <= lax.broadcasted_iota(jnp.int32, (tokens, tokens), 1)
    ).astype(BF16)
    parts = nn(stacked(rate[...]).astype(BF16), upto)
    across = parts[0:heads] + parts[heads : 2 * heads] + parts[2 * heads : 3 * heads]
    across = across * LOG2E
    rows[...] = across
    split[...] = stacked(across).T.astype(BF16)
    span[0] = jnp.broadcast_to(across[:, tokens - 1 : tokens], (heads, dim))
    q_load.start()
    corner = lax.broadcasted_iota(jnp.int32, (dim, dim), 0) >= lax.broadcasted_iota(
        jnp.int32, (dim, dim), 1
    )
    bias[...] = jnp.where(corner, 0.0, LOW)

    def cols_pair(c):
        pair = (mine(c), others(c))
        at = lax.broadcasted_iota(jnp.int32, (128, dim), 0)
        pick = jnp.concatenate(
            [
                ((at == h) | (at == h + heads) | (at == h + 2 * heads)).astype(F32).astype(BF16)
                for h in pair
            ],
            axis=1,
        )
        for r in (slice(n, n + 256) for n in range(0, tokens, 256)):
            wide = nn(split[r, :], pick)
            for n, h in enumerate(pair):
                cols[h, r, :] = wide[:, n * dim : (n + 1) * dim]

    def sp_copy(b):
        return pltpu.make_async_remote_copy(
            src_ref=span.at[b], dst_ref=span_in.at[b], send_sem=sp_send.at[b],
            recv_sem=sp_recv.at[b], device_id=partner(b), device_id_type=MESH,
        )

    def last_copy(o):
        if o == 1:
            slot = core
        elif o == n_seq - 1:
            slot = 1 - core
        else:
            slot = 1
        return pltpu.make_async_remote_copy(
            src_ref=span.at[0], dst_ref=span_in.at[me], send_sem=sp_send.at[0],
            recv_sem=sp_recv.at[slot], device_id=(lax.rem(me + o, n_seq), z), device_id_type=MESH,
        )

    def lasts(count, slot):
        part = span_in.at[pl.ds(0, count)]
        return pltpu.make_async_remote_copy(
            src_ref=part, dst_ref=part, send_sem=sp_send.at[0], recv_sem=sp_recv.at[slot],
            device_id=partner(0), device_id_type=MESH,
        )

    def s0_copy(d, h, slot, count=1):
        part = pl.ds(h, count)
        return pltpu.make_async_remote_copy(
            src_ref=own.at[d, part], dst_ref=other.at[d, part], send_sem=s0_send.at[d],
            recv_sem=s0_recv.at[d, slot], device_id=partner(0), device_id_type=MESH,
        )

    def s0_start(d, c, needed):
        if needed:
            s0_copy(d, others(c), c).start()
        else:
            s0_copy(d, mine(c), half).start()

    def st_copy(d, s, c):
        return pltpu.make_async_remote_copy(
            src_ref=sent.at[d, s, c], dst_ref=got.at[d, s, c], send_sem=st_send.at[d, s],
            recv_sem=st_recv.at[d, s, c], device_id=partner(s + 1), device_id_type=MESH,
        )

    def fin_copy(d, c):
        return pltpu.make_async_remote_copy(
            src_ref=edge.at[d, c], dst_ref=far.at[d, c], send_sem=fin_send.at[d],
            recv_sem=fin_recv.at[d, c // group], device_id=partner(0), device_id_type=MESH,
        )

    def set_factors(b, here, there, before):
        for d in (0, 1):
            f = takes(d, b).astype(F32)
            factor[d, b, 0] = jnp.exp2(there * (1.0 - f))
            factor[d, b, 1] = jnp.exp2(here * f)
            factor[d, b, 2] = jnp.exp2(there * f) if b == 0 else f * jnp.exp2(before(d))

    def span_step(b):
        if crossed:
            return crossed_spans(b)
        sp_copy(b).wait_recv()
        here, there = span[b], span_in[b]
        if b + 1 < bits:
            span[b + 1] = here + there
            sp_copy(b + 1).start()

        def before(d):
            total = jnp.zeros((heads, dim), F32)
            for r in range(1, b):
                total = total + takes(d, r).astype(F32) * span_in[r]
            return total

        set_factors(b, here, there, before)

    def crossed_spans(b):
        if b == 0:
            lasts(1, 0).wait_recv()
            set_factors(0, span[0], span_in[partner(0)[0]], None)
            return
        lasts(n_seq - 2, 1).wait_recv()

        def chip(at):
            first = at - lax.rem(at, 2)
            return span_in[first] + span_in[first + 1]

        span_in[me] = span[0]
        mine_all, along_x, along_y = chip(me), chip(partner(1)[0]), chip(partner(2)[0])
        aside = chip(partner(1)[0] + partner(2)[0] - me)
        set_factors(1, mine_all, along_x, lambda d: jnp.zeros((heads, dim), F32))
        set_factors(
            2, mine_all + along_x, along_y + aside, lambda d: takes(d, 1).astype(F32) * along_x
        )
        for d in (0, 1):
            f = takes(d, 1).astype(F32)
            factor[d, bits, 0] = jnp.exp2(aside + mine_all)
            factor[d, bits, 1] = jnp.exp2(f * along_x + (1.0 - f) * aside)

    def row_of(d, b, n, h):
        return factor[d, b, n, pl.ds(h, 1), :]

    def send_level(d, s, c):
        if s == chips - 1:

            @pl.when(takes(d, s + 1) == 0)
            def _():
                st_copy(d, s, c).start()
        else:
            st_copy(d, s, c).start()

    def level0(d, c, crosses):
        h = mine(c)
        s0_copy(d, h, c).wait_recv()
        total = row_of(d, 0, 0, h) * own[d, h] + row_of(d, 0, 1, h) * other[d, h]
        if not crossed:
            sent[d, 0, c] = total
            send_level(d, 0, c)
        elif crosses:
            sent[d, 1, c] = total

            @pl.when(takes(d, 2) == 0)
            def _():
                st_copy(d, 1, c).start()
        else:
            sent[d, 0, c] = total

            @pl.when((takes(d, 1) == 0) | (takes(d, 2) == 0))
            def _():
                st_copy(d, 0, c).start()

    def even_first(d, c):
        h = mine(c)
        fx, fy = takes(d, 1), takes(d, 2)

        @pl.when((fx == 1) | (fy == 0))
        def _():
            st_copy(d, 0, c).wait_recv()
            theirs = got[d, 0, c]
            edge[d, c] = fx.astype(F32) * theirs

            @pl.when(fy == 0)
            def _():
                sent[d, 1, c] = row_of(d, 1, 0, h) * sent[d, 0, c] + row_of(d, 1, 1, h) * theirs
                st_copy(d, 1, c).start()

        @pl.when((fx == 0) & (fy == 1))
        def _():
            edge[d, c] = jnp.zeros((dim, dim), F32)

    def even_second(d, c):
        @pl.when(takes(d, 2) == 1)
        def _():
            st_copy(d, 1, c).wait_recv()
            edge[d, c] = edge[d, c] + row_of(d, 2, 2, mine(c)) * got[d, 1, c]

        fin_copy(d, c).start()

    def odd_first(d, c):
        fx, fy = takes(d, 1), takes(d, 2)

        @pl.when(fy == 1)
        def _():
            st_copy(d, 1, c).wait_recv()

        @pl.when((fx == 0) & (fy == 1))
        def _():
            sent[d, 0, c] = row_of(d, bits, 0, mine(c)) * got[d, 1, c] + sent[d, 1, c]

        @pl.when((fx == 1) & (fy == 1))
        def _():
            sent[d, 0, c] = got[d, 1, c]

        @pl.when((fx == 0) & (fy == 0))
        def _():
            sent[d, 0, c] = sent[d, 1, c]

        @pl.when((fx == 0) | (fy == 1))
        def _():
            st_copy(d, 0, c).start()

    def odd_second(d, c):
        fx, fy = takes(d, 1), takes(d, 2)

        @pl.when((fx == 1) | (fy == 1))
        def _():
            st_copy(d, 0, c).wait_recv()

        @pl.when(fy == 1)
        def _():
            edge[d, c] = got[d, 0, c] + row_of(d, bits, 1, mine(c)) * got[d, 1, c]

        @pl.when((fx == 1) & (fy == 0))
        def _():
            edge[d, c] = got[d, 0, c]

        @pl.when((fx == 0) & (fy == 0))
        def _():
            edge[d, c] = jnp.zeros((dim, dim), F32)

        fin_copy(d, c).start()

    def step(d, s, c):
        h = mine(c)

        def arrive():
            st_copy(d, s, c).wait_recv()
            theirs = got[d, s, c]
            on_top = row_of(d, s + 1, 2, h) * theirs
            edge[d, c] = on_top if s == 0 else edge[d, c] + on_top
            if s + 1 < chips:
                sent[d, s + 1, c] = (
                    row_of(d, s + 1, 0, h) * sent[d, s, c] + row_of(d, s + 1, 1, h) * theirs
                )

        if s + 1 < chips:
            arrive()
            send_level(d, s + 1, c)
            return
        pl.when(takes(d, s + 1) == 1)(arrive)
        if s == 0:

            @pl.when(takes(d, s + 1) == 0)
            def _():
                edge[d, c] = jnp.zeros((dim, dim), F32)

        fin_copy(d, c).start()

    def put(d, chunks, target):
        f = takes(d, 0).astype(F32)
        pltpu.make_async_remote_copy(
            src_ref=edge.at[d, pl.ds(chunks[0], group)], dst_ref=far.at[d, pl.ds(chunks[0], group)],
            send_sem=fin_send.at[d], recv_sem=fin_recv.at[d, chunks[0] // group],
            device_id=partner(0), device_id_type=MESH,
        ).wait_recv()
        for c in chunks:
            for h, end in ((mine(c), edge), (others(c), far)):
                target[h] = (row_of(d, 0, 2, h) * end[d, c] + f * other[d, h]).astype(BF16)

    def local(*some):
        scaled = []
        for h in some:
            last = cols[h, tokens - 1 : tokens, :]
            scaled.append((k[:, lane(h)].astype(F32) * jnp.exp2(last - cols[h])).astype(BF16))
        for h, x in zip(some, scaled):
            own[0, h] = tn(x, v[:, lane(h)])

    def next_cols(c):
        cols_pair(c - (c // half) * (c - half + 1))

    def first_exchange(d, body, done):
        for n, (c, needed) in enumerate(((0, True), (1, True), (0, False), (1, False))):
            if n >= done:
                body(others(c) if needed else mine(c))
                s0_start(d, c, needed)
        if d == 0:
            for c in range(group):
                next_cols(2 + c)
            span_step(0)

        def block_of(n):
            some = [2 + n * group + e for e in range(group)]
            body(*(h for c in some for h in (others(c), mine(c))))
            if d == 0:
                for c in some:
                    next_cols(c + group)
            for needed in (True, False):
                for c in some:
                    s0_start(d, c, needed)
            return some

        ahead = d == 0 and crossed
        if ahead:
            level0(d, 0, False)
            level0(d, 1, True)
            block_of(0)

        @pl.loop(1 if ahead else 0, (half - 2) // group)
        def _(n):
            for e, c in enumerate(block_of(n)):
                level0(d, c - 2, e == 1)

        if d == 0:
            span_step(1)

    def last_levels0(d):
        for e, c in enumerate((half - 2, half - 1)):
            level0(d, c, e == 1)
        s0_copy(d, (1 - core) * half, half, half).wait_recv()

    def ticks(d, body, finish):
        if crossed:
            trips = half // 2

            def first(m):
                even_first(d, 2 * m)
                odd_first(d, 2 * m + 1)

            def second(m):
                even_second(d, 2 * m)
                odd_second(d, 2 * m + 1)

            def third(m):
                finish(2 * m, 2 * m + 1)

            stages = [(0, first), (trips, second), (trips + 1, third)]
        else:
            trips = half
            stages = [(2 * s, functools.partial(step, d, s)) for s in range(chips)]
            stages.append((2 * chips - 1, finish))

        @pl.loop(0, max(half, trips + stages[-1][0]))
        def _(t):
            @pl.when(t < half)
            def _():
                body(t)

            @pl.when(t == 0)
            def _():
                last_levels0(d)

            for n, (lag, stage) in enumerate(stages):
                if d == 0 and 1 <= n + 1 < bits and n >= 1 and not crossed:

                    @pl.when(t == lag)
                    def _():
                        span_step(n + 1)

                @pl.when((t >= lag) & (t < trips + lag))
                def _():
                    stage(t - lag)

    cols_pair(0)
    for c in first_waits:
        c.wait()
    local(others(0))
    pl.semaphore_wait(barrier, len(others_along) + n_tp - 1)
    s0_start(0, 0, True)
    if crossed:
        for o in range(1, n_seq):
            last_copy(o).start()
    else:
        sp_copy(0).start()
    cols_pair(1)
    for c in more_waits:
        c.wait()
    up_load.start()
    gate_load.start()
    first_exchange(0, local, 1)

    tiles = [(i, j) for i in range(nb) for j in range(i + 1)]
    sub = block // dim

    def span_of(i):
        return slice(i * block, (i + 1) * block)

    def decayed(s, h, i, j):
        row = rows[pl.ds(h, 1), j * block : (j + 1) * block]

        def parted(x, t, lo, hi):
            m = cols[h, j * block + hi - 1 : j * block + hi, :]
            width = (hi - lo) // dim
            right = jnp.exp2(jnp.concatenate([m] * width, axis=1) - row[:, lo:hi])
            left = jnp.exp2(cols[h, t : t + x.shape[0], :] - m)
            return (x * right) * jnp.concatenate([left] * width, axis=1)

        if i != j:
            return parted(s, i * block, 0, block).astype(BF16)
        lines = []
        for a in range(sub):
            t = slice(a * dim, (a + 1) * dim)
            line = []
            if a:
                for b in range(a):
                    line.append(
                        parted(s[t, b * dim : (b + 1) * dim], i * block + a * dim, b * dim, (b + 1) * dim)
                    )
            gap = cols[h, i * block + a * dim : i * block + (a + 1) * dim, :] - row[:, t]
            line.append(s[t, t] * jnp.exp2(gap + bias[...]))
            if a + 1 < sub:
                line.append(jnp.zeros((dim, (sub - 1 - a) * dim), F32))
            lines.append(jnp.concatenate([x.astype(BF16) for x in line], axis=1))
        return jnp.concatenate(lines, axis=0)

    def before_norm(h, i):
        r = span_of(i)
        s = jax.nn.sigmoid(gate[r, lane(h)].astype(F32))
        sig[h, r, :] = s
        dnorm[h, r, :] = up[r, lane(h)].astype(F32) * s

    def intra_pair(c):
        work = [(h, i, j) for h in (mine(c), others(c)) for i, j in tiles]

        def scores(h, i, j):
            return nt(q[span_of(i), lane(h)], k[span_of(j), lane(h)])

        ahead = scores(*work[0])
        total = None
        for n, (h, i, j) in enumerate(work):
            s = ahead
            if n + 1 < len(work):
                ahead = scores(*work[n + 1])
            p = decayed(s, h, i, j)
            probs[h, tiles.index((i, j))] = p
            o = nn(p, v[span_of(j), lane(h)])
            total = o if j == 0 else total + o
            if i == j:
                inside[h, span_of(i), :] = total
                before_norm(h, i)

    def finish_attn(*chunks):
        put(0, chunks, state)
        for r in (slice(n, n + 128) for n in range(0, tokens, 128)):
            square, inner = scale_ref[r, :], center_ref[r, :]
            for h in [h for c in chunks for h in (mine(c), others(c))]:
                a = inside[h, r, :] + jnp.exp2(cols[h, r, :]) * nn(q[r, lane(h)], state[h])
                attn[h, r, :] = a
                square = square + a * a
                inner = inner + dnorm[h, r, :] * a
            scale_ref[r, :] = square
            center_ref[r, :] = inner

    scale_ref[...] = jnp.zeros_like(scale_ref)
    center_ref[...] = jnp.zeros_like(center_ref)
    q_load.wait()
    up_load.wait()
    gate_load.wait()
    ticks(0, intra_pair, finish_attn)

    strips = tokens // 128

    def packed(x):
        turned = jnp.sum(x.T, axis=0, keepdims=True)
        return [turned[:, n * 128 : (n + 1) * 128] for n in range(strips)]

    spare = -2 * strips % 8
    pieces = packed(scale_ref[...]) + packed(center_ref[...])
    if spare:
        pieces.append(jnp.zeros((spare, 128), F32))
    sums[...] = jnp.concatenate(pieces, axis=0)

    def tp_copy(d):
        return pltpu.make_async_remote_copy(
            src_ref=sums, dst_ref=sums_in.at[d - 1], send_sem=tp_send.at[0],
            recv_sem=tp_recv.at[0], device_id=(me, lax.rem(z + d, n_tp)), device_id_type=MESH,
        )

    for d in range(1, n_tp):
        tp_copy(d).start()

    def all_sent(d):
        for b in (0, 1):
            s0_copy(d, b * half, 0, half).wait_send()

        def sent_all(s, count):
            part = pl.ds(0, count)
            pltpu.make_async_remote_copy(
                src_ref=sent.at[d, s, part], dst_ref=got.at[d, s, part], send_sem=st_send.at[d, s],
                recv_sem=st_recv.at[d, s, 0], device_id=partner(s + 1), device_id_type=MESH,
            ).wait_send()

        if crossed:
            pl.when(takes(d, 1) == 0)(lambda: sent_all(0, half))
            pl.when(takes(d, 1) == 1)(lambda: sent_all(0, half // 2))
        else:
            for s in range(chips - 1):
                sent_all(s, half)
        pl.when(takes(d, chips) == 0)(lambda: sent_all(chips - 1, half))
        pltpu.make_async_remote_copy(
            src_ref=edge.at[d], dst_ref=far.at[d], send_sem=fin_send.at[d],
            recv_sem=fin_recv.at[d, 0], device_id=partner(0), device_id_type=MESH,
        ).wait_send()

    @pl.loop(0, heads)
    def _(h):
        grow = jnp.exp2(cols[h])
        grown[:, lane(h)] = (q[:, lane(h)].astype(F32) * grow).astype(BF16)

    all_sent(0)
    if crossed:
        lasts(n_seq - 1, 0).wait_send()
    else:
        for b in range(bits):
            sp_copy(b).wait_send()
    total = sums[...]
    every = pltpu.make_async_remote_copy(
        src_ref=sums_in, dst_ref=sums_in, send_sem=tp_send.at[0], recv_sem=tp_recv.at[0],
        device_id=partner(0), device_id_type=MESH,
    )
    if n_tp > 1:
        every.wait_recv()
    for d in range(1, n_tp):
        total = total + sums_in[d - 1]
    scale = lax.rsqrt(total[0:strips] / width + 1e-06)
    center = total[strips : 2 * strips] * scale / width
    for n in range(strips):
        r = slice(n * 128, (n + 1) * 128)
        scale_ref[r, :] = jnp.broadcast_to(scale[n : n + 1, :], (128, 128)).T
        center_ref[r, :] = jnp.broadcast_to(center[n : n + 1, :], (128, 128)).T

    def grads(*some):
        for h in some:
            weighted = None
            for i in range(nb):
                r = span_of(i)
                sc = scale_ref[r, :]
                g = (sc * (dnorm[h, r, :] - attn[h, r, :] * sc * center_ref[r, :])).astype(BF16)
                grad[r, lane(h)] = g
                w = tn(grown[r, lane(h)], g)
                weighted = w if weighted is None else weighted + w
            own[1, h] = weighted

    def outputs(h):
        for i in range(nb):
            r = span_of(i)
            s = sig[h, r, :]
            normed = attn[h, r, :] * scale_ref[r, :]
            up[r, lane(h)] = (normed * s).astype(BF16)
            gate[r, lane(h)] = (dnorm[h, r, :] * normed * (1.0 - s)).astype(BF16)

    first_exchange(1, grads, 0)
    pl.loop(0, heads)(outputs)

    def backward_pair(c):
        pair = (mine(c), others(c))
        work = [(e, i, j) for e in (0, 1) for i, j in tiles]

        def scores(e, i, j):
            return nt(grad[span_of(i), lane(pair[e])], v[span_of(j), lane(pair[e])])

        def add(parts, n, x):
            parts[n] = x if n not in parts else parts[n] + x

        ahead = scores(*work[0])
        dq, dk, dv = {}, {}, {}
        for n, (e, i, j) in enumerate(work):
            h = pair[e]
            s = ahead
            if n + 1 < len(work):
                ahead = scores(*work[n + 1])
            r = span_of(i)
            add(dv, (e, j), tn(grad[r, lane(h)], probs[h, tiles.index((i, j))]))
            pg = decayed(s, h, i, j)
            add(dk, (e, j), tn(q[r, lane(h)], pg))
            add(dq, (e, i), nn(pg, k[span_of(j), lane(h)]))
            if i == j:
                carried = jnp.exp2(cols[h, r, :]) * nt(grad[r, lane(h)], state[h])
                grown[r, lane(h)] = (dq[e, i] + carried).astype(BF16)
            if i == nb - 1:
                dkt[h, :, span_of(j)] = dk[e, j]
                dvt[h, :, span_of(j)] = dv[e, j]

    def put_grads(*chunks):
        put(1, chunks, state_grad)

    ticks(1, backward_pair, put_grads)

    all_sent(1)
    if n_tp > 1:
        every.wait_send()


def last_kernel(
    heads, dim, tokens,
    out_ref, gg_ref, dq_ref, k, v, dkt, dvt, state_grad, rows,
    out_hbm, dq_hbm, dk_hbm, dv_hbm, gg_hbm,
    dk, dv, sem, pair_sem,
):
    block = min(256, tokens)
    many = 4 if heads % 4 == 0 else 2
    trips = heads // many
    whole = [
        pltpu.make_async_copy(a, b, sem.at[i])
        for i, (a, b) in enumerate(((out_ref, out_hbm), (gg_ref, gg_hbm), (dq_ref, dq_hbm)))
    ]
    for c in whole:
        c.start()

    def strips(i):
        part = pl.ds(pl.multiple_of(i * many * dim, many * dim), many * dim)
        return [
            pltpu.make_async_copy(a.at[:, part], b.at[:, part], pair_sem.at[n])
            for n, (a, b) in enumerate(((dk, dk_hbm), (dv, dv_hbm)))
        ]

    @pl.loop(0, trips)
    def _(i):
        for h in [many * i + n for n in range(many)]:
            at = pl.ds(pl.multiple_of(h * dim, dim), dim)
            row = rows[pl.ds(h, 1), :]
            tail = jnp.exp2(row[:, tokens - 1 : tokens] - row)
            for n in range(tokens // block):
                r = slice(n * block, (n + 1) * block)
                key = dkt[h, :, r] + tail[:, r] * nt(state_grad[h], v[r, at])
                value = dvt[h, :, r] + tail[:, r] * t0(state_grad[h], k[r, at])
                dk[r, at] = key.astype(BF16).T
                dv[r, at] = value.astype(BF16).T
        for c in strips(i):
            c.start()

    for n, (a, b) in enumerate(((dk, dk_hbm), (dv, dv_hbm))):
        pltpu.make_async_copy(a, b, pair_sem.at[n]).wait()
    for c in whole:
        c.wait()


def solution(mesh):
    n_seq, n_tp = mesh.shape["seq"], mesh.shape["tp"]

    def shards(queries, keys, values, gate, log_decay, out_grad):
        tokens, flat = queries.shape
        heads = log_decay.shape[1]
        dim = flat // heads
        half = heads // 2
        bits = n_seq.bit_length() - 1
        chips = bits - 1
        block = min(256, tokens)
        nb = tokens // block
        tile = (dim, dim)
        dma = pltpu.SemaphoreType.DMA
        peers = max(n_tp - 1, 1)
        crossed = chips == 2 and half % 2 == 0
        spans = 2 if crossed else bits
        ends = half // 2 if crossed else half
        sums = (-(-2 * (tokens // 128) // 8) * 8, 128)
        hbm = pl.BlockSpec(memory_space=pltpu.HBM)
        vmem = pl.BlockSpec(memory_space=pltpu.VMEM)
        big = pltpu.VMEM((tokens, flat), BF16)
        wide = pltpu.VMEM((heads, tokens, dim), F32)
        turned = pltpu.VMEM((heads, dim, tokens), F32)
        flops = 2 * tokens * tokens * flat * 5 + 2 * tokens * flat * dim * 7
        results = pl.pallas_call(
            functools.partial(kernel, n_seq, n_tp, heads, dim, tokens),
            out_shape=[
                big, big, big, big, big, turned, turned,
                pltpu.VMEM((heads, *tile), BF16), pltpu.VMEM((heads, tokens), F32),
            ],
            in_specs=[hbm] * 6,
            out_specs=[vmem] * 9,
            scratch_shapes=[
                pltpu.VMEM((heads, tokens), F32), big, wide, pltpu.VMEM((tokens, 128), BF16),
                pltpu.VMEM(tile, F32), wide, wide, wide, wide, big,
                pltpu.VMEM((heads, nb * (nb + 1) // 2, block, block), BF16),
                pltpu.VMEM((2, heads, *tile), F32),
                pltpu.VMEM((2, heads, *tile), F32),
                pltpu.VMEM((2, chips, half, *tile), F32),
                pltpu.VMEM((2, chips, half, *tile), F32),
                pltpu.VMEM((2, half, *tile), F32),
                pltpu.VMEM((2, half, *tile), F32),
                pltpu.VMEM((heads, *tile), BF16),
                pltpu.VMEM((bits, heads, dim), F32), pltpu.VMEM((n_seq, heads, dim), F32),
                pltpu.VMEM((2, bits + 1, 3, heads, dim), F32),
                pltpu.VMEM(sums, F32), pltpu.VMEM((peers, *sums), F32),
                pltpu.VMEM((tokens, dim), F32), pltpu.VMEM((tokens, dim), F32),
                dma((8,)), dma((spans,)), dma((spans,)), dma((2,)), dma((2, half + 1)),
                dma((2, chips)), dma((2, chips, half)), dma((2,)), dma((2, ends)),
                dma((1,)), dma((1,)),
            ],
            compiler_params=pltpu.CompilerParams(
                collective_id=0, has_side_effects=True, vmem_limit_bytes=44 << 20
            ),
            cost_estimate=pl.CostEstimate(
                flops=flops, bytes_accessed=tokens * flat * 10, transcendentals=0
            ),
        )(queries, keys, values, gate, log_decay.T, out_grad)
        return tuple(
            pl.pallas_call(
                functools.partial(last_kernel, heads, dim, tokens),
                out_shape=[jax.ShapeDtypeStruct((tokens, flat), BF16)] * 5,
                in_specs=[vmem] * 9,
                out_specs=[hbm] * 5,
                scratch_shapes=[big, big, dma((3,)), dma((2,))],
                compiler_params=pltpu.CompilerParams(vmem_limit_bytes=16 << 20),
                cost_estimate=pl.CostEstimate(
                    flops=4 * tokens * flat * dim, bytes_accessed=tokens * flat * 10, transcendentals=0
                ),
            )(*results)
        )

    spec = P("seq", "tp")
    return jax.shard_map(
        shards, mesh=mesh, in_specs=(spec,) * 6, out_specs=(spec,) * 5, check_vma=False
    )
```
